128 devices in a mesh: tan: 4 (over x), grid: 32 (over z, y, core).
Axes of the slice: x: 4, y: 4, z: 4, core: 2. Of those that a mesh axis runs over, the one named last changes fastest.
Arguments:
- base: float32 [2, 256, 256], P(None, 'grid'), may hold values from 0.05 to 0.6
- tangents: float32 [512, 2, 256, 256], P('tan', None, 'grid'), may hold values from -6 to 6
Outputs:
- frames: float32 [512, 2, 256, 256], P('tan', None, 'grid')
- factor: float32 [512, 512], P('tan')
The draws below stay inside these ranges and needn't reach their ends.
All inputs are finite; a program needn't handle non-finite values.
Results may differ from the reference program's by a relative error of at most 0.000092.
Values sent between devices are 32-bit elements; how exact they have to be, the bound alone decides.
A program may use at most 128 MiB of HBM per device.

```python
import math
import jax
import jax.numpy as jnp
from jax import lax

K = 512
NX = 256
NY = 256
STEPS = 2


def block_levels(own_key, extent, split, least, largest):
    level = 1.0
    for dim, shards_of in split:
        heights = jax.random.uniform(jax.random.fold_in(jax.random.fold_in(own_key, 6), dim), (shards_of,), jnp.float32, least / len(split), largest / len(split))
        level = level * jnp.repeat(jnp.exp(heights), extent[dim] // shards_of).reshape((-1,) + (1,) * (len(extent) - 1 - dim))
    return level


def noise(rng, dims, deviation, most, shards=(), kind=jnp.bfloat16):
    loudness = block_levels(rng, dims, shards, -0.22, 0.18) if shards else 1.0
    entries = jax.random.normal(rng, dims, jnp.float32) * deviation * loudness
    return jnp.minimum(jnp.maximum(entries, -most), most).astype(kind)


def setup_inputs(seed: int = 0) -> dict:
    seeds = jax.random.split(jax.random.key(seed), 3)
    return {
        "base": jnp.clip(0.05 + 0.55 * jax.random.uniform(seeds[0], (2, NX, NY), jnp.float32) ** block_levels(seeds[0], (2, NX, NY), ((1, 32),), -0.2, 0.2), 0.05, 0.6),
        "tangents": noise(seeds[1], (K, 2, NX, NY), 1.0, 6.0, ((0, 4), (2, 32)), jnp.float32),
    }


spread_u = 1.0
spread_v = 0.5
feed_rate = 0.04
kill_rate = 0.06
step_size = 0.33

def reaction_terms(centre, spread):
    substrate = centre[0, 0]
    catalyst = centre[0, 1]
    growth = substrate * catalyst * catalyst
    base_sub = spread_u * spread[0, 0] - growth + feed_rate * (1.0 - substrate)
    base_cat = spread_v * spread[0, 1] + growth - (feed_rate + kill_rate) * catalyst
    coupling = catalyst * catalyst * centre[1:, 0] + 2.0 * substrate * catalyst * centre[1:, 1]
    pert_sub = spread_u * spread[1:, 0] - coupling - feed_rate * centre[1:, 0]
    pert_cat = spread_v * spread[1:, 1] + coupling - (feed_rate + kill_rate) * centre[1:, 1]
    base_rate = jnp.stack([base_sub, base_cat])[None]
    pert_rate = jnp.stack([pert_sub, pert_cat], 1)
    return jnp.concatenate([base_rate, pert_rate], 0)

def rates(state):
    spread = jnp.roll(state, -1, 2) + jnp.roll(state, 1, 2) + jnp.roll(state, 1, 3) + jnp.roll(state, -1, 3) - 4.0 * state
    return reaction_terms(state, spread)

def advance_block(block, base):
    state = jnp.concatenate([base[None], block], 0)
    for step in range(STEPS):
        slope_one = rates(state)
        slope_two = rates(state + 0.5 * step_size * slope_one)
        slope_three = rates(state + 0.5 * step_size * slope_two)
        slope_four = rates(state + step_size * slope_three)
        state = state + step_size / 6.0 * (slope_one + 2.0 * slope_two + 2.0 * slope_three + slope_four)
    return state[1:]

def reference(base, tangents):
    width = math.gcd(K, 64)
    blocks = tangents.reshape(K // width, width, 2, NX, NY)
    advanced = lax.map(lambda block: advance_block(block, base), blocks)
    matrix = advanced.reshape(K, 2 * NX * NY)
    gram = jnp.dot(matrix.astype(jnp.float32), matrix.T.astype(jnp.float32), precision=lax.Precision.HIGHEST, preferred_element_type=jnp.float32) / (2.0 * NX * NY)
    factor = jnp.linalg.cholesky(gram)
    inverse = jax.scipy.linalg.solve_triangular(factor, jnp.eye(K, dtype=jnp.float32), lower=True)
    frames = jnp.dot(inverse.astype(jnp.float32), matrix.astype(jnp.float32), precision=lax.Precision.HIGHEST, preferred_element_type=jnp.float32)
    return (frames.reshape(K, 2, NX, NY), factor)
```

```python
import functools
import jax
import jax.numpy as jnp
from jax import lax
from jax.experimental import pallas as pl
from jax.experimental.pallas import tpu as pltpu
from jax.sharding import Mesh
from jax.sharding import PartitionSpec as P

K = 512
NX = 256
NY = 256
GRID = ("grid_0", "grid_1", "grid_2")
HI = lax.Precision.HIGHEST

def padded_to(lines, count):
    spare = -lines.shape[0] % count
    if not spare:
        return lines
    return jnp.concatenate([lines, jnp.zeros((spare, *lines.shape[1:]), lines.dtype)])


def from_everyone(value, axis):
    count = lax.axis_size(axis)
    return lax.all_to_all(
        jnp.broadcast_to(value[None], (count, *value.shape)), axis, 0, 0, tiled=True
    )


def joined_along(blocks, dim):
    shape = list(blocks.shape[1:])
    shape[dim] *= blocks.shape[0]
    return jnp.moveaxis(blocks, 0, dim).reshape(shape)


def gather_axes(value, axes, dim):
    far, near = axes
    leading = from_everyone(value, far)
    blocks = jnp.swapaxes(from_everyone(leading, near), 0, 1)
    return joined_along(blocks.reshape(-1, *value.shape), dim)


def cut_along(value, dim, count):
    shape = value.shape
    blocks = value.reshape(*shape[:dim], count, shape[dim] // count, *shape[dim + 1 :])
    return jnp.moveaxis(blocks, dim, 0)


def sent_and_summed(value, axis, dim):
    count = lax.axis_size(axis)
    blocks = lax.all_to_all(cut_along(value, dim, count), axis, 0, 0, tiled=True)
    return jnp.sum(blocks, axis=0)


def sum_by_axis(value, axes, dim):
    far, near = axes
    own = sent_and_summed(cut_along(value, dim, lax.axis_size(far)), near, dim + 1)
    return jnp.sum(lax.all_to_all(own, far, 0, 0, tiled=True), axis=0)


def sum_by_parts(value, axes):
    lines = value.reshape(-1, value.shape[-1])
    padded = padded_to(lines, lax.axis_size(axes[0]) * lax.axis_size(axes[1]))
    whole = gather_axes(sum_by_axis(padded, axes, 0), axes, 0)
    return lax.slice_in_dim(whole, 0, len(lines)).reshape(value.shape)


def factor_block(d, rows, width=16):
    lane = lax.broadcasted_iota(jnp.int32, (8, 128), 1)
    sub = lax.broadcasted_iota(jnp.int32, (8, 128), 0)
    wide = lambda x: jnp.broadcast_to(x, (8, 128))
    e = [jnp.where(lane == sub + 8 * i, 1.0, 0.0).astype(jnp.float32) for i in range(16)]
    for s in range(0, 128, width):
        t0 = s // 8
        c = [
            {i: wide(d[i][:, s + j : s + j + 1]) for i in range(t0 + j // 8, 16)}
            for j in range(width)
        ]
        for j in range(width):
            tj, sj = t0 + j // 8, j % 8
            r = lax.rsqrt(wide(c[j][tj][sj : sj + 1, :]))
            low = {i: c[j][i] * r for i in range(tj, 16)}
            for k in range(j + 1, width):
                tk, sk = t0 + k // 8, k % 8
                m = wide(low[tk][sk : sk + 1, :])
                for i in range(tk, 16):
                    c[k][i] = c[k][i] - low[i] * m
            row_d = wide(d[tj][sj : sj + 1, :]) * r
            row_e = wide(e[tj][sj : sj + 1, :]) * r
            rows(s + j, row_d[0:1], row_e[0:1])
            for i in range(tj, 16):
                d[i] = d[i] - low[i] * row_d
                e[i] = e[i] - low[i] * row_e


def dot(a, b, dims=((1,), (0,))):
    return lax.dot_general(a, b, (dims, ((), ())), precision=HI, preferred_element_type=jnp.float32)


def factor_kernel(width, scale, g_ref, inv_ref, fac_ref, a_ref, e_ref, u_ref, w_ref):
    a_ref[...] = g_ref[...] * scale
    e_ref[...] = jnp.zeros_like(e_ref)
    u_ref[...] = jnp.zeros_like(u_ref)
    inv_ref[...] = jnp.zeros_like(inv_ref)

    def step(k, carry):
        at = pl.multiple_of(k * 128, 128)
        d = [a_ref[pl.ds(pl.multiple_of(at + 8 * i, 8), 8), pl.ds(at, 128)] for i in range(16)]

        def rows(j, row_d, row_e):
            w_ref[j : j + 1, 0:128] = row_d
            w_ref[j : j + 1, 128:256] = row_e

        factor_block(d, rows, width)
        for kk in range(4):
            @pl.when(k == kk)
            def _():
                lo, hi = kk * 128, kk * 128 + 128
                upper = lax.broadcasted_iota(jnp.int32, (128, 128), 1) >= lax.broadcasted_iota(jnp.int32, (128, 128), 0)
                u_ref[lo:hi, lo:hi] = jnp.where(upper, w_ref[:, 0:128], 0.0)
                w = w_ref[:, 128:256]
                inv_ref[lo:hi, lo:hi] = w
                if kk:
                    inv_ref[lo:hi, 0:lo] = dot(w, e_ref[lo:hi, 0:lo])
                if kk < 3:
                    right = dot(w, a_ref[lo:hi, hi:512])
                    u_ref[lo:hi, hi:512] = right
                    left = right.T
                    a_ref[hi:512, hi:512] = a_ref[hi:512, hi:512] - dot(left, right)
                    e_ref[hi:512, 0:hi] = e_ref[hi:512, 0:hi] - dot(left, inv_ref[lo:hi, 0:hi])
        return carry

    lax.fori_loop(0, 4, step, 0)
    t = pl.multiple_of(lax.axis_index("tan") * 128, 128)
    fac_ref[...] = u_ref[:, pl.ds(t, 128)].T


def factored(gram, scale, width=16):
    return pl.pallas_call(
        functools.partial(factor_kernel, width, scale),
        out_shape=(jax.ShapeDtypeStruct((K, K), jnp.float32), jax.ShapeDtypeStruct((K // 4, K), jnp.float32)),
        in_specs=[pl.BlockSpec(memory_space=pltpu.VMEM)],
        out_specs=(pl.BlockSpec(memory_space=pltpu.VMEM),) * 2,
        scratch_shapes=[pltpu.VMEM((K, K), jnp.float32)] * 3 + [pltpu.VMEM((128, 256), jnp.float32)],
        name="factor",
    )(gram)


spread_u, spread_v, feed_rate, kill_rate, step_size = 1.0, 0.5, 0.04, 0.06, 0.33
STAGES = (0.5 * step_size, 0.5 * step_size, step_size, step_size / 6.0) * 2

def base_coefficients(u, v, coef_ref):
    def lap(x):
        return (pltpu.roll(x, 1, 0) + pltpu.roll(x, 23, 0) + pltpu.roll(x, 1, 1) + pltpu.roll(x, NY - 1, 1) - 4.0 * x)

    def slopes(u, v):
        growth = u * v * v
        return (
            spread_u * lap(u) - growth + feed_rate * (1.0 - u),
            spread_v * lap(v) + growth - (feed_rate + kill_rate) * v,
        )

    for step in range(2):
        su, sv = u, v
        tu = tv = 0.0
        for stage in range(4):
            scale = STAGES[stage]
            square, cross = v2uv(su, sv)
            own = {0: 1.0, 1: 0.0, 2: 0.0, 3: 1.0 / 3.0}[stage]
            coef_ref[step * 4 + stage, 0] = own - scale * (4.0 * spread_u + feed_rate + square)
            coef_ref[step * 4 + stage, 1] = scale * cross
            coef_ref[step * 4 + stage, 2] = scale * square
            coef_ref[step * 4 + stage, 3] = own + scale * (cross - 4.0 * spread_v - feed_rate - kill_rate)
            if step == 1 and stage == 3:
                break
            ku, kv = slopes(su, sv)
            weight = (1.0, 2.0, 2.0, 1.0)[stage]
            tu, tv = tu + weight * ku, tv + weight * kv
            if stage < 3:
                ahead = (0.5, 0.5, 1.0)[stage] * step_size
                su, sv = u + ahead * ku, v + ahead * kv
        u, v = u + step_size / 6.0 * tu, v + step_size / 6.0 * tv


def v2uv(u, v):
    return v * v, 2.0 * u * v


def advance_group(get, put, coef_ref, z_refs, y_ref):
    first = get
    for stage in range(8):
        phase = stage % 4
        scale = STAGES[stage]
        out_lo, out_hi = stage + 1, 23 - stage
        src = {0: first, 1: reader(z_refs[0]), 2: reader(z_refs[1]), 3: reader(z_refs[2])}[phase]
        window = {}

        def at(row):
            if row not in window:
                window[row] = (src(0, row), src(1, row))
            return window[row]

        for row in range(out_lo, out_hi):
            up, mid, down = at(row - 1), at(row), at(row + 1)
            sums = [
                (up[f] + down[f]) + (pltpu.roll(mid[f], 1, 1) + pltpu.roll(mid[f], NY - 1, 1))
                for f in range(2)
            ]
            cp, bp, cq, aq = (coef_ref[stage, n, row : row + 1, :] for n in range(4))
            p = scale * spread_u * sums[0] + (cp * mid[0] - bp * mid[1])
            q = scale * spread_v * sums[1] + (cq * mid[0] + aq * mid[1])
            for f, new in ((0, p), (1, q)):
                if phase in (1, 2):
                    new = new + first(f, row)
                if phase == 3:
                    two = z_refs[1][f, row]
                    new = new + (1.0 / 3.0) * ((z_refs[0][f, row] - first(f, row)) + (two + two))
                if stage == 7:
                    put(f, row - 8, new)
                elif phase == 3:
                    y_ref[f, row] = new
                else:
                    z_refs[phase][f, row] = new
            del window[row - 1]
        if stage == 3:
            first = reader(y_ref)


def reader(ref):
    return lambda f, row: ref[f, row]


def rk_kernel(ub_ref, x_ref, top_ref, bot_ref, o_ref, coef_ref, z0, z1, z2, y_ref):
    base_coefficients(ub_ref[0], ub_ref[1], coef_ref)

    def group(g, carry):
        lane = pl.ds(pl.multiple_of(g * 8, 8), 8)

        def get(f, row):
            ref = (top_ref, x_ref, bot_ref)[row // 8]
            return ref[f, row % 8, lane, :]

        def put(f, row, value):
            o_ref[f, row, lane, :] = value

        advance_group(get, put, coef_ref, (z0, z1, z2), y_ref)
        return carry

    lax.fori_loop(0, 16, group, 0)


def advanced(base_ext, x, top, bot):
    return pl.pallas_call(
        rk_kernel,
        out_shape=jax.ShapeDtypeStruct(x.shape, jnp.float32),
        in_specs=[pl.BlockSpec(memory_space=pltpu.VMEM)] * 4,
        out_specs=pl.BlockSpec(memory_space=pltpu.VMEM),
        scratch_shapes=[pltpu.VMEM((8, 4, 24, NY), jnp.float32)] + [pltpu.VMEM((2, 24, 8, NY), jnp.float32)] * 4,
        name="advance",
    )(base_ext, x, top, bot)


def gram_kernel(v_ref, g_ref):
    for i in range(4):
        lo = i * 128
        total = None
        for f in range(2):
            for row in range(2):
                part = dot(v_ref[f, row, lo : lo + 128, :], v_ref[f, row, lo:K, :], ((1,), (1,)))
                total = part if total is None else total + part
        g_ref[lo : lo + 128, lo:K] = total
        if lo:
            g_ref[lo : lo + 128, 0:lo] = jnp.zeros((128, lo), jnp.float32)


def partial_gram(v):
    return pl.pallas_call(
        gram_kernel,
        out_shape=jax.ShapeDtypeStruct((K, K), jnp.float32),
        in_specs=[pl.BlockSpec(memory_space=pltpu.VMEM)],
        out_specs=pl.BlockSpec(memory_space=pltpu.VMEM),
        name="gram",
    )(v)


def frames_kernel(inv_ref, v_ref, o_ref):
    for i in range(4):
        lo = i * 128
        for f in range(2):
            for row in range(2):
                o_ref[f, row, lo : lo + 128, :] = dot(inv_ref[lo : lo + 128, 0 : lo + 128], v_ref[f, row, 0 : lo + 128, :])


def framed(inv, v):
    return pl.pallas_call(
        frames_kernel,
        out_shape=jax.ShapeDtypeStruct(v.shape, jnp.float32),
        in_specs=[pl.BlockSpec(memory_space=pltpu.VMEM)] * 2,
        out_specs=pl.BlockSpec(memory_space=pltpu.VMEM),
        name="frames",
    )(inv, v)


def neighbours(band):
    count = lax.axis_size(GRID)
    return (
        lax.ppermute(band, GRID, [(i, (i + 1) % count) for i in range(count)]),
        lax.ppermute(band, GRID, [((i + 1) % count, i) for i in range(count)]),
    )


def per_device(base, tangents):
    x = jnp.transpose(tangents, (1, 2, 0, 3))
    above, below = neighbours(base)
    top, bottom = neighbours(x)
    v = advanced(jnp.concatenate([above, base, below], 1), x, top, bottom)
    v = lax.all_to_all(v, "tan", split_axis=1, concat_axis=2, tiled=True)
    gram = sum_by_parts(partial_gram(v), (("tan", "grid_0", "grid_1"), "grid_2"))
    inverse, factor_rows = factored(gram, 1.0 / (2.0 * NX * NY), 8)
    frames = lax.all_to_all(framed(inverse, v), "tan", split_axis=2, concat_axis=1, tiled=True)
    return (jnp.transpose(frames, (2, 0, 1, 3)), factor_rows)


def solution(mesh):
    split = Mesh(
        mesh.devices.reshape(mesh.shape["tan"], 4, 4, 2), ("tan", "grid_0", "grid_1", "grid_2")
    )
    placed = (P(None, GRID, None), P("tan", None, GRID, None))
    return jax.shard_map(
        per_device,
        mesh=split,
        in_specs=placed,
        out_specs=(P("tan", None, GRID, None), P("tan", None)),
        check_vma=False,
    )
```

```python
import functools
import jax
import jax.numpy as jnp
from jax import lax
from jax.experimental import pallas as pl
from jax.experimental.pallas import tpu as pltpu
from jax.sharding import Mesh
from jax.sharding import PartitionSpec as P

K = 512
NX = 256
NY = 256
GRID = ("grid_0", "grid_1", "grid_2")
HI = lax.Precision.HIGHEST

def factor_block(d, rows, width=16):
    lane = lax.broadcasted_iota(jnp.int32, (8, 128), 1)
    sub = lax.broadcasted_iota(jnp.int32, (8, 128), 0)
    wide = lambda x: jnp.broadcast_to(x, (8, 128))
    e = [jnp.where(lane == sub + 8 * i, 1.0, 0.0).astype(jnp.float32) for i in range(16)]
    for s in range(0, 128, width):
        t0 = s // 8
        c = [
            {i: wide(d[i][:, s + j : s + j + 1]) for i in range(t0 + j // 8, 16)}
            for j in range(width)
        ]
        for j in range(width):
            tj, sj = t0 + j // 8, j % 8
            r = lax.rsqrt(wide(c[j][tj][sj : sj + 1, :]))
            low = {i: c[j][i] * r for i in range(tj, 16)}
            for k in range(j + 1, width):
                tk, sk = t0 + k // 8, k % 8
                m = wide(low[tk][sk : sk + 1, :])
                for i in range(tk, 16):
                    c[k][i] = c[k][i] - low[i] * m
            row_d = wide(d[tj][sj : sj + 1, :]) * r
            row_e = wide(e[tj][sj : sj + 1, :]) * r
            rows(s + j, row_d[0:1], row_e[0:1])
            for i in range(tj, 16):
                d[i] = d[i] - low[i] * row_d
                e[i] = e[i] - low[i] * row_e


def dot(a, b, dims=((1,), (0,))):
    return lax.dot_general(a, b, (dims, ((), ())), precision=HI, preferred_element_type=jnp.float32)


def factor_kernel(width, scale, g_ref, inv_ref, fac_ref, a_ref, e_ref, u_ref, w_ref):
    block = 0
    for i in range(4):
        for j in range(i, 4):
            a_ref[i * 128 : i * 128 + 128, j * 128 : j * 128 + 128] = g_ref[block * 128 : block * 128 + 128] * scale
            block += 1
    e_ref[...] = jnp.zeros_like(e_ref)
    u_ref[...] = jnp.zeros_like(u_ref)
    inv_ref[...] = jnp.zeros_like(inv_ref)

    def step(k, carry):
        at = pl.multiple_of(k * 128, 128)
        d = [a_ref[pl.ds(pl.multiple_of(at + 8 * i, 8), 8), pl.ds(at, 128)] for i in range(16)]

        def rows(j, row_d, row_e):
            w_ref[j : j + 1, 0:128] = row_d
            w_ref[j : j + 1, 128:256] = row_e

        factor_block(d, rows, width)
        for kk in range(4):
            @pl.when(k == kk)
            def _():
                lo, hi = kk * 128, kk * 128 + 128
                upper = lax.broadcasted_iota(jnp.int32, (128, 128), 1) >= lax.broadcasted_iota(jnp.int32, (128, 128), 0)
                u_ref[lo:hi, lo:hi] = jnp.where(upper, w_ref[:, 0:128], 0.0)
                w = w_ref[:, 128:256]
                inv_ref[lo:hi, lo:hi] = w
                if kk:
                    inv_ref[lo:hi, 0:lo] = dot(w, e_ref[lo:hi, 0:lo])
                if kk < 3:
                    right = dot(w, a_ref[lo:hi, hi:512])
                    u_ref[lo:hi, hi:512] = right
                    left = right.T
                    a_ref[hi:512, hi:512] = a_ref[hi:512, hi:512] - dot(left, right)
                    e_ref[hi:512, 0:hi] = e_ref[hi:512, 0:hi] - dot(left, inv_ref[lo:hi, 0:hi])
        return carry

    lax.fori_loop(0, 4, step, 0)
    t = pl.multiple_of(lax.axis_index("tan") * 128, 128)
    fac_ref[...] = u_ref[:, pl.ds(t, 128)].T


def factored(gram, scale, width=16):
    return pl.pallas_call(
        functools.partial(factor_kernel, width, scale),
        out_shape=(jax.ShapeDtypeStruct((K, K), jnp.float32), jax.ShapeDtypeStruct((K // 4, K), jnp.float32)),
        in_specs=[pl.BlockSpec(memory_space=pltpu.VMEM)],
        out_specs=(pl.BlockSpec(memory_space=pltpu.VMEM),) * 2,
        scratch_shapes=[pltpu.VMEM((K, K), jnp.float32)] * 3 + [pltpu.VMEM((128, 256), jnp.float32)],
        name="factor",
    )(gram)


spread_u, spread_v, feed_rate, kill_rate, step_size = 1.0, 0.5, 0.04, 0.06, 0.33
STAGES = (0.5 * step_size, 0.5 * step_size, step_size, step_size / 6.0) * 2

def base_coefficients(u, v, coef_ref):
    def lap(x):
        return (pltpu.roll(x, 1, 0) + pltpu.roll(x, 23, 0) + pltpu.roll(x, 1, 1) + pltpu.roll(x, NY - 1, 1) - 4.0 * x)

    def slopes(u, v):
        growth = u * v * v
        return (
            spread_u * lap(u) - growth + feed_rate * (1.0 - u),
            spread_v * lap(v) + growth - (feed_rate + kill_rate) * v,
        )

    for step in range(2):
        su, sv = u, v
        tu = tv = 0.0
        for stage in range(4):
            scale = STAGES[stage]
            square, cross = v2uv(su, sv)
            own = {0: 1.0, 1: 0.0, 2: 0.0, 3: 1.0 / 3.0}[stage]
            coef_ref[step * 4 + stage, 0] = own - scale * (4.0 * spread_u + feed_rate + square)
            coef_ref[step * 4 + stage, 1] = scale * cross
            coef_ref[step * 4 + stage, 2] = scale * square
            coef_ref[step * 4 + stage, 3] = own + scale * (cross - 4.0 * spread_v - feed_rate - kill_rate)
            if step == 1 and stage == 3:
                break
            ku, kv = slopes(su, sv)
            weight = (1.0, 2.0, 2.0, 1.0)[stage]
            tu, tv = tu + weight * ku, tv + weight * kv
            if stage < 3:
                ahead = (0.5, 0.5, 1.0)[stage] * step_size
                su, sv = u + ahead * ku, v + ahead * kv
        u, v = u + step_size / 6.0 * tu, v + step_size / 6.0 * tv


def v2uv(u, v):
    return v * v, 2.0 * u * v


def advance_group(get, put, coef_ref, z_refs, y_ref):
    first = get
    for stage in range(8):
        phase = stage % 4
        scale = STAGES[stage]
        out_lo, out_hi = stage + 1, 23 - stage
        src = {0: first, 1: reader(z_refs[0]), 2: reader(z_refs[1]), 3: reader(z_refs[2])}[phase]
        window = {}

        def at(row):
            if row not in window:
                window[row] = (src(0, row), src(1, row))
            return window[row]

        for row in range(out_lo, out_hi):
            up, mid, down = at(row - 1), at(row), at(row + 1)
            sums = [
                (up[f] + down[f]) + (pltpu.roll(mid[f], 1, 1) + pltpu.roll(mid[f], NY - 1, 1))
                for f in range(2)
            ]
            cp, bp, cq, aq = (coef_ref[stage, n, row : row + 1, :] for n in range(4))
            p = scale * spread_u * sums[0] + (cp * mid[0] - bp * mid[1])
            q = scale * spread_v * sums[1] + (cq * mid[0] + aq * mid[1])
            for f, new in ((0, p), (1, q)):
                if phase in (1, 2):
                    new = new + first(f, row)
                if phase == 3:
                    two = z_refs[1][f, row]
                    new = new + (1.0 / 3.0) * ((z_refs[0][f, row] - first(f, row)) + (two + two))
                if stage == 7:
                    put(f, row - 8, new)
                elif phase == 3:
                    y_ref[f, row] = new
                else:
                    z_refs[phase][f, row] = new
            del window[row - 1]
        if stage == 3:
            first = reader(y_ref)


def reader(ref):
    return lambda f, row: ref[f, row]


CHUNK = 16
CHUNKS = 128 // CHUNK
MESH_ID = pl.DeviceIdType.MESH


def place():
    return tuple(lax.axis_index(a) for a in ("tan",) + GRID)


def band_at(index):
    return {"grid_0": index // 8, "grid_1": index // 2 % 4, "grid_2": index % 2}


def along(core, turn, shift):
    x, z, y, _ = place()
    order = ((x, y), (y, z), (z, x))[turn]
    spot = order[0] * (1 - core) + order[1] * core
    first, second = shift * (1 - core), shift * core
    steps = {0: (first, 0, second), 1: (0, second, first), 2: (second, first, 0)}[turn]
    there = {
        "tan": (x + steps[0]) % 4,
        "grid_0": (z + steps[1]) % 4,
        "grid_1": (y + steps[2]) % 4,
    }
    return there, spot


def remote(source, target, send, receive, device):
    return pltpu.make_async_remote_copy(
        src_ref=source, dst_ref=target, send_sem=send, recv_sem=receive, device_id=device, device_id_type=MESH_ID
    )


def greet(devices):
    barrier = pltpu.get_barrier_semaphore()
    for device in devices:
        pl.semaphore_signal(barrier, inc=1, device_id=device, device_id_type=MESH_ID)
    pl.semaphore_wait(barrier, len(devices))


def sum_over_devices(part, acc, from_core, got_a, got_b, got_c, mid, low, total, sends, receives):
    x, z, y, core = place()
    other = {"grid_2": 1 - core}
    half = lambda c: pl.ds(pl.multiple_of(c * 640, 128), 640)
    copy = remote(part.at[half(1 - core)], from_core, sends.at[0], receives.at[0], other)
    copy.start()
    copy.wait()
    acc[...] = part[half(core)] + from_core[...]
    copies = []
    for k in (1, 3, 2):
        there, spot = along(core, 0, k)
        rows = pl.ds(pl.multiple_of((spot + k) % 4 * 160, 8), 160)
        copies.append(remote(acc.at[rows], got_a.at[k - 1], sends.at[k], receives.at[k], there))
        copies[-1].start()
    for copy in copies:
        copy.wait()
    spot_a = along(core, 0, 0)[1]
    mid[...] = (acc[pl.ds(pl.multiple_of(spot_a * 160, 8), 160)] + got_a[0]) + (got_a[1] + got_a[2])
    copies = []
    for k in (1, 3, 2):
        there, spot = along(core, 1, k)
        rows = pl.ds(pl.multiple_of((spot + k) % 4 * 40, 8), 40)
        copies.append(remote(mid.at[rows], got_b.at[k - 1], sends.at[3 + k], receives.at[3 + k], there))
        copies[-1].start()
    for copy in copies:
        copy.wait()
    spot_b = along(core, 1, 0)[1]
    low[...] = (mid[pl.ds(pl.multiple_of(spot_b * 40, 8), 40)] + got_b[0]) + (got_b[1] + got_b[2])
    copies = []
    for k in (1, 3, 2):
        there, spot_c = along(core, 2, k)
        copies.append(remote(low, got_c.at[spot_c], sends.at[6 + k], receives.at[6 + k], there))
        copies[-1].start()
    got_c[along(core, 2, 0)[1]] = low[...]
    for copy in copies:
        copy.wait()
    own_b = pl.ds(pl.multiple_of(spot_a * 160 + spot_b * 40 + core * 640, 8), 40)
    total[own_b] = (got_c[0] + got_c[1]) + (got_c[2] + got_c[3])
    copies = []
    for k in (1, 3, 2):
        there, _ = along(core, 1, k)
        copies.append(remote(total.at[own_b], total.at[own_b], sends.at[9 + k], receives.at[9 + k], there))
        copies[-1].start()
    for copy in copies:
        copy.wait()
    own_a = pl.ds(pl.multiple_of(spot_a * 160 + core * 640, 8), 160)
    copies = []
    for k in (1, 3, 2):
        there, _ = along(core, 0, k)
        copies.append(remote(total.at[own_a], total.at[own_a], sends.at[12 + k], receives.at[12 + k], there))
        copies[-1].start()
    for copy in copies:
        copy.wait()
    copy = remote(total.at[half(core)], total.at[half(core)], sends.at[16], receives.at[16], other)
    copy.start()
    copy.wait()


def packed_gram(v, part):
    block = 0
    for i in range(4):
        lo = i * 128
        total = None
        for f in range(2):
            for row in range(2):
                term = dot(v[f, row, lo : lo + 128, :], v[f, row, lo:K, :], ((1,), (1,)))
                total = term if total is None else total + term
        for j in range(i, 4):
            part[block * 128 : block * 128 + 128] = total[:, (j - i) * 128 : (j - i) * 128 + 128]
            block += 1


def evolve_kernel(
    base_ref, x_ref, v_out, total,
    base_above, base_below, top, bottom, out, v, part, acc, from_core, got_a, got_b, got_c, mid, low,
    coef_ref, z0, z1, z2, y_ref,
    base_send, base_recv, halo_send, halo_recv, give_send, give_recv, sum_send, sum_recv, out_sem,
):
    x, z, y, core = place()
    band = (z * 4 + y) * 2 + core
    after, before = band_at((band + 1) % 32), band_at((band + 31) % 32)
    peers = [{"tan": (x + k) % 4} for k in (1, 2, 3)]
    greet(
        [after, before, {"grid_2": 1 - core}] + peers
        + [{"grid_1": (y + k) % 4} for k in (1, 2, 3)] + [{"grid_0": (z + k) % 4} for k in (1, 2, 3)]
    )
    bases = (
        remote(base_ref, base_above, base_send.at[0], base_recv.at[0], after),
        remote(base_ref, base_below, base_send.at[1], base_recv.at[1], before),
    )
    for copy in bases:
        copy.start()

    def halos(c):
        some = pl.ds(pl.multiple_of(c * CHUNK, CHUNK), CHUNK)
        return (
            remote(x_ref.at[:, :, some], top.at[:, :, some], halo_send.at[c, 0], halo_recv.at[c, 0], after),
            remote(x_ref.at[:, :, some], bottom.at[:, :, some], halo_send.at[c, 1], halo_recv.at[c, 1], before),
        )

    def gifts(c):
        some = pl.ds(pl.multiple_of(c * CHUNK, CHUNK), CHUNK)
        mine = pl.ds(pl.multiple_of(x * 128 + c * CHUNK, CHUNK), CHUNK)
        return [
            remote(
                out.at[:, pl.ds((x + k) % 4 * 2, 2), some], v.at[:, :, mine],
                give_send.at[c, k - 1], give_recv.at[c, k - 1], {"tan": (x + k) % 4},
            )
            for k in (1, 3, 2)
        ]

    def give(c):
        some = pl.ds(pl.multiple_of(c * CHUNK, CHUNK), CHUNK)
        mine = pl.ds(pl.multiple_of(x * 128 + c * CHUNK, CHUNK), CHUNK)
        v[:, :, mine] = out[:, pl.ds(x * 2, 2), some]
        for copy in gifts(c):
            copy.start()

    def start_halo(c, carry):
        for copy in halos(c):
            copy.start()
        return carry

    lax.fori_loop(0, CHUNKS, start_halo, 0)
    for copy in bases:
        copy.wait_recv()
    u, w = (jnp.concatenate([base_above[f], base_ref[f], base_below[f]], 0) for f in range(2))
    base_coefficients(u, w, coef_ref)

    def advance_chunk(c, carry):
        for copy in halos(c):
            copy.wait_recv()

        @pl.when(c > 0)
        def _():
            give(c - 1)

        def group(g, carry):
            eight = pl.ds(pl.multiple_of(c * CHUNK + g * 8, 8), 8)

            def get(f, row):
                ref = (top, x_ref, bottom)[row // 8]
                return ref[f, row % 8, eight, :]

            def put(f, row, value):
                out[f, row, eight, :] = value

            advance_group(get, put, coef_ref, (z0, z1, z2), y_ref)
            return carry

        return lax.fori_loop(0, CHUNK // 8, group, carry)

    lax.fori_loop(0, CHUNKS, advance_chunk, 0)
    give(CHUNKS - 1)

    def receive(c, carry):
        for copy in gifts(c):
            copy.wait_recv()
        return carry

    lax.fori_loop(0, CHUNKS, receive, 0)
    keep = pltpu.make_async_copy(v, v_out, out_sem)
    keep.start()
    packed_gram(v, part)
    sum_over_devices(part, acc, from_core, got_a, got_b, got_c, mid, low, total, sum_send, sum_recv)

    def finish(c, carry):
        for copy in halos(c):
            copy.wait_send()
        for copy in gifts(c):
            copy.wait_send()
        return carry

    lax.fori_loop(0, CHUNKS, finish, 0)
    for copy in bases:
        copy.wait_send()
    keep.wait()


def evolved(base, x):
    f32 = lambda *shape: pltpu.VMEM(shape, jnp.float32)
    sem = pltpu.SemaphoreType.DMA
    return pl.pallas_call(
        evolve_kernel,
        out_shape=(jax.ShapeDtypeStruct((2, 2, K, NY), jnp.float32), jax.ShapeDtypeStruct((1280, 128), jnp.float32)),
        in_specs=[pl.BlockSpec(memory_space=pltpu.VMEM)] * 2,
        out_specs=(pl.BlockSpec(memory_space=pl.ANY), pl.BlockSpec(memory_space=pltpu.VMEM)),
        scratch_shapes=[
            f32(2, 8, NY), f32(2, 8, NY), f32(2, 8, 128, NY), f32(2, 8, 128, NY), f32(2, 8, 128, NY), f32(2, 2, K, NY),
            f32(1280, 128), f32(640, 128), f32(640, 128), f32(3, 160, 128), f32(3, 40, 128), f32(4, 40, 128),
            f32(160, 128), f32(40, 128),
            f32(8, 4, 24, NY), f32(2, 24, 8, NY), f32(2, 24, 8, NY), f32(2, 24, 8, NY), f32(2, 24, 8, NY),
            sem((2,)), sem((2,)), sem((CHUNKS, 2)), sem((CHUNKS, 2)), sem((CHUNKS, 3)), sem((CHUNKS, 3)),
            sem((17,)), sem((17,)), sem(()),
        ],
        compiler_params=pltpu.CompilerParams(collective_id=0, has_side_effects=True, vmem_limit_bytes=40 * 1024 * 1024),
        name="evolve",
    )(base, x)


def return_kernel(inv_ref, v_ref, o_ref, made, own, send, receive, own_sem):
    x, z, y, core = place()
    greet([{"tan": (x + k) % 4} for k in (1, 2, 3)])

    def gift(k, f, row):
        n = f * 2 + row
        return remote(
            made.at[k - 1, f, row], o_ref.at[f, x * 2 + row], send.at[k - 1, n], receive.at[k - 1, n], {"tan": (x + k) % 4}
        )

    def frame(block, f, row):
        rows = inv_ref[pl.ds(pl.multiple_of(block * 128, 128), 128), :]
        return dot(rows, v_ref[f, row])

    pairs = [(f, row) for f in range(2) for row in range(2)]
    for f, row in pairs:
        for k in (1, 3, 2):
            made[k - 1, f, row] = frame((x + k) % 4, f, row)
            gift(k, f, row).start()
    keeps = []
    for f, row in pairs:
        own[f, row] = frame(x, f, row)
        keeps.append(pltpu.make_async_copy(own.at[f, row], o_ref.at[f, x * 2 + row], own_sem.at[f * 2 + row]))
        keeps[-1].start()
    for f, row in pairs:
        for k in (1, 3, 2):
            gift(k, f, row).wait()
    for keep in keeps:
        keep.wait()


def returned(inv, v):
    f32 = lambda *shape: pltpu.VMEM(shape, jnp.float32)
    sem = pltpu.SemaphoreType.DMA
    return pl.pallas_call(
        return_kernel,
        out_shape=jax.ShapeDtypeStruct((2, 8, 128, NY), jnp.float32),
        in_specs=[pl.BlockSpec(memory_space=pltpu.VMEM)] * 2,
        out_specs=pl.BlockSpec(memory_space=pl.ANY),
        scratch_shapes=[f32(3, 2, 2, 128, NY), f32(2, 2, 128, NY), sem((3, 4)), sem((3, 4)), sem((4,))],
        compiler_params=pltpu.CompilerParams(collective_id=1, has_side_effects=True, vmem_limit_bytes=40 * 1024 * 1024),
        name="give_back",
    )(inv, v)


def per_device(base, tangents):
    x = jnp.transpose(tangents, (1, 2, 0, 3))
    v, gram = evolved(base, x)
    inverse, factor_rows = factored(gram, 1.0 / (2.0 * NX * NY), 8)
    frames = returned(inverse, v)
    return (jnp.transpose(frames, (2, 0, 1, 3)), factor_rows)


def solution(mesh):
    split = Mesh(
        mesh.devices.reshape(mesh.shape["tan"], 4, 4, 2), ("tan", "grid_0", "grid_1", "grid_2")
    )
    placed = (P(None, GRID, None), P("tan", None, GRID, None))
    return jax.shard_map(
        per_device,
        mesh=split,
        in_specs=placed,
        out_specs=(P("tan", None, GRID, None), P("tan", None)),
        check_vma=False,
    )
```

```python
import functools
import jax
import jax.numpy as jnp
from jax import lax
from jax.experimental import pallas as pl
from jax.experimental.pallas import tpu as pltpu
from jax.sharding import Mesh
from jax.sharding import PartitionSpec as P

K = 512
NX = 256
NY = 256
GRID = ("grid_0", "grid_1", "grid_2")
HI = lax.Precision.HIGHEST

def factor_block(d, rows, width=16):
    lane = lax.broadcasted_iota(jnp.int32, (8, 128), 1)
    sub = lax.broadcasted_iota(jnp.int32, (8, 128), 0)
    wide = lambda x: jnp.broadcast_to(x, (8, 128))
    e = [jnp.where(lane == sub + 8 * i, 1.0, 0.0).astype(jnp.float32) for i in range(16)]
    for s in range(0, 128, width):
        t0 = s // 8
        c = [
            {i: wide(d[i][:, s + j : s + j + 1]) for i in range(t0 + j // 8, 16)}
            for j in range(width)
        ]
        for j in range(width):
            tj, sj = t0 + j // 8, j % 8
            r = lax.rsqrt(wide(c[j][tj][sj : sj + 1, :]))
            low = {i: c[j][i] * r for i in range(tj, 16)}
            for k in range(j + 1, width):
                tk, sk = t0 + k // 8, k % 8
                m = wide(low[tk][sk : sk + 1, :])
                for i in range(tk, 16):
                    c[k][i] = c[k][i] - low[i] * m
            row_d = wide(d[tj][sj : sj + 1, :]) * r
            row_e = wide(e[tj][sj : sj + 1, :]) * r
            rows(s + j, row_d[0:1], row_e[0:1])
            for i in range(tj, 16):
                d[i] = d[i] - low[i] * row_d
                e[i] = e[i] - low[i] * row_e


def dot(a, b, dims=((1,), (0,))):
    return lax.dot_general(a, b, (dims, ((), ())), precision=HI, preferred_element_type=jnp.float32)


def factor(width, scale, g_ref, inv_ref, fac_ref, a_ref, e_ref, u_ref, w_ref):
    block = 0
    for i in range(4):
        for j in range(i, 4):
            a_ref[i * 128 : i * 128 + 128, j * 128 : j * 128 + 128] = g_ref[block * 128 : block * 128 + 128] * scale
            block += 1
    e_ref[...] = jnp.zeros_like(e_ref)
    u_ref[...] = jnp.zeros_like(u_ref)
    inv_ref[...] = jnp.zeros_like(inv_ref)

    def step(k, carry):
        at = pl.multiple_of(k * 128, 128)
        d = [a_ref[pl.ds(pl.multiple_of(at + 8 * i, 8), 8), pl.ds(at, 128)] for i in range(16)]

        def rows(j, row_d, row_e):
            w_ref[j : j + 1, 0:128] = row_d
            w_ref[j : j + 1, 128:256] = row_e

        factor_block(d, rows, width)
        for kk in range(4):
            @pl.when(k == kk)
            def _():
                lo, hi = kk * 128, kk * 128 + 128
                upper = lax.broadcasted_iota(jnp.int32, (128, 128), 1) >= lax.broadcasted_iota(jnp.int32, (128, 128), 0)
                u_ref[lo:hi, lo:hi] = jnp.where(upper, w_ref[:, 0:128], 0.0)
                w = w_ref[:, 128:256]
                inv_ref[lo:hi, lo:hi] = w
                if kk:
                    inv_ref[lo:hi, 0:lo] = dot(w, e_ref[lo:hi, 0:lo])
                if kk < 3:
                    right = dot(w, a_ref[lo:hi, hi:512])
                    u_ref[lo:hi, hi:512] = right
                    left = right.T
                    a_ref[hi:512, hi:512] = a_ref[hi:512, hi:512] - dot(left, right)
                    e_ref[hi:512, 0:hi] = e_ref[hi:512, 0:hi] - dot(left, inv_ref[lo:hi, 0:hi])
        return carry

    lax.fori_loop(0, 4, step, 0)
    t = pl.multiple_of(lax.axis_index("tan") * 128, 128)
    fac_ref[...] = u_ref[:, pl.ds(t, 128)].T


spread_u, spread_v, feed_rate, kill_rate, step_size = 1.0, 0.5, 0.04, 0.06, 0.33
STAGES = (0.5 * step_size, 0.5 * step_size, step_size, step_size / 6.0) * 2

def base_coefficients(u, v, coef_ref):
    def lap(x):
        return (pltpu.roll(x, 1, 0) + pltpu.roll(x, 23, 0) + pltpu.roll(x, 1, 1) + pltpu.roll(x, NY - 1, 1) - 4.0 * x)

    def slopes(u, v):
        growth = u * v * v
        return (
            spread_u * lap(u) - growth + feed_rate * (1.0 - u),
            spread_v * lap(v) + growth - (feed_rate + kill_rate) * v,
        )

    for step in range(2):
        su, sv = u, v
        tu = tv = 0.0
        for stage in range(4):
            scale = STAGES[stage]
            square, cross = v2uv(su, sv)
            own = {0: 1.0, 1: 0.0, 2: 0.0, 3: 1.0 / 3.0}[stage]
            coef_ref[step * 4 + stage, 0] = own - scale * (4.0 * spread_u + feed_rate + square)
            coef_ref[step * 4 + stage, 1] = scale * cross
            coef_ref[step * 4 + stage, 2] = scale * square
            coef_ref[step * 4 + stage, 3] = own + scale * (cross - 4.0 * spread_v - feed_rate - kill_rate)
            if step == 1 and stage == 3:
                break
            ku, kv = slopes(su, sv)
            weight = (1.0, 2.0, 2.0, 1.0)[stage]
            tu, tv = tu + weight * ku, tv + weight * kv
            if stage < 3:
                ahead = (0.5, 0.5, 1.0)[stage] * step_size
                su, sv = u + ahead * ku, v + ahead * kv
        u, v = u + step_size / 6.0 * tu, v + step_size / 6.0 * tv


def v2uv(u, v):
    return v * v, 2.0 * u * v


def advance_group(get, put, coef_ref, z_refs, y_ref):
    first = get
    for stage in range(8):
        phase = stage % 4
        scale = STAGES[stage]
        out_lo, out_hi = stage + 1, 23 - stage
        src = {0: first, 1: reader(z_refs[0]), 2: reader(z_refs[1]), 3: reader(z_refs[2])}[phase]
        window = {}

        def at(row):
            if row not in window:
                window[row] = (src(0, row), src(1, row))
            return window[row]

        for row in range(out_lo, out_hi):
            up, mid, down = at(row - 1), at(row), at(row + 1)
            sums = [
                (up[f] + down[f]) + (pltpu.roll(mid[f], 1, 1) + pltpu.roll(mid[f], NY - 1, 1))
                for f in range(2)
            ]
            cp, bp, cq, aq = (coef_ref[stage, n, row : row + 1, :] for n in range(4))
            p = scale * spread_u * sums[0] + (cp * mid[0] - bp * mid[1])
            q = scale * spread_v * sums[1] + (cq * mid[0] + aq * mid[1])
            for f, new in ((0, p), (1, q)):
                if phase in (1, 2):
                    new = new + first(f, row)
                if phase == 3:
                    two = z_refs[1][f, row]
                    new = new + (1.0 / 3.0) * ((z_refs[0][f, row] - first(f, row)) + (two + two))
                if stage == 7:
                    put(f, row - 8, new)
                elif phase == 3:
                    y_ref[f, row] = new
                else:
                    z_refs[phase][f, row] = new
            del window[row - 1]
        if stage == 3:
            first = reader(y_ref)


def reader(ref):
    return lambda f, row: ref[f, row]


CHUNK = 16
CHUNKS = 128 // CHUNK
MESH_ID = pl.DeviceIdType.MESH


def place():
    return tuple(lax.axis_index(a) for a in ("tan",) + GRID)


def band_at(index):
    return {"grid_0": index // 8, "grid_1": index // 2 % 4, "grid_2": index % 2}


def along(core, turn, shift):
    x, z, y, _ = place()
    if turn == 2:
        return {"tan": (x + shift) % 4}, x
    on_y = 1 - core if turn == 0 else core
    spot = y * on_y + z * (1 - on_y)
    return {"grid_0": (z + shift * (1 - on_y)) % 4, "grid_1": (y + shift * on_y) % 4}, spot


def remote(source, target, send, receive, device):
    return pltpu.make_async_remote_copy(
        src_ref=source, dst_ref=target, send_sem=send, recv_sem=receive, device_id=device, device_id_type=MESH_ID
    )


def greet(devices):
    barrier = pltpu.get_barrier_semaphore()
    for device in devices:
        pl.semaphore_signal(barrier, inc=1, device_id=device, device_id_type=MESH_ID)
    pl.semaphore_wait(barrier, len(devices))


def sum_over_devices(part, acc, from_core, got_a, got_b, got_c, mid, low, total, sends, receives, then):
    x, z, y, core = place()
    other = {"grid_2": 1 - core}
    half = lambda c: pl.ds(pl.multiple_of(c * 640, 128), 640)
    copy = remote(part.at[half(1 - core)], from_core, sends.at[0], receives.at[0], other)
    copy.start()
    copy.wait()
    acc[...] = part[half(core)] + from_core[...]
    copies = []
    for k in (1, 3, 2):
        there, spot = along(core, 0, k)
        rows = pl.ds(pl.multiple_of((spot + k) % 4 * 160, 8), 160)
        copies.append(remote(acc.at[rows], got_a.at[k - 1], sends.at[k], receives.at[k], there))
        copies[-1].start()
    for copy in copies:
        copy.wait()
    spot_a = along(core, 0, 0)[1]
    mid[...] = (acc[pl.ds(pl.multiple_of(spot_a * 160, 8), 160)] + got_a[0]) + (got_a[1] + got_a[2])
    copies = []
    for k in (1, 3, 2):
        there, spot = along(core, 1, k)
        rows = pl.ds(pl.multiple_of((spot + k) % 4 * 40, 8), 40)
        copies.append(remote(mid.at[rows], got_b.at[k - 1], sends.at[3 + k], receives.at[3 + k], there))
        copies[-1].start()
    for copy in copies:
        copy.wait()
    spot_b = along(core, 1, 0)[1]
    low[...] = (mid[pl.ds(pl.multiple_of(spot_b * 40, 8), 40)] + got_b[0]) + (got_b[1] + got_b[2])
    copies = []
    for k in (1, 3, 2):
        there, spot_c = along(core, 2, k)
        copies.append(remote(low, got_c.at[spot_c], sends.at[6 + k], receives.at[6 + k], there))
        copies[-1].start()
    got_c[along(core, 2, 0)[1]] = low[...]
    for copy in copies:
        copy.wait()
    then()
    own_b = pl.ds(pl.multiple_of(spot_a * 160 + spot_b * 40 + core * 640, 8), 40)
    total[own_b] = (got_c[0] + got_c[1]) + (got_c[2] + got_c[3])
    copies = []
    for k in (1, 3, 2):
        there, _ = along(core, 1, k)
        copies.append(remote(total.at[own_b], total.at[own_b], sends.at[9 + k], receives.at[9 + k], there))
        copies[-1].start()
    for copy in copies:
        copy.wait()
    own_a = pl.ds(pl.multiple_of(spot_a * 160 + core * 640, 8), 160)
    copies = []
    for k in (1, 3, 2):
        there, _ = along(core, 0, k)
        copies.append(remote(total.at[own_a], total.at[own_a], sends.at[12 + k], receives.at[12 + k], there))
        copies[-1].start()
    for copy in copies:
        copy.wait()
    copy = remote(total.at[half(core)], total.at[half(core)], sends.at[16], receives.at[16], other)
    copy.start()
    copy.wait()


def packed_gram(v, part):
    block = 0
    for i in range(4):
        lo = i * 128
        total = None
        for f in range(2):
            for row in range(2):
                term = dot(v[f, row, lo : lo + 128, :], v[f, row, lo:K, :], ((1,), (1,)))
                total = term if total is None else total + term
        for j in range(i, 4):
            part[block * 128 : block * 128 + 128] = total[:, (j - i) * 128 : (j - i) * 128 + 128]
            block += 1


def whole_kernel(
    base_ref, x_ref, o_ref, fac_ref,
    base_above, base_below, top, bottom, out, v, part, acc, from_core, got_a, got_b, got_c, mid, low, total,
    coef_ref, z0, z1, z2, y_ref, a_ref, e_ref, u_ref, w_ref, inv, opposite, made, own,
    base_send, base_recv, halo_send, halo_recv, give_send, give_recv, sum_send, sum_recv,
    ahead_send, ahead_recv, back_send, back_recv, own_sem,
):
    x, z, y, core = place()
    band = (z * 4 + y) * 2 + core
    after, before = band_at((band + 1) % 32), band_at((band + 31) % 32)
    peers = [{"tan": (x + k) % 4} for k in (1, 2, 3)]
    greet(
        [after, before, {"grid_2": 1 - core}] + peers
        + [{"grid_1": (y + k) % 4} for k in (1, 2, 3)] + [{"grid_0": (z + k) % 4} for k in (1, 2, 3)]
    )
    bases = (
        remote(base_ref, base_above, base_send.at[0], base_recv.at[0], after),
        remote(base_ref, base_below, base_send.at[1], base_recv.at[1], before),
    )
    for copy in bases:
        copy.start()

    def halos(c):
        some = pl.ds(pl.multiple_of(c * CHUNK, CHUNK), CHUNK)
        return (
            remote(x_ref.at[:, :, some], top.at[:, :, some], halo_send.at[c, 0], halo_recv.at[c, 0], after),
            remote(x_ref.at[:, :, some], bottom.at[:, :, some], halo_send.at[c, 1], halo_recv.at[c, 1], before),
        )

    def gifts(c):
        some = pl.ds(pl.multiple_of(c * CHUNK, CHUNK), CHUNK)
        mine = pl.ds(pl.multiple_of(x * 128 + c * CHUNK, CHUNK), CHUNK)
        return [
            remote(
                out.at[:, pl.ds((x + k) % 4 * 2, 2), some], v.at[:, :, mine],
                give_send.at[c, k - 1], give_recv.at[c, k - 1], {"tan": (x + k) % 4},
            )
            for k in (1, 3, 2)
        ]

    def give(c):
        some = pl.ds(pl.multiple_of(c * CHUNK, CHUNK), CHUNK)
        mine = pl.ds(pl.multiple_of(x * 128 + c * CHUNK, CHUNK), CHUNK)
        v[:, :, mine] = out[:, pl.ds(x * 2, 2), some]
        for copy in gifts(c):
            copy.start()

    def start_halo(c, carry):
        for copy in halos(c):
            copy.start()
        return carry

    lax.fori_loop(0, CHUNKS, start_halo, 0)
    for copy in bases:
        copy.wait_recv()
    u, w = (jnp.concatenate([base_above[f], base_ref[f], base_below[f]], 0) for f in range(2))
    base_coefficients(u, w, coef_ref)

    def advance_chunk(c, carry):
        for copy in halos(c):
            copy.wait_recv()

        @pl.when(c > 0)
        def _():
            give(c - 1)

        def group(g, carry):
            eight = pl.ds(pl.multiple_of(c * CHUNK + g * 8, 8), 8)

            def get(f, row):
                ref = (top, x_ref, bottom)[row // 8]
                return ref[f, row % 8, eight, :]

            def put(f, row, value):
                out[f, row, eight, :] = value

            advance_group(get, put, coef_ref, (z0, z1, z2), y_ref)
            return carry

        return lax.fori_loop(0, CHUNK // 8, group, carry)

    lax.fori_loop(0, CHUNKS, advance_chunk, 0)
    give(CHUNKS - 1)

    def receive(c, carry):
        for copy in gifts(c):
            copy.wait_recv()
        return carry

    lax.fori_loop(0, CHUNKS, receive, 0)
    packed_gram(v, part)

    def ahead(k, chip):
        rows = pl.ds((chip + k + 2) % 4 * 2, 2)
        block = pl.ds(pl.multiple_of(chip * 128, 128), 128)
        return remote(
            out.at[:, rows], opposite.at[:, :, block], ahead_send.at[k - 1], ahead_recv.at[k - 1], {"tan": (chip + k) % 4}
        )

    def send_ahead():
        for k in (1, 2, 3):
            @pl.when(x + k < 4)
            def _():
                ahead(k, x).start()

    sum_over_devices(part, acc, from_core, got_a, got_b, got_c, mid, low, total, sum_send, sum_recv, send_ahead)
    factor(8, 1.0 / (2.0 * NX * NY), total, inv, fac_ref, a_ref, e_ref, u_ref, w_ref)

    pairs = [(f, row) for f in range(2) for row in range(2)]

    def back(n, k, f, row):
        return remote(
            made.at[n, f, row], o_ref.at[f, x * 2 + row],
            back_send.at[n, f * 2 + row], back_recv.at[n, f * 2 + row], {"tan": (x + k) % 4},
        )

    def frame(block, fields):
        return dot(inv[pl.ds(pl.multiple_of(block * 128, 128), 128), :], fields)

    for f, row in pairs:
        for n, k in ((0, 1), (1, 3)):
            @pl.when((x + k) % 4 != 0)
            def _():
                made[n, f, row] = frame((x + k) % 4, v[f, row])
                back(n, k, f, row).start()
    keeps = []

    def keep(n, chip, f, row, value):
        own[n, f, row] = value
        copy = pltpu.make_async_copy(own.at[n, f, row], o_ref.at[f, chip * 2 + row], own_sem.at[n, f * 2 + row])
        copy.start()
        return copy

    for f, row in pairs:
        keeps.append(keep(0, x, f, row, frame(x, v[f, row])))
    opposite[:, :, pl.ds(pl.multiple_of(x * 128, 128), 128)] = out[:, pl.ds((x + 2) % 4 * 2, 2)]
    for k in (1, 2, 3):
        @pl.when(x + k < 4)
        def _():
            opposite[:, :, pl.ds(pl.multiple_of((x + k) % 4 * 128, 128), 128)] = jnp.zeros((2, 2, 128, NY), jnp.float32)

        @pl.when(x >= k)
        def _():
            ahead(k, x - k).wait_recv()
    for f, row in pairs:
        keeps.append(keep(1, (x + 2) % 4, f, row, frame(x, opposite[f, row])))

    @pl.when(x == 0)
    def _():
        corner = inv[0:128, 0:128]
        copies = []
        for n, chip in ((2, 1), (3, 3)):
            for f, row in pairs:
                copies.append(keep(n, chip, f, row, dot(corner, out[f, chip * 2 + row])))
        for copy in copies:
            copy.wait()

    @pl.when(x != 0)
    def _():
        for f, row in pairs:
            for n, k in ((0, 1), (1, 3)):
                back(n, k, f, row).wait_recv()

    for f, row in pairs:
        for n, k in ((0, 1), (1, 3)):
            @pl.when((x + k) % 4 != 0)
            def _():
                back(n, k, f, row).wait_send()
    for k in (1, 2, 3):
        @pl.when(x + k < 4)
        def _():
            ahead(k, x).wait_send()

    def finish(c, carry):
        for copy in halos(c):
            copy.wait_send()
        for copy in gifts(c):
            copy.wait_send()
        return carry

    lax.fori_loop(0, CHUNKS, finish, 0)
    for copy in bases:
        copy.wait_send()
    for copy in keeps:
        copy.wait()


def whole(base, x):
    f32 = lambda *shape: pltpu.VMEM(shape, jnp.float32)
    sem = pltpu.SemaphoreType.DMA
    return pl.pallas_call(
        whole_kernel,
        out_shape=(jax.ShapeDtypeStruct((2, 8, 128, NY), jnp.float32), jax.ShapeDtypeStruct((128, K), jnp.float32)),
        in_specs=[pl.BlockSpec(memory_space=pltpu.VMEM)] * 2,
        out_specs=(pl.BlockSpec(memory_space=pl.ANY), pl.BlockSpec(memory_space=pltpu.VMEM)),
        scratch_shapes=[
            f32(2, 8, NY), f32(2, 8, NY), f32(2, 8, 128, NY), f32(2, 8, 128, NY), f32(2, 8, 128, NY), f32(2, 2, K, NY),
            f32(1280, 128), f32(640, 128), f32(640, 128), f32(3, 160, 128), f32(3, 40, 128), f32(4, 40, 128),
            f32(160, 128), f32(40, 128), f32(1280, 128),
            f32(8, 4, 24, NY), f32(2, 24, 8, NY), f32(2, 24, 8, NY), f32(2, 24, 8, NY), f32(2, 24, 8, NY),
            f32(K, K), f32(K, K), f32(K, K), f32(128, 256), f32(K, K), f32(2, 2, K, NY),
            f32(2, 2, 2, 128, NY), f32(4, 2, 2, 128, NY),
            sem((2,)), sem((2,)), sem((CHUNKS, 2)), sem((CHUNKS, 2)), sem((CHUNKS, 3)), sem((CHUNKS, 3)),
            sem((17,)), sem((17,)), sem((3,)), sem((3,)), sem((2, 4)), sem((2, 4)), sem((4, 4)),
        ],
        compiler_params=pltpu.CompilerParams(collective_id=0, has_side_effects=True, vmem_limit_bytes=48 * 1024 * 1024),
        name="whole",
    )(base, x)


def per_device(base, tangents):
    x = jnp.transpose(tangents, (1, 2, 0, 3))
    frames, factor_rows = whole(base, x)
    return (jnp.transpose(frames, (2, 0, 1, 3)), factor_rows)


def solution(mesh):
    split = Mesh(
        mesh.devices.reshape(mesh.shape["tan"], 4, 4, 2), ("tan", "grid_0", "grid_1", "grid_2")
    )
    placed = (P(None, GRID, None), P("tan", None, GRID, None))
    return jax.shard_map(
        per_device,
        mesh=split,
        in_specs=placed,
        out_specs=(P("tan", None, GRID, None), P("tan", None)),
        check_vma=False,
    )
```

```python
import functools
import jax
import jax.numpy as jnp
from jax import lax
from jax.experimental import pallas as pl
from jax.experimental.pallas import tpu as pltpu
from jax.sharding import Mesh
from jax.sharding import PartitionSpec as P

K = 512
NX = 256
NY = 256
GRID = ("grid_0", "grid_1", "grid_2")
HI = lax.Precision.HIGHEST

def factor_block(d, rows, width=16):
    lane = lax.broadcasted_iota(jnp.int32, (8, 128), 1)
    sub = lax.broadcasted_iota(jnp.int32, (8, 128), 0)
    wide = lambda x: jnp.broadcast_to(x, (8, 128))
    e = [jnp.where(lane == sub + 8 * i, 1.0, 0.0).astype(jnp.float32) for i in range(16)]
    for s in range(0, 128, width):
        t0 = s // 8
        c = [
            {i: wide(d[i][:, s + j : s + j + 1]) for i in range(t0 + j // 8, 16)}
            for j in range(width)
        ]
        for j in range(width):
            tj, sj = t0 + j // 8, j % 8
            r = lax.rsqrt(wide(c[j][tj][sj : sj + 1, :]))
            low = {i: c[j][i] * r for i in range(tj, 16)}
            for k in range(j + 1, width):
                tk, sk = t0 + k // 8, k % 8
                m = wide(low[tk][sk : sk + 1, :])
                for i in range(tk, 16):
                    c[k][i] = c[k][i] - low[i] * m
            row_d = wide(d[tj][sj : sj + 1, :]) * r
            row_e = wide(e[tj][sj : sj + 1, :]) * r
            rows(s + j, row_d[0:1], row_e[0:1])
            for i in range(tj, 16):
                d[i] = d[i] - low[i] * row_d
                e[i] = e[i] - low[i] * row_e


def dot(a, b, dims=((1,), (0,))):
    return lax.dot_general(a, b, (dims, ((), ())), precision=HI, preferred_element_type=jnp.float32)


def factor(width, scale, g_ref, inv_ref, fac_ref, a_ref, e_ref, u_ref, w_ref):
    block = 0
    for i in range(4):
        for j in range(i, 4):
            a_ref[i * 128 : i * 128 + 128, j * 128 : j * 128 + 128] = g_ref[block * 128 : block * 128 + 128] * scale
            block += 1
    e_ref[...] = jnp.zeros_like(e_ref)
    u_ref[...] = jnp.zeros_like(u_ref)
    inv_ref[...] = jnp.zeros_like(inv_ref)

    def step(k, carry):
        at = pl.multiple_of(k * 128, 128)
        d = [a_ref[pl.ds(pl.multiple_of(at + 8 * i, 8), 8), pl.ds(at, 128)] for i in range(16)]

        def rows(j, row_d, row_e):
            w_ref[j : j + 1, 0:128] = row_d
            w_ref[j : j + 1, 128:256] = row_e

        factor_block(d, rows, width)
        for kk in range(4):
            @pl.when(k == kk)
            def _():
                lo, hi = kk * 128, kk * 128 + 128
                upper = lax.broadcasted_iota(jnp.int32, (128, 128), 1) >= lax.broadcasted_iota(jnp.int32, (128, 128), 0)
                u_ref[lo:hi, lo:hi] = jnp.where(upper, w_ref[:, 0:128], 0.0)
                w = w_ref[:, 128:256]
                inv_ref[lo:hi, lo:hi] = w
                if kk:
                    inv_ref[lo:hi, 0:lo] = dot(w, e_ref[lo:hi, 0:lo])
                if kk < 3:
                    right = dot(w, a_ref[lo:hi, hi:512])
                    u_ref[lo:hi, hi:512] = right
                    left = right.T
                    a_ref[hi:512, hi:512] = a_ref[hi:512, hi:512] - dot(left, right)
                    e_ref[hi:512, 0:hi] = e_ref[hi:512, 0:hi] - dot(left, inv_ref[lo:hi, 0:hi])
        return carry

    lax.fori_loop(0, 4, step, 0)
    t = pl.multiple_of(lax.axis_index("tan") * 128, 128)
    fac_ref[...] = u_ref[:, pl.ds(t, 128)].T


spread_u, spread_v, feed_rate, kill_rate, step_size = 1.0, 0.5, 0.04, 0.06, 0.33
STAGES = (0.5 * step_size, 0.5 * step_size, step_size, step_size / 6.0) * 2

def base_coefficients(u, v, coef_ref):
    def lap(x):
        return (pltpu.roll(x, 1, 0) + pltpu.roll(x, 23, 0) + pltpu.roll(x, 1, 1) + pltpu.roll(x, NY - 1, 1) - 4.0 * x)

    def slopes(u, v):
        growth = u * v * v
        return (
            spread_u * lap(u) - growth + feed_rate * (1.0 - u),
            spread_v * lap(v) + growth - (feed_rate + kill_rate) * v,
        )

    for step in range(2):
        su, sv = u, v
        tu = tv = 0.0
        for stage in range(4):
            scale = STAGES[stage]
            square, cross = v2uv(su, sv)
            own = {0: 1.0, 1: 0.0, 2: 0.0, 3: 1.0 / 3.0}[stage]
            coef_ref[step * 4 + stage, 0] = own - scale * (4.0 * spread_u + feed_rate + square)
            coef_ref[step * 4 + stage, 1] = scale * cross
            coef_ref[step * 4 + stage, 2] = scale * square
            coef_ref[step * 4 + stage, 3] = own + scale * (cross - 4.0 * spread_v - feed_rate - kill_rate)
            if step == 1 and stage == 3:
                break
            ku, kv = slopes(su, sv)
            weight = (1.0, 2.0, 2.0, 1.0)[stage]
            tu, tv = tu + weight * ku, tv + weight * kv
            if stage < 3:
                ahead = (0.5, 0.5, 1.0)[stage] * step_size
                su, sv = u + ahead * ku, v + ahead * kv
        u, v = u + step_size / 6.0 * tu, v + step_size / 6.0 * tv


def v2uv(u, v):
    return v * v, 2.0 * u * v


def advance_group(get, put, coef_ref, z_refs, y_ref):
    first = get
    for stage in range(8):
        phase = stage % 4
        scale = STAGES[stage]
        out_lo, out_hi = stage + 1, 23 - stage
        src = {0: first, 1: reader(z_refs[0]), 2: reader(z_refs[1]), 3: reader(z_refs[2])}[phase]
        window = {}

        def at(row):
            if row not in window:
                window[row] = (src(0, row), src(1, row))
            return window[row]

        for row in range(out_lo, out_hi):
            up, mid, down = at(row - 1), at(row), at(row + 1)
            sums = [
                (up[f] + down[f]) + (pltpu.roll(mid[f], 1, 1) + pltpu.roll(mid[f], NY - 1, 1))
                for f in range(2)
            ]
            cp, bp, cq, aq = (coef_ref[stage, n, row : row + 1, :] for n in range(4))
            p = scale * spread_u * sums[0] + (cp * mid[0] - bp * mid[1])
            q = scale * spread_v * sums[1] + (cq * mid[0] + aq * mid[1])
            for f, new in ((0, p), (1, q)):
                if phase in (1, 2):
                    new = new + first(f, row)
                if phase == 3:
                    two = z_refs[1][f, row]
                    new = new + (1.0 / 3.0) * ((z_refs[0][f, row] - first(f, row)) + (two + two))
                if stage == 7:
                    put(f, row - 8, new)
                elif phase == 3:
                    y_ref[f, row] = new
                else:
                    z_refs[phase][f, row] = new
            del window[row - 1]
        if stage == 3:
            first = reader(y_ref)


def reader(ref):
    return lambda f, row: ref[f, row]


CHUNK = 8
CHUNKS = 128 // CHUNK
PACKED = [(i, j) for i in range(4) for j in range(i, 4)]
MESH_ID = pl.DeviceIdType.MESH


def place():
    return tuple(lax.axis_index(a) for a in ("tan",) + GRID)


def band_at(index):
    return {"grid_0": index // 8, "grid_1": index // 2 % 4, "grid_2": index % 2}


def along(core, turn, shift):
    x, z, y, _ = place()
    if turn == 2:
        return {"tan": (x + shift) % 4}, x
    on_y = 1 - core if turn == 0 else core
    spot = y * on_y + z * (1 - on_y)
    return {"grid_0": (z + shift * (1 - on_y)) % 4, "grid_1": (y + shift * on_y) % 4}, spot


def remote(source, target, send, receive, device):
    return pltpu.make_async_remote_copy(
        src_ref=source, dst_ref=target, send_sem=send, recv_sem=receive, device_id=device, device_id_type=MESH_ID
    )


def greet(devices):
    barrier = pltpu.get_barrier_semaphore()
    for device in devices:
        pl.semaphore_signal(barrier, inc=1, device_id=device, device_id_type=MESH_ID)
    pl.semaphore_wait(barrier, len(devices))


def sum_over_devices(part, acc, from_core, got_a, got_b, got_c, mid, low, total, sends, receives, then):
    x, z, y, core = place()
    other = {"grid_2": 1 - core}
    half = lambda c: pl.ds(pl.multiple_of(c * 640, 128), 640)
    copy = remote(part.at[half(1 - core)], from_core, sends.at[0], receives.at[0], other)
    copy.start()
    copy.wait()
    acc[...] = part[half(core)] + from_core[...]
    copies = []
    for k in (1, 3, 2):
        there, spot = along(core, 0, k)
        rows = pl.ds(pl.multiple_of((spot + k) % 4 * 160, 8), 160)
        copies.append(remote(acc.at[rows], got_a.at[k - 1], sends.at[k], receives.at[k], there))
        copies[-1].start()
    for copy in copies:
        copy.wait()
    spot_a = along(core, 0, 0)[1]
    mid[...] = (acc[pl.ds(pl.multiple_of(spot_a * 160, 8), 160)] + got_a[0]) + (got_a[1] + got_a[2])
    copies = []
    for k in (1, 3, 2):
        there, spot = along(core, 1, k)
        rows = pl.ds(pl.multiple_of((spot + k) % 4 * 40, 8), 40)
        copies.append(remote(mid.at[rows], got_b.at[k - 1], sends.at[3 + k], receives.at[3 + k], there))
        copies[-1].start()
    for copy in copies:
        copy.wait()
    spot_b = along(core, 1, 0)[1]
    low[...] = (mid[pl.ds(pl.multiple_of(spot_b * 40, 8), 40)] + got_b[0]) + (got_b[1] + got_b[2])
    copies = []
    for k in (1, 3, 2):
        there, spot_c = along(core, 2, k)
        copies.append(remote(low, got_c.at[spot_c], sends.at[6 + k], receives.at[6 + k], there))
        copies[-1].start()
    got_c[along(core, 2, 0)[1]] = low[...]
    for copy in copies:
        copy.wait()
    then()
    own_b = pl.ds(pl.multiple_of(spot_a * 160 + spot_b * 40 + core * 640, 8), 40)
    total[own_b] = (got_c[0] + got_c[1]) + (got_c[2] + got_c[3])
    copies = []
    for k in (1, 3, 2):
        there, _ = along(core, 1, k)
        copies.append(remote(total.at[own_b], total.at[own_b], sends.at[9 + k], receives.at[9 + k], there))
        copies[-1].start()
    for copy in copies:
        copy.wait()
    own_a = pl.ds(pl.multiple_of(spot_a * 160 + core * 640, 8), 160)
    copies = []
    for k in (1, 3, 2):
        there, _ = along(core, 0, k)
        copies.append(remote(total.at[own_a], total.at[own_a], sends.at[12 + k], receives.at[12 + k], there))
        copies[-1].start()
    for copy in copies:
        copy.wait()
    copy = remote(total.at[half(core)], total.at[half(core)], sends.at[16], receives.at[16], other)
    copy.start()
    copy.wait()


def packed_gram(v, part):
    for i in range(2):
        lo = i * 256
        total = None
        for f in range(2):
            for row in range(2):
                term = dot(v[f, row, lo : lo + 256, :], v[f, row, lo:K, :], ((1,), (1,)))
                total = term if total is None else total + term
        for a in range(2):
            for b in range(a, 4 - 2 * i):
                block = PACKED.index((2 * i + a, 2 * i + b))
                part[block * 128 : block * 128 + 128] = total[a * 128 : a * 128 + 128, b * 128 : b * 128 + 128]


def whole_kernel(
    base_ref, x_hbm, o_ref, fac_ref, x_ref,
    base_above, base_below, top, bottom, out, v, part, acc, from_core, got_a, got_b, got_c, mid, low, total,
    coef_ref, z0, z1, z2, y_ref, first, a_ref, e_ref, u_ref, w_ref, inv, turned, opposite, made, own,
    base_send, base_recv, halo_send, halo_recv, give_send, give_recv, sum_send, sum_recv,
    ahead_send, ahead_recv, back_send, back_recv, own_sem, load_sem,
):
    x, z, y, core = place()
    band = (z * 4 + y) * 2 + core
    after, before = band_at((band + 1) % 32), band_at((band + 31) % 32)
    peers = [{"tan": (x + k) % 4} for k in (1, 2, 3)]
    load = pltpu.make_async_copy(x_hbm, x_ref, load_sem)
    load.start()
    greet(
        [after, before, {"grid_2": 1 - core}] + peers
        + [{"grid_1": (y + k) % 4} for k in (1, 2, 3)] + [{"grid_0": (z + k) % 4} for k in (1, 2, 3)]
    )
    bases = (
        remote(base_ref, base_above, base_send.at[0], base_recv.at[0], after),
        remote(base_ref, base_below, base_send.at[1], base_recv.at[1], before),
    )
    for copy in bases:
        copy.start()

    def halos(c):
        some = pl.ds(pl.multiple_of(c * CHUNK, CHUNK), CHUNK)
        return (
            remote(x_ref.at[some], top.at[some], halo_send.at[c, 0], halo_recv.at[c, 0], after),
            remote(x_ref.at[some], bottom.at[some], halo_send.at[c, 1], halo_recv.at[c, 1], before),
        )

    def gifts(c):
        some = pl.ds(pl.multiple_of(c * CHUNK, CHUNK), CHUNK)
        mine = pl.ds(pl.multiple_of(x * 128 + c * CHUNK, CHUNK), CHUNK)
        return [
            remote(
                out.at[:, pl.ds((x + k) % 4 * 2, 2), some], v.at[:, :, mine],
                give_send.at[c, k - 1], give_recv.at[c, k - 1], {"tan": (x + k) % 4},
            )
            for k in (1, 3, 2)
        ]

    def give(c):
        some = pl.ds(pl.multiple_of(c * CHUNK, CHUNK), CHUNK)
        mine = pl.ds(pl.multiple_of(x * 128 + c * CHUNK, CHUNK), CHUNK)
        v[:, :, mine] = out[:, pl.ds(x * 2, 2), some]
        for copy in gifts(c):
            copy.start()

    def start_halo(c, carry):
        for copy in halos(c):
            copy.start()
        return carry

    load.wait()
    lax.fori_loop(0, CHUNKS, start_halo, 0)
    for copy in bases:
        copy.wait_recv()
    u, w = (jnp.concatenate([base_above[f], base_ref[f], base_below[f]], 0) for f in range(2))
    base_coefficients(u, w, coef_ref)

    def advance_chunk(c, carry):
        for copy in halos(c):
            copy.wait_recv()

        @pl.when(c > 0)
        def _():
            give(c - 1)

        def group(g, carry):
            eight = pl.ds(pl.multiple_of(c * CHUNK + g * 8, 8), 8)

            for n, ref in enumerate((top, x_ref, bottom)):
                for f in range(2):
                    first[f, n * 8 : n * 8 + 8] = jnp.swapaxes(ref[eight, f], 0, 1)

            def put(f, row, value):
                out[f, row, eight, :] = value

            advance_group(reader(first), put, coef_ref, (z0, z1, z2), y_ref)
            return carry

        return lax.fori_loop(0, CHUNK // 8, group, carry)

    lax.fori_loop(0, CHUNKS, advance_chunk, 0)
    give(CHUNKS - 1)

    def receive(c, carry):
        for copy in gifts(c):
            copy.wait_recv()
        return carry

    lax.fori_loop(0, CHUNKS, receive, 0)
    def ahead(k, chip):
        rows = pl.ds((chip + k + 2) % 4 * 2, 2)
        block = pl.ds(pl.multiple_of(chip * 128, 128), 128)
        return remote(
            out.at[:, rows], opposite.at[:, :, block], ahead_send.at[k - 1], ahead_recv.at[k - 1], {"tan": (chip + k) % 4}
        )

    def send_ahead(shifts):
        for k in shifts:
            @pl.when(x + k < 4)
            def _():
                ahead(k, x).start()

    send_ahead((1, 3))
    packed_gram(v, part)
    sum_over_devices(part, acc, from_core, got_a, got_b, got_c, mid, low, total, sum_send, sum_recv, lambda: send_ahead((2,)))
    factor(8, 1.0 / (2.0 * NX * NY), total, inv, fac_ref, a_ref, e_ref, u_ref, w_ref)

    pairs = [(f, row) for f in range(2) for row in range(2)]

    def back(n, k, f, row):
        return remote(
            made.at[n, f, row], o_ref.at[f, x * 2 + row],
            back_send.at[n, f * 2 + row], back_recv.at[n, f * 2 + row], {"tan": (x + k) % 4},
        )

    def rows_of(block):
        return inv[pl.ds(pl.multiple_of(block % 4 * 128, 128), 128), :]

    turned[...] = jnp.concatenate([rows_of(x + 1), rows_of(x + 3), rows_of(x)], 0)
    keeps = []

    def keep(n, chip, f, row, value):
        own[n, f, row] = value
        copy = pltpu.make_async_copy(own.at[n, f, row], o_ref.at[f, chip * 2 + row], own_sem.at[n, f * 2 + row])
        copy.start()
        return copy

    for f, row in pairs:
        frames = dot(turned[...], v[f, row])
        for n, k in ((0, 1), (1, 3)):
            made[n, f, row] = frames[n * 128 : n * 128 + 128]
            back(n, k, f, row).start()
        keeps.append(keep(0, x, f, row, frames[256:384]))
    opposite[:, :, pl.ds(pl.multiple_of(x * 128, 128), 128)] = out[:, pl.ds((x + 2) % 4 * 2, 2)]
    for k in (1, 2, 3):
        @pl.when(x + k < 4)
        def _():
            opposite[:, :, pl.ds(pl.multiple_of((x + k) % 4 * 128, 128), 128)] = jnp.zeros((2, 2, 128, NY), jnp.float32)

        @pl.when(x >= k)
        def _():
            ahead(k, x - k).wait_recv()
    for f, row in pairs:
        keeps.append(keep(1, (x + 2) % 4, f, row, dot(turned[256:384, :], opposite[f, row])))

    for f, row in pairs:
        for n, k in ((0, 1), (1, 3)):
            back(n, k, f, row).wait()
    for k in (1, 2, 3):
        @pl.when(x + k < 4)
        def _():
            ahead(k, x).wait_send()

    def finish(c, carry):
        for copy in halos(c):
            copy.wait_send()
        for copy in gifts(c):
            copy.wait_send()
        return carry

    lax.fori_loop(0, CHUNKS, finish, 0)
    for copy in bases:
        copy.wait_send()
    for copy in keeps:
        copy.wait()


def whole(base, x):
    f32 = lambda *shape: pltpu.VMEM(shape, jnp.float32)
    sem = pltpu.SemaphoreType.DMA
    return pl.pallas_call(
        whole_kernel,
        out_shape=(jax.ShapeDtypeStruct((2, 8, 128, NY), jnp.float32), jax.ShapeDtypeStruct((128, K), jnp.float32)),
        in_specs=[pl.BlockSpec(memory_space=pltpu.VMEM), pl.BlockSpec(memory_space=pl.ANY)],
        out_specs=(pl.BlockSpec(memory_space=pl.ANY), pl.BlockSpec(memory_space=pltpu.VMEM)),
        scratch_shapes=[
            f32(128, 2, 8, NY), f32(2, 8, NY), f32(2, 8, NY), f32(128, 2, 8, NY), f32(128, 2, 8, NY), f32(2, 8, 128, NY), f32(2, 2, K, NY),
            f32(1280, 128), f32(640, 128), f32(640, 128), f32(3, 160, 128), f32(3, 40, 128), f32(4, 40, 128),
            f32(160, 128), f32(40, 128), f32(1280, 128),
            f32(8, 4, 24, NY), f32(2, 24, 8, NY), f32(2, 24, 8, NY), f32(2, 24, 8, NY), f32(2, 24, 8, NY), f32(2, 24, 8, NY),
            f32(K, K), f32(K, K), f32(K, K), f32(128, 256), f32(K, K), f32(384, K), f32(2, 2, K, NY),
            f32(2, 2, 2, 128, NY), f32(2, 2, 2, 128, NY),
            sem((2,)), sem((2,)), sem((CHUNKS, 2)), sem((CHUNKS, 2)), sem((CHUNKS, 3)), sem((CHUNKS, 3)),
            sem((17,)), sem((17,)), sem((3,)), sem((3,)), sem((2, 4)), sem((2, 4)), sem((2, 4)), sem(()),
        ],
        compiler_params=pltpu.CompilerParams(collective_id=0, has_side_effects=True, vmem_limit_bytes=48 * 1024 * 1024),
        name="whole",
    )(base, x)


def per_device(base, tangents):
    frames, factor_rows = whole(base, tangents)
    return (jnp.transpose(frames, (2, 0, 1, 3)), factor_rows)


def solution(mesh):
    split = Mesh(
        mesh.devices.reshape(mesh.shape["tan"], 4, 4, 2), ("tan", "grid_0", "grid_1", "grid_2")
    )
    placed = (P(None, GRID, None), P("tan", None, GRID, None))
    return jax.shard_map(
        per_device,
        mesh=split,
        in_specs=placed,
        out_specs=(P("tan", None, GRID, None), P("tan", None)),
        check_vma=False,
    )
```

```python
import functools
import jax
import jax.numpy as jnp
from jax import lax
from jax.experimental import pallas as pl
from jax.experimental.pallas import tpu as pltpu
from jax.sharding import Mesh
from jax.sharding import PartitionSpec as P

K = 512
NX = 256
NY = 256
GRID = ("grid_0", "grid_1", "grid_2")
HI = lax.Precision.HIGHEST

def factor_block(d, rows, width=16):
    lane = lax.broadcasted_iota(jnp.int32, (8, 128), 1)
    sub = lax.broadcasted_iota(jnp.int32, (8, 128), 0)
    wide = lambda x: jnp.broadcast_to(x, (8, 128))
    e = [jnp.where(lane == sub + 8 * i, 1.0, 0.0).astype(jnp.float32) for i in range(16)]
    for s in range(0, 128, width):
        t0 = s // 8
        c = [
            {i: wide(d[i][:, s + j : s + j + 1]) for i in range(t0 + j // 8, 16)}
            for j in range(width)
        ]
        for j in range(width):
            tj, sj = t0 + j // 8, j % 8
            r = lax.rsqrt(wide(c[j][tj][sj : sj + 1, :]))
            low = {i: c[j][i] * r for i in range(tj, 16)}
            for k in range(j + 1, width):
                tk, sk = t0 + k // 8, k % 8
                m = wide(low[tk][sk : sk + 1, :])
                for i in range(tk, 16):
                    c[k][i] = c[k][i] - low[i] * m
            row_d = wide(d[tj][sj : sj + 1, :]) * r
            row_e = wide(e[tj][sj : sj + 1, :]) * r
            rows(s + j, row_d[0:1], row_e[0:1])
            for i in range(tj, 16):
                d[i] = d[i] - low[i] * row_d
                e[i] = e[i] - low[i] * row_e


def dot(a, b, dims=((1,), (0,))):
    return lax.dot_general(a, b, (dims, ((), ())), precision=HI, preferred_element_type=jnp.float32)


def factor(width, scale, g_ref, inv_ref, fac_ref, a_ref, e_ref, u_ref, w_ref):
    block = 0
    for i in range(4):
        for j in range(i, 4):
            for h in range(2):
                at, to = h * 640 + block * 64, i * 128 + h * 64
                a_ref[to : to + 64, j * 128 : j * 128 + 128] = g_ref[at : at + 64] * scale
            block += 1
    e_ref[...] = jnp.zeros_like(e_ref)
    u_ref[...] = jnp.zeros_like(u_ref)
    inv_ref[...] = jnp.zeros_like(inv_ref)

    def step(k, carry):
        at = pl.multiple_of(k * 128, 128)
        d = [a_ref[pl.ds(pl.multiple_of(at + 8 * i, 8), 8), pl.ds(at, 128)] for i in range(16)]

        def rows(j, row_d, row_e):
            w_ref[j : j + 1, 0:128] = row_d
            w_ref[j : j + 1, 128:256] = row_e

        factor_block(d, rows, width)
        for kk in range(4):
            @pl.when(k == kk)
            def _():
                lo, hi = kk * 128, kk * 128 + 128
                upper = lax.broadcasted_iota(jnp.int32, (128, 128), 1) >= lax.broadcasted_iota(jnp.int32, (128, 128), 0)
                u_ref[lo:hi, lo:hi] = jnp.where(upper, w_ref[:, 0:128], 0.0)
                w = w_ref[:, 128:256]
                inv_ref[lo:hi, lo:hi] = w
                if kk:
                    inv_ref[lo:hi, 0:lo] = dot(w, e_ref[lo:hi, 0:lo])
                if kk < 3:
                    right = dot(w, a_ref[lo:hi, hi:512])
                    u_ref[lo:hi, hi:512] = right
                    left = right.T
                    a_ref[hi:512, hi:512] = a_ref[hi:512, hi:512] - dot(left, right)
                    e_ref[hi:512, 0:hi] = e_ref[hi:512, 0:hi] - dot(left, inv_ref[lo:hi, 0:hi])
        return carry

    lax.fori_loop(0, 4, step, 0)
    t = pl.multiple_of(lax.axis_index("tan") * 128, 128)
    fac_ref[...] = u_ref[:, pl.ds(t, 128)].T


spread_u, spread_v, feed_rate, kill_rate, step_size = 1.0, 0.5, 0.04, 0.06, 0.33
STAGES = (0.5 * step_size, 0.5 * step_size, step_size, step_size / 6.0) * 2

def base_coefficients(u, v, coef_ref):
    def lap(x):
        return (pltpu.roll(x, 1, 0) + pltpu.roll(x, 23, 0) + pltpu.roll(x, 1, 1) + pltpu.roll(x, NY - 1, 1) - 4.0 * x)

    def slopes(u, v):
        growth = u * v * v
        return (
            spread_u * lap(u) - growth + feed_rate * (1.0 - u),
            spread_v * lap(v) + growth - (feed_rate + kill_rate) * v,
        )

    for step in range(2):
        su, sv = u, v
        tu = tv = 0.0
        for stage in range(4):
            scale = STAGES[stage]
            square, cross = v2uv(su, sv)
            own = {0: 1.0, 1: 0.0, 2: 0.0, 3: 1.0 / 3.0}[stage]
            coef_ref[step * 4 + stage, 0] = own - scale * (4.0 * spread_u + feed_rate + square)
            coef_ref[step * 4 + stage, 1] = scale * cross
            coef_ref[step * 4 + stage, 2] = scale * square
            coef_ref[step * 4 + stage, 3] = own + scale * (cross - 4.0 * spread_v - feed_rate - kill_rate)
            if step == 1 and stage == 3:
                break
            ku, kv = slopes(su, sv)
            weight = (1.0, 2.0, 2.0, 1.0)[stage]
            tu, tv = tu + weight * ku, tv + weight * kv
            if stage < 3:
                ahead = (0.5, 0.5, 1.0)[stage] * step_size
                su, sv = u + ahead * ku, v + ahead * kv
        u, v = u + step_size / 6.0 * tu, v + step_size / 6.0 * tv


def v2uv(u, v):
    return v * v, 2.0 * u * v


def advance_group(get, put, coef_ref, z_refs, y_ref):
    first = get
    for stage in range(8):
        phase = stage % 4
        scale = STAGES[stage]
        out_lo, out_hi = stage + 1, 23 - stage
        src = {0: first, 1: reader(z_refs[0]), 2: reader(z_refs[1]), 3: reader(z_refs[2])}[phase]
        window = {}

        def at(row):
            if row not in window:
                window[row] = (src(0, row), src(1, row))
            return window[row]

        for row in range(out_lo, out_hi):
            up, mid, down = at(row - 1), at(row), at(row + 1)
            sums = [
                (up[f] + down[f]) + (pltpu.roll(mid[f], 1, 1) + pltpu.roll(mid[f], NY - 1, 1))
                for f in range(2)
            ]
            cp, bp, cq, aq = (coef_ref[stage, n, row : row + 1, :] for n in range(4))
            p = scale * spread_u * sums[0] + (cp * mid[0] - bp * mid[1])
            q = scale * spread_v * sums[1] + (cq * mid[0] + aq * mid[1])
            for f, new in ((0, p), (1, q)):
                if phase in (1, 2):
                    new = new + first(f, row)
                if phase == 3:
                    two = z_refs[1][f, row]
                    new = new + (1.0 / 3.0) * ((z_refs[0][f, row] - first(f, row)) + (two + two))
                if stage == 7:
                    put(f, row - 8, new)
                elif phase == 3:
                    y_ref[f, row] = new
                else:
                    z_refs[phase][f, row] = new
            del window[row - 1]
        if stage == 3:
            first = reader(y_ref)


def reader(ref):
    return lambda f, row: ref[f, row]


CHUNK = 8
CHUNKS = 128 // CHUNK
PACKED = [(i, j) for i in range(4) for j in range(i, 4)]
MESH_ID = pl.DeviceIdType.MESH


def place():
    return tuple(lax.axis_index(a) for a in ("tan",) + GRID)


def band_at(index):
    return {"grid_0": index // 8, "grid_1": index // 2 % 4, "grid_2": index % 2}


def along(core, turn, shift):
    x, z, y, _ = place()
    if turn == 2:
        return {"tan": (x + shift) % 4}, x
    on_y = 1 - core if turn == 0 else core
    spot = y * on_y + z * (1 - on_y)
    return {"grid_0": (z + shift * (1 - on_y)) % 4, "grid_1": (y + shift * on_y) % 4}, spot


def remote(source, target, send, receive, device):
    return pltpu.make_async_remote_copy(
        src_ref=source, dst_ref=target, send_sem=send, recv_sem=receive, device_id=device, device_id_type=MESH_ID
    )


def greet(devices):
    barrier = pltpu.get_barrier_semaphore()
    for device in devices:
        pl.semaphore_signal(barrier, inc=1, device_id=device, device_id_type=MESH_ID)
    pl.semaphore_wait(barrier, len(devices))


def packed_gram(i, v, part):
    lo = i * 256
    total = None
    for f in range(2):
        for row in range(2):
            term = dot(v[f, row, lo : lo + 256, :], v[f, row, lo:K, :], ((1,), (1,)))
            total = term if total is None else total + term
    for a in range(2):
        for b in range(a, 4 - 2 * i):
            block = PACKED.index((2 * i + a, 2 * i + b))
            for h in range(2):
                to, at = h * 640 + block * 64, a * 128 + h * 64
                part[to : to + 64] = total[at : at + 64, b * 128 : b * 128 + 128]


def sum_over_devices(v, part, acc, from_core, got_a, got_b, got_c, mid, low, total, sends, receives, then):
    core = place()[3]
    other = {"grid_2": 1 - core}

    def swap(n):
        lo, count = ((0, 224), (224, 224), (448, 192))[n]
        away = pl.ds(pl.multiple_of((1 - core) * 640 + lo, 32), count)
        return remote(part.at[away], from_core.at[lo : lo + count], sends.at[n], receives.at[n], other)

    packed_gram(0, v, part)
    swap(0).start()
    swap(1).start()
    packed_gram(1, v, part)
    swap(2).start()
    for n in range(3):
        swap(n).wait()
    acc[...] = part[pl.ds(pl.multiple_of(core * 640, 128), 640)] + from_core[...]
    copies = []
    for k in (2, 1, 3):
        there, spot = along(core, 0, k)
        rows = pl.ds(pl.multiple_of((spot + k) % 4 * 160, 8), 160)
        copies.append(remote(acc.at[rows], got_a.at[k - 1], sends.at[2 + k], receives.at[2 + k], there))
        copies[-1].start()
    for copy in copies:
        copy.wait()
    spot_a = along(core, 0, 0)[1]
    mid[...] = (acc[pl.ds(pl.multiple_of(spot_a * 160, 8), 160)] + got_a[0]) + (got_a[1] + got_a[2])
    copies = []
    for k in (2, 1, 3):
        there, spot = along(core, 1, k)
        rows = pl.ds(pl.multiple_of((spot + k) % 4 * 40, 8), 40)
        copies.append(remote(mid.at[rows], got_b.at[k - 1], sends.at[5 + k], receives.at[5 + k], there))
        copies[-1].start()
    for copy in copies:
        copy.wait()
    spot_b = along(core, 1, 0)[1]
    low[...] = (mid[pl.ds(pl.multiple_of(spot_b * 40, 8), 40)] + got_b[0]) + (got_b[1] + got_b[2])
    copies = []
    for k in (2, 1, 3):
        there, spot_c = along(core, 2, k)
        copies.append(remote(low, got_c.at[spot_c], sends.at[8 + k], receives.at[8 + k], there))
        copies[-1].start()
    got_c[along(core, 2, 0)[1]] = low[...]
    for copy in copies:
        copy.wait()

    def piece(of_core, a, b):
        return total.at[pl.ds(pl.multiple_of(of_core * 640 + a % 4 * 160 + b % 4 * 40, 8), 40)]

    def to_b(k):
        mine = piece(core, spot_a, spot_b)
        return remote(mine, mine, sends.at[11 + k], receives.at[11 + k], along(core, 1, k)[0])

    def to_a(k, kb):
        held = piece(core, spot_a, spot_b + 4 - kb)
        return remote(held, held, sends.at[15 + (k - 1) * 4 + kb], receives.at[15 + (k - 1) * 4 + kb], along(core, 0, k)[0])

    def to_core(ka, kb):
        held = piece(core, spot_a + 4 - ka, spot_b + 4 - kb)
        return remote(held, held, sends.at[27 + ka * 4 + kb], receives.at[27 + ka * 4 + kb], other)

    total[pl.ds(pl.multiple_of(spot_a * 160 + spot_b * 40 + core * 640, 8), 40)] = (got_c[0] + got_c[1]) + (got_c[2] + got_c[3])
    for k in (2, 1, 3):
        to_b(k).start()
    for k in (2, 1, 3):
        to_a(k, 0).start()
    to_core(0, 0).start()
    then()
    for kb in (1, 3, 2):
        to_b(kb).wait_recv()
        for k in (2, 1, 3):
            to_a(k, kb).start()
        to_core(0, kb).start()
    for kb in (0, 1, 3, 2):
        for ka in (1, 3, 2):
            to_a(ka, kb).wait_recv()
            to_core(ka, kb).start()
    for kb in range(4):
        for ka in range(4):
            to_core(ka, kb).wait_recv()
    for k in (1, 2, 3):
        to_b(k).wait_send()
        for kb in range(4):
            to_a(k, kb).wait_send()
    for kb in range(4):
        for ka in range(4):
            to_core(ka, kb).wait_send()


def whole_kernel(
    base_hbm, x_hbm, o_ref, fac_ref, base_ref, x_ref,
    base_above, base_below, top, bottom, out, v, part, acc, from_core, got_a, got_b, got_c, mid, low, total,
    coef_ref, z0, z1, z2, y_ref, first, a_ref, e_ref, u_ref, w_ref, inv, turned, opposite, made, own,
    base_send, base_recv, halo_send, halo_recv, give_send, give_recv, sum_send, sum_recv,
    ahead_send, ahead_recv, back_send, back_recv, own_sem, load_sem,
):
    x, z, y, core = place()
    band = (z * 4 + y) * 2 + core
    after, before = band_at((band + 1) % 32), band_at((band + 31) % 32)
    peers = [{"tan": (x + k) % 4} for k in (1, 2, 3)]
    load = pltpu.make_async_copy(x_hbm, x_ref, load_sem.at[0])
    load_base = pltpu.make_async_copy(base_hbm, base_ref, load_sem.at[1])
    load_base.start()
    load.start()
    greet(
        [after, before, {"grid_2": 1 - core}] + peers
        + [{"grid_1": (y + k) % 4} for k in (1, 2, 3)] + [{"grid_0": (z + k) % 4} for k in (1, 2, 3)]
    )
    bases = (
        remote(base_ref, base_above, base_send.at[0], base_recv.at[0], after),
        remote(base_ref, base_below, base_send.at[1], base_recv.at[1], before),
    )
    load_base.wait()
    for copy in bases:
        copy.start()

    def halos(c):
        some = pl.ds(pl.multiple_of(c * CHUNK, CHUNK), CHUNK)
        return (
            remote(x_ref.at[some], top.at[some], halo_send.at[c, 0], halo_recv.at[c, 0], after),
            remote(x_ref.at[some], bottom.at[some], halo_send.at[c, 1], halo_recv.at[c, 1], before),
        )

    def gifts(c):
        some = pl.ds(pl.multiple_of(c * CHUNK, CHUNK), CHUNK)
        mine = pl.ds(pl.multiple_of(x * 128 + c * CHUNK, CHUNK), CHUNK)
        return [
            remote(
                out.at[:, pl.ds((x + k) % 4 * 2, 2), some], v.at[:, :, mine],
                give_send.at[c, k - 1], give_recv.at[c, k - 1], {"tan": (x + k) % 4},
            )
            for k in (1, 3, 2)
        ]

    def give(c):
        some = pl.ds(pl.multiple_of(c * CHUNK, CHUNK), CHUNK)
        mine = pl.ds(pl.multiple_of(x * 128 + c * CHUNK, CHUNK), CHUNK)
        v[:, :, mine] = out[:, pl.ds(x * 2, 2), some]
        for copy in gifts(c):
            copy.start()

    def start_halo(c, carry):
        for copy in halos(c):
            copy.start()
        return carry

    load.wait()
    lax.fori_loop(0, CHUNKS, start_halo, 0)
    for copy in bases:
        copy.wait_recv()
    u, w = (jnp.concatenate([base_above[f], base_ref[f], base_below[f]], 0) for f in range(2))
    base_coefficients(u, w, coef_ref)

    def advance_chunk(c, carry):
        for copy in halos(c):
            copy.wait_recv()

        @pl.when(c > 0)
        def _():
            give(c - 1)

        def group(g, carry):
            eight = pl.ds(pl.multiple_of(c * CHUNK + g * 8, 8), 8)

            for n, ref in enumerate((top, x_ref, bottom)):
                for f in range(2):
                    first[f, n * 8 : n * 8 + 8] = jnp.swapaxes(ref[eight, f], 0, 1)

            def put(f, row, value):
                out[f, row, eight, :] = value

            advance_group(reader(first), put, coef_ref, (z0, z1, z2), y_ref)
            return carry

        return lax.fori_loop(0, CHUNK // 8, group, carry)

    lax.fori_loop(0, CHUNKS, advance_chunk, 0)
    give(CHUNKS - 1)

    def receive(c, carry):
        for copy in gifts(c):
            copy.wait_recv()
        return carry

    lax.fori_loop(0, CHUNKS, receive, 0)
    def ahead(k, chip):
        rows = pl.ds((chip + k + 2) % 4 * 2, 2)
        block = pl.ds(pl.multiple_of(chip * 128, 128), 128)
        return remote(
            out.at[:, rows], opposite.at[:, :, block], ahead_send.at[k - 1], ahead_recv.at[k - 1], {"tan": (chip + k) % 4}
        )

    def send_ahead(shifts):
        for k in shifts:
            @pl.when(x + k < 4)
            def _():
                ahead(k, x).start()

    send_ahead((1, 3))
    sum_over_devices(v, part, acc, from_core, got_a, got_b, got_c, mid, low, total, sum_send, sum_recv, lambda: send_ahead((2,)))
    factor(8, 1.0 / (2.0 * NX * NY), total, inv, fac_ref, a_ref, e_ref, u_ref, w_ref)

    pairs = [(f, row) for f in range(2) for row in range(2)]

    def back(n, k, f, row):
        return remote(
            made.at[n, f, row], o_ref.at[f, x * 2 + row],
            back_send.at[n, f * 2 + row], back_recv.at[n, f * 2 + row], {"tan": (x + k) % 4},
        )

    def rows_of(block):
        return inv[pl.ds(pl.multiple_of(block % 4 * 128, 128), 128), :]

    turned[...] = jnp.concatenate([rows_of(x + 1), rows_of(x + 3), rows_of(x)], 0)
    keeps = []

    def keep(n, chip, f, row, value):
        own[n, f, row] = value
        copy = pltpu.make_async_copy(own.at[n, f, row], o_ref.at[f, chip * 2 + row], own_sem.at[n, f * 2 + row])
        copy.start()
        return copy

    for f, row in pairs:
        frames = dot(turned[...], v[f, row])
        for n, k in ((0, 1), (1, 3)):
            made[n, f, row] = frames[n * 128 : n * 128 + 128]
            back(n, k, f, row).start()
        keeps.append(keep(0, x, f, row, frames[256:384]))
    opposite[:, :, pl.ds(pl.multiple_of(x * 128, 128), 128)] = out[:, pl.ds((x + 2) % 4 * 2, 2)]
    for k in (1, 2, 3):
        @pl.when(x + k < 4)
        def _():
            opposite[:, :, pl.ds(pl.multiple_of((x + k) % 4 * 128, 128), 128)] = jnp.zeros((2, 2, 128, NY), jnp.float32)

        @pl.when(x >= k)
        def _():
            ahead(k, x - k).wait_recv()
    for f, row in pairs:
        keeps.append(keep(1, (x + 2) % 4, f, row, dot(turned[256:384, :], opposite[f, row])))

    for f, row in pairs:
        for n, k in ((0, 1), (1, 3)):
            back(n, k, f, row).wait()
    for k in (1, 2, 3):
        @pl.when(x + k < 4)
        def _():
            ahead(k, x).wait_send()

    def finish(c, carry):
        for copy in halos(c):
            copy.wait_send()
        for copy in gifts(c):
            copy.wait_send()
        return carry

    lax.fori_loop(0, CHUNKS, finish, 0)
    for copy in bases:
        copy.wait_send()
    for copy in keeps:
        copy.wait()


def whole(base, x):
    f32 = lambda *shape: pltpu.VMEM(shape, jnp.float32)
    sem = pltpu.SemaphoreType.DMA
    return pl.pallas_call(
        whole_kernel,
        out_shape=(jax.ShapeDtypeStruct((2, 8, 128, NY), jnp.float32), jax.ShapeDtypeStruct((128, K), jnp.float32)),
        in_specs=[pl.BlockSpec(memory_space=pl.ANY)] * 2,
        out_specs=(pl.BlockSpec(memory_space=pl.ANY), pl.BlockSpec(memory_space=pltpu.VMEM)),
        scratch_shapes=[
            f32(2, 8, NY), f32(128, 2, 8, NY), f32(2, 8, NY), f32(2, 8, NY), f32(128, 2, 8, NY), f32(128, 2, 8, NY), f32(2, 8, 128, NY), f32(2, 2, K, NY),
            f32(1280, 128), f32(640, 128), f32(640, 128), f32(3, 160, 128), f32(3, 40, 128), f32(4, 40, 128),
            f32(160, 128), f32(40, 128), f32(1280, 128),
            f32(8, 4, 24, NY), f32(2, 24, 8, NY), f32(2, 24, 8, NY), f32(2, 24, 8, NY), f32(2, 24, 8, NY), f32(2, 24, 8, NY),
            f32(K, K), f32(K, K), f32(K, K), f32(128, 256), f32(K, K), f32(384, K), f32(2, 2, K, NY),
            f32(2, 2, 2, 128, NY), f32(2, 2, 2, 128, NY),
            sem((2,)), sem((2,)), sem((CHUNKS, 2)), sem((CHUNKS, 2)), sem((CHUNKS, 3)), sem((CHUNKS, 3)),
            sem((43,)), sem((43,)), sem((3,)), sem((3,)), sem((2, 4)), sem((2, 4)), sem((2, 4)), sem((2,)),
        ],
        compiler_params=pltpu.CompilerParams(collective_id=0, has_side_effects=True, vmem_limit_bytes=67043328),
        name="whole",
    )(base, x)


def per_device(base, tangents):
    frames, factor_rows = whole(base, tangents)
    return (jnp.transpose(frames, (2, 0, 1, 3)), factor_rows)


def solution(mesh):
    split = Mesh(
        mesh.devices.reshape(mesh.shape["tan"], 4, 4, 2), ("tan", "grid_0", "grid_1", "grid_2")
    )
    placed = (P(None, GRID, None), P("tan", None, GRID, None))
    return jax.shard_map(
        per_device,
        mesh=split,
        in_specs=placed,
        out_specs=(P("tan", None, GRID, None), P("tan", None)),
        check_vma=False,
    )
```

```python
import functools
import jax
import jax.numpy as jnp
from jax import lax
from jax.experimental import pallas as pl
from jax.experimental.pallas import tpu as pltpu
from jax.sharding import Mesh
from jax.sharding import PartitionSpec as P

K = 512
NX = 256
NY = 256
GRID = ("grid_0", "grid_1", "grid_2")
HI = lax.Precision.HIGHEST

def factor_block(d, rows):
    lane = lax.broadcasted_iota(jnp.int32, (8, 128), 1)
    sub = lax.broadcasted_iota(jnp.int32, (8, 128), 0)
    wide = lambda x: jnp.broadcast_to(x, (8, 128))
    e = [jnp.where(lane == sub + 8 * i, 1.0, 0.0).astype(jnp.float32) for i in range(16)]
    head = [wide(d[0][:, j : j + 1]) for j in range(8)]
    for t in range(16):
        s = t * 8
        column = [{i: wide(d[i][:, s + j : s + j + 1]) for i in range(t + 1, 16)} for j in range(8)]
        ahead = [wide(d[t + 1][:, s + 8 + j : s + 9 + j]) for j in range(8)] if t < 15 else None
        for j in range(8):
            r = lax.rsqrt(wide(head[j][j : j + 1, :]))
            top = head[j] * r
            pivots = {k: wide(top[k : k + 1, :]) for k in range(j + 1, 8)}
            for k in range(j + 1, 8):
                head[k] = head[k] - top * pivots[k]
            row_d = wide(d[t][j : j + 1, :]) * r
            row_e = wide(e[t][j : j + 1, :]) * r
            rows(s + j, row_d[0:1], row_e[0:1])
            if j < 7:
                d[t] = d[t] - top * row_d
                e[t] = e[t] - top * row_e
            for i in range(t + 1, 16):
                low = column[j][i] * r
                if i == t + 1:
                    for k in range(8):
                        ahead[k] = ahead[k] - low * wide(low[k : k + 1, :])
                for k in range(j + 1, 8):
                    column[k][i] = column[k][i] - low * pivots[k]
                d[i] = d[i] - low * row_d
                e[i] = e[i] - low * row_e
        head = ahead


def dot(a, b, dims=((1,), (0,))):
    return lax.dot_general(a, b, (dims, ((), ())), precision=HI, preferred_element_type=jnp.float32)


def factor(scale, g_ref, inv_ref, fac_ref, a_ref, e_ref, u_ref, w_ref):
    block = 0
    for i in range(4):
        for j in range(i, 4):
            for h in range(2):
                at, to = h * 640 + block * 64, i * 128 + h * 64
                a_ref[to : to + 64, j * 128 : j * 128 + 128] = g_ref[at : at + 64] * scale
            block += 1
    e_ref[...] = jnp.zeros_like(e_ref)
    u_ref[...] = jnp.zeros_like(u_ref)
    inv_ref[...] = jnp.zeros_like(inv_ref)

    def step(k, carry):
        at = pl.multiple_of(k * 128, 128)
        d = [a_ref[pl.ds(pl.multiple_of(at + 8 * i, 8), 8), pl.ds(at, 128)] for i in range(16)]

        def rows(j, row_d, row_e):
            w_ref[j : j + 1, 0:128] = row_d
            w_ref[j : j + 1, 128:256] = row_e

        factor_block(d, rows)
        for kk in range(4):
            @pl.when(k == kk)
            def _():
                lo, hi = kk * 128, kk * 128 + 128
                upper = lax.broadcasted_iota(jnp.int32, (128, 128), 1) >= lax.broadcasted_iota(jnp.int32, (128, 128), 0)
                u_ref[lo:hi, lo:hi] = jnp.where(upper, w_ref[:, 0:128], 0.0)
                w = w_ref[:, 128:256]
                inv_ref[lo:hi, lo:hi] = w
                if kk:
                    inv_ref[lo:hi, 0:lo] = dot(w, e_ref[lo:hi, 0:lo])
                if kk < 3:
                    right = dot(w, a_ref[lo:hi, hi:512])
                    u_ref[lo:hi, hi:512] = right
                    left = right.T
                    a_ref[hi:512, hi:512] = a_ref[hi:512, hi:512] - dot(left, right)
                    e_ref[hi:512, 0:hi] = e_ref[hi:512, 0:hi] - dot(left, inv_ref[lo:hi, 0:hi])
        return carry

    lax.fori_loop(0, 4, step, 0)
    t = pl.multiple_of(lax.axis_index("tan") * 128, 128)
    fac_ref[...] = u_ref[:, pl.ds(t, 128)].T


spread_u, spread_v, feed_rate, kill_rate, step_size = 1.0, 0.5, 0.04, 0.06, 0.33
STAGES = (0.5 * step_size, 0.5 * step_size, step_size, step_size / 6.0) * 2

def base_coefficients(u, v, coef_ref):
    def lap(x):
        return (pltpu.roll(x, 1, 0) + pltpu.roll(x, 23, 0) + pltpu.roll(x, 1, 1) + pltpu.roll(x, NY - 1, 1) - 4.0 * x)

    def slopes(u, v):
        growth = u * v * v
        return (
            spread_u * lap(u) - growth + feed_rate * (1.0 - u),
            spread_v * lap(v) + growth - (feed_rate + kill_rate) * v,
        )

    for step in range(2):
        su, sv = u, v
        tu = tv = 0.0
        for stage in range(4):
            scale = STAGES[stage]
            square, cross = v2uv(su, sv)
            own = {0: 1.0, 1: 0.0, 2: 0.0, 3: 1.0 / 3.0}[stage]
            coef_ref[step * 4 + stage, 0] = own - scale * (4.0 * spread_u + feed_rate + square)
            coef_ref[step * 4 + stage, 1] = scale * cross
            coef_ref[step * 4 + stage, 2] = scale * square
            coef_ref[step * 4 + stage, 3] = own + scale * (cross - 4.0 * spread_v - feed_rate - kill_rate)
            if step == 1 and stage == 3:
                break
            ku, kv = slopes(su, sv)
            weight = (1.0, 2.0, 2.0, 1.0)[stage]
            tu, tv = tu + weight * ku, tv + weight * kv
            if stage < 3:
                ahead = (0.5, 0.5, 1.0)[stage] * step_size
                su, sv = u + ahead * ku, v + ahead * kv
        u, v = u + step_size / 6.0 * tu, v + step_size / 6.0 * tv


def v2uv(u, v):
    return v * v, 2.0 * u * v


def advance_group(get, put, coef_ref, z_refs, y_ref):
    first = get
    for stage in range(8):
        phase = stage % 4
        scale = STAGES[stage]
        out_lo, out_hi = stage + 1, 23 - stage
        src = {0: first, 1: reader(z_refs[0]), 2: reader(z_refs[1]), 3: reader(z_refs[2])}[phase]
        window = {}

        def at(row):
            if row not in window:
                window[row] = (src(0, row), src(1, row))
            return window[row]

        for row in range(out_lo, out_hi):
            up, mid, down = at(row - 1), at(row), at(row + 1)
            sums = [
                (up[f] + down[f]) + (pltpu.roll(mid[f], 1, 1) + pltpu.roll(mid[f], NY - 1, 1))
                for f in range(2)
            ]
            cp, bp, cq, aq = (coef_ref[stage, n, row : row + 1, :] for n in range(4))
            p = scale * spread_u * sums[0] + (cp * mid[0] - bp * mid[1])
            q = scale * spread_v * sums[1] + (cq * mid[0] + aq * mid[1])
            for f, new in ((0, p), (1, q)):
                if phase in (1, 2):
                    new = new + first(f, row)
                if phase == 3:
                    two = z_refs[1][f, row]
                    new = new + (1.0 / 3.0) * ((z_refs[0][f, row] - first(f, row)) + (two + two))
                if stage == 7:
                    put(f, row - 8, new)
                elif phase == 3:
                    y_ref[f, row] = new
                else:
                    z_refs[phase][f, row] = new
            del window[row - 1]
        if stage == 3:
            first = reader(y_ref)


def reader(ref):
    return lambda f, row: ref[f, row]


CHUNK = 8
CHUNKS = 128 // CHUNK
PACKED = [(i, j) for i in range(4) for j in range(i, 4)]
MESH_ID = pl.DeviceIdType.MESH


def place():
    return tuple(lax.axis_index(a) for a in ("tan",) + GRID)


def band_at(index):
    return {"grid_0": index // 8, "grid_1": index // 2 % 4, "grid_2": index % 2}


def along(core, turn, shift):
    x, z, y, _ = place()
    if turn == 2:
        return {"tan": (x + shift) % 4}, x
    on_y = 1 - core if turn == 0 else core
    spot = y * on_y + z * (1 - on_y)
    return {"grid_0": (z + shift * (1 - on_y)) % 4, "grid_1": (y + shift * on_y) % 4}, spot


def remote(source, target, send, receive, device):
    return pltpu.make_async_remote_copy(
        src_ref=source, dst_ref=target, send_sem=send, recv_sem=receive, device_id=device, device_id_type=MESH_ID
    )


def greet(devices):
    barrier = pltpu.get_barrier_semaphore()
    for device in devices:
        pl.semaphore_signal(barrier, inc=1, device_id=device, device_id_type=MESH_ID)
    pl.semaphore_wait(barrier, len(devices))


def packed_gram(i, v, part):
    lo = i * 256
    total = None
    for f in range(2):
        for row in range(2):
            term = dot(v[f, row, lo : lo + 256, :], v[f, row, lo:K, :], ((1,), (1,)))
            total = term if total is None else total + term
    for a in range(2):
        for b in range(a, 4 - 2 * i):
            block = PACKED.index((2 * i + a, 2 * i + b))
            for h in range(2):
                to, at = h * 640 + block * 64, a * 128 + h * 64
                part[to : to + 64] = total[at : at + 64, b * 128 : b * 128 + 128]


def sum_over_devices(v, part, acc, from_core, got_a, got_b, got_c, mid, low, total, sends, receives, then):
    core = place()[3]
    other = {"grid_2": 1 - core}

    def swap(n):
        lo, count = ((0, 224), (224, 224), (448, 192))[n]
        away = pl.ds(pl.multiple_of((1 - core) * 640 + lo, 32), count)
        return remote(part.at[away], from_core.at[lo : lo + count], sends.at[n], receives.at[n], other)

    packed_gram(0, v, part)
    swap(0).start()
    swap(1).start()
    packed_gram(1, v, part)
    swap(2).start()
    for n in range(3):
        swap(n).wait()
    acc[...] = part[pl.ds(pl.multiple_of(core * 640, 128), 640)] + from_core[...]
    copies = []
    for k in (2, 1, 3):
        there, spot = along(core, 0, k)
        rows = pl.ds(pl.multiple_of((spot + k) % 4 * 160, 8), 160)
        copies.append(remote(acc.at[rows], got_a.at[k - 1], sends.at[2 + k], receives.at[2 + k], there))
        copies[-1].start()
    for copy in copies:
        copy.wait()
    spot_a = along(core, 0, 0)[1]
    mid[...] = (acc[pl.ds(pl.multiple_of(spot_a * 160, 8), 160)] + got_a[0]) + (got_a[1] + got_a[2])
    copies = []
    for k in (2, 1, 3):
        there, spot = along(core, 1, k)
        rows = pl.ds(pl.multiple_of((spot + k) % 4 * 40, 8), 40)
        copies.append(remote(mid.at[rows], got_b.at[k - 1], sends.at[5 + k], receives.at[5 + k], there))
        copies[-1].start()
    for copy in copies:
        copy.wait()
    spot_b = along(core, 1, 0)[1]
    low[...] = (mid[pl.ds(pl.multiple_of(spot_b * 40, 8), 40)] + got_b[0]) + (got_b[1] + got_b[2])
    copies = []
    for k in (2, 1, 3):
        there, spot_c = along(core, 2, k)
        copies.append(remote(low, got_c.at[spot_c], sends.at[8 + k], receives.at[8 + k], there))
        copies[-1].start()
    got_c[along(core, 2, 0)[1]] = low[...]
    for copy in copies:
        copy.wait()

    def piece(of_core, a, b):
        return total.at[pl.ds(pl.multiple_of(of_core * 640 + a % 4 * 160 + b % 4 * 40, 8), 40)]

    def to_b(k):
        mine = piece(core, spot_a, spot_b)
        return remote(mine, mine, sends.at[11 + k], receives.at[11 + k], along(core, 1, k)[0])

    def to_a(k, kb):
        held = piece(core, spot_a, spot_b + 4 - kb)
        return remote(held, held, sends.at[15 + (k - 1) * 4 + kb], receives.at[15 + (k - 1) * 4 + kb], along(core, 0, k)[0])

    def to_core(ka, kb):
        held = piece(core, spot_a + 4 - ka, spot_b + 4 - kb)
        return remote(held, held, sends.at[27 + ka * 4 + kb], receives.at[27 + ka * 4 + kb], other)

    total[pl.ds(pl.multiple_of(spot_a * 160 + spot_b * 40 + core * 640, 8), 40)] = (got_c[0] + got_c[1]) + (got_c[2] + got_c[3])
    for k in (2, 1, 3):
        to_b(k).start()
    for k in (2, 1, 3):
        to_a(k, 0).start()
    to_core(0, 0).start()
    then()
    for kb in (1, 3, 2):
        to_b(kb).wait_recv()
        for k in (2, 1, 3):
            to_a(k, kb).start()
        to_core(0, kb).start()
    for kb in (0, 1, 3, 2):
        for ka in (1, 3, 2):
            to_a(ka, kb).wait_recv()
            to_core(ka, kb).start()
    for kb in range(4):
        for ka in range(4):
            to_core(ka, kb).wait_recv()
    for k in (1, 2, 3):
        to_b(k).wait_send()
        for kb in range(4):
            to_a(k, kb).wait_send()
    for kb in range(4):
        for ka in range(4):
            to_core(ka, kb).wait_send()


def whole_kernel(
    base_hbm, x_hbm, o_ref, fac_ref, base_ref, x_ref,
    base_above, base_below, top, bottom, out, v, part, acc, from_core, got_a, got_b, got_c, mid, low, total,
    coef_ref, z0, z1, z2, y_ref, first, a_ref, e_ref, u_ref, w_ref, inv, turned, opposite, made, own,
    base_send, base_recv, halo_send, halo_recv, give_send, give_recv, sum_send, sum_recv,
    ahead_send, ahead_recv, back_send, back_recv, own_sem, load_sem,
):
    x, z, y, core = place()
    band = (z * 4 + y) * 2 + core
    after, before = band_at((band + 1) % 32), band_at((band + 31) % 32)
    peers = [{"tan": (x + k) % 4} for k in (1, 2, 3)]
    load = pltpu.make_async_copy(x_hbm, x_ref, load_sem.at[0])
    load_base = pltpu.make_async_copy(base_hbm, base_ref, load_sem.at[1])
    load_base.start()
    load.start()
    greet(
        [after, before, {"grid_2": 1 - core}] + peers
        + [{"grid_1": (y + k) % 4} for k in (1, 2, 3)] + [{"grid_0": (z + k) % 4} for k in (1, 2, 3)]
    )
    bases = (
        remote(base_ref, base_above, base_send.at[0], base_recv.at[0], after),
        remote(base_ref, base_below, base_send.at[1], base_recv.at[1], before),
    )
    load_base.wait()
    for copy in bases:
        copy.start()

    def halos(c):
        some = pl.ds(pl.multiple_of(c * CHUNK, CHUNK), CHUNK)
        return (
            remote(x_ref.at[some], top.at[some], halo_send.at[c, 0], halo_recv.at[c, 0], after),
            remote(x_ref.at[some], bottom.at[some], halo_send.at[c, 1], halo_recv.at[c, 1], before),
        )

    def gifts(c):
        some = pl.ds(pl.multiple_of(c * CHUNK, CHUNK), CHUNK)
        mine = pl.ds(pl.multiple_of(x * 128 + c * CHUNK, CHUNK), CHUNK)
        return [
            remote(
                out.at[:, pl.ds((x + k) % 4 * 2, 2), some], v.at[:, :, mine],
                give_send.at[c, k - 1], give_recv.at[c, k - 1], {"tan": (x + k) % 4},
            )
            for k in (1, 3, 2)
        ]

    def give(c):
        some = pl.ds(pl.multiple_of(c * CHUNK, CHUNK), CHUNK)
        mine = pl.ds(pl.multiple_of(x * 128 + c * CHUNK, CHUNK), CHUNK)
        v[:, :, mine] = out[:, pl.ds(x * 2, 2), some]
        for copy in gifts(c):
            copy.start()

    def start_halo(c, carry):
        for copy in halos(c):
            copy.start()
        return carry

    load.wait()
    lax.fori_loop(0, CHUNKS, start_halo, 0)
    for copy in bases:
        copy.wait_recv()
    u, w = (jnp.concatenate([base_above[f], base_ref[f], base_below[f]], 0) for f in range(2))
    base_coefficients(u, w, coef_ref)

    def advance_chunk(c, carry):
        for copy in halos(c):
            copy.wait_recv()

        @pl.when(c > 0)
        def _():
            give(c - 1)

        def group(g, carry):
            eight = pl.ds(pl.multiple_of(c * CHUNK + g * 8, 8), 8)

            for n, ref in enumerate((top, x_ref, bottom)):
                for f in range(2):
                    first[f, n * 8 : n * 8 + 8] = jnp.swapaxes(ref[eight, f], 0, 1)

            def put(f, row, value):
                out[f, row, eight, :] = value

            advance_group(reader(first), put, coef_ref, (z0, z1, z2), y_ref)
            return carry

        return lax.fori_loop(0, CHUNK // 8, group, carry)

    lax.fori_loop(0, CHUNKS, advance_chunk, 0)
    give(CHUNKS - 1)

    def receive(c, carry):
        for copy in gifts(c):
            copy.wait_recv()
        return carry

    lax.fori_loop(0, CHUNKS, receive, 0)
    def ahead(k, chip):
        rows = pl.ds((chip + k + 2) % 4 * 2, 2)
        block = pl.ds(pl.multiple_of(chip * 128, 128), 128)
        return remote(
            out.at[:, rows], opposite.at[:, :, block], ahead_send.at[k - 1], ahead_recv.at[k - 1], {"tan": (chip + k) % 4}
        )

    def send_ahead(shifts):
        for k in shifts:
            @pl.when(x + k < 4)
            def _():
                ahead(k, x).start()

    send_ahead((1, 3))
    sum_over_devices(v, part, acc, from_core, got_a, got_b, got_c, mid, low, total, sum_send, sum_recv, lambda: send_ahead((2,)))
    factor(1.0 / (2.0 * NX * NY), total, inv, fac_ref, a_ref, e_ref, u_ref, w_ref)

    pairs = [(f, row) for f in range(2) for row in range(2)]

    def back(n, k, f, row):
        return remote(
            made.at[n, f, row], o_ref.at[f, x * 2 + row],
            back_send.at[n, f * 2 + row], back_recv.at[n, f * 2 + row], {"tan": (x + k) % 4},
        )

    def rows_of(block):
        return inv[pl.ds(pl.multiple_of(block % 4 * 128, 128), 128), :]

    turned[...] = jnp.concatenate([rows_of(x + 1), rows_of(x + 3), rows_of(x)], 0)
    keeps = []

    def keep(n, chip, f, row, value):
        own[n, f, row] = value
        copy = pltpu.make_async_copy(own.at[n, f, row], o_ref.at[f, chip * 2 + row], own_sem.at[n, f * 2 + row])
        copy.start()
        return copy

    for f, row in pairs:
        frames = dot(turned[...], v[f, row])
        for n, k in ((0, 1), (1, 3)):
            made[n, f, row] = frames[n * 128 : n * 128 + 128]
            back(n, k, f, row).start()
        keeps.append(keep(0, x, f, row, frames[256:384]))
    opposite[:, :, pl.ds(pl.multiple_of(x * 128, 128), 128)] = out[:, pl.ds((x + 2) % 4 * 2, 2)]
    for k in (1, 2, 3):
        @pl.when(x + k < 4)
        def _():
            opposite[:, :, pl.ds(pl.multiple_of((x + k) % 4 * 128, 128), 128)] = jnp.zeros((2, 2, 128, NY), jnp.float32)

        @pl.when(x >= k)
        def _():
            ahead(k, x - k).wait_recv()
    for f, row in pairs:
        keeps.append(keep(1, (x + 2) % 4, f, row, dot(turned[256:384, :], opposite[f, row])))

    for f, row in pairs:
        for n, k in ((0, 1), (1, 3)):
            back(n, k, f, row).wait()
    for k in (1, 2, 3):
        @pl.when(x + k < 4)
        def _():
            ahead(k, x).wait_send()

    def finish(c, carry):
        for copy in halos(c):
            copy.wait_send()
        for copy in gifts(c):
            copy.wait_send()
        return carry

    lax.fori_loop(0, CHUNKS, finish, 0)
    for copy in bases:
        copy.wait_send()
    for copy in keeps:
        copy.wait()


def whole(base, x):
    f32 = lambda *shape: pltpu.VMEM(shape, jnp.float32)
    sem = pltpu.SemaphoreType.DMA
    return pl.pallas_call(
        whole_kernel,
        out_shape=(jax.ShapeDtypeStruct((2, 8, 128, NY), jnp.float32), jax.ShapeDtypeStruct((128, K), jnp.float32)),
        in_specs=[pl.BlockSpec(memory_space=pltpu.HBM)] * 2,
        out_specs=(pl.BlockSpec(memory_space=pl.ANY), pl.BlockSpec(memory_space=pltpu.VMEM)),
        scratch_shapes=[
            f32(2, 8, NY), f32(128, 2, 8, NY), f32(2, 8, NY), f32(2, 8, NY), f32(128, 2, 8, NY), f32(128, 2, 8, NY), f32(2, 8, 128, NY), f32(2, 2, K, NY),
            f32(1280, 128), f32(640, 128), f32(640, 128), f32(3, 160, 128), f32(3, 40, 128), f32(4, 40, 128),
            f32(160, 128), f32(40, 128), f32(1280, 128),
            f32(8, 4, 24, NY), f32(2, 24, 8, NY), f32(2, 24, 8, NY), f32(2, 24, 8, NY), f32(2, 24, 8, NY), f32(2, 24, 8, NY),
            f32(K, K), f32(K, K), f32(K, K), f32(128, 256), f32(K, K), f32(384, K), f32(2, 2, K, NY),
            f32(2, 2, 2, 128, NY), f32(2, 2, 2, 128, NY),
            sem((2,)), sem((2,)), sem((CHUNKS, 2)), sem((CHUNKS, 2)), sem((CHUNKS, 3)), sem((CHUNKS, 3)),
            sem((43,)), sem((43,)), sem((3,)), sem((3,)), sem((2, 4)), sem((2, 4)), sem((2, 4)), sem((2,)),
        ],
        compiler_params=pltpu.CompilerParams(collective_id=0, has_side_effects=True, vmem_limit_bytes=52000 * 1024),
        name="whole",
    )(base, x)


def per_device(base, tangents):
    frames, factor_rows = whole(base, tangents)
    return (jnp.transpose(frames, (2, 0, 1, 3)), factor_rows)


def solution(mesh):
    split = Mesh(
        mesh.devices.reshape(mesh.shape["tan"], 4, 4, 2), ("tan", "grid_0", "grid_1", "grid_2")
    )
    placed = (P(None, GRID, None), P("tan", None, GRID, None))
    return jax.shard_map(
        per_device,
        mesh=split,
        in_specs=placed,
        out_specs=(P("tan", None, GRID, None), P("tan", None)),
        check_vma=False,
    )
```

```python
import functools
import jax
import jax.numpy as jnp
from jax import lax
from jax.experimental import pallas as pl
from jax.experimental.pallas import tpu as pltpu
from jax.sharding import Mesh
from jax.sharding import PartitionSpec as P

K = 512
NX = 256
NY = 256
GRID = ("grid_0", "grid_1", "grid_2")
HI = lax.Precision.HIGHEST

def factor_block(d, rows):
    lane = lax.broadcasted_iota(jnp.int32, (8, 128), 1)
    sub = lax.broadcasted_iota(jnp.int32, (8, 128), 0)
    wide = lambda x: jnp.broadcast_to(x, (8, 128))
    e = [jnp.where(lane == sub + 8 * i, 1.0, 0.0).astype(jnp.float32) for i in range(16)]
    head = [wide(d[0][:, j : j + 1]) for j in range(8)]
    for t in range(16):
        s = t * 8
        column = [{i: wide(d[i][:, s + j : s + j + 1]) for i in range(t + 1, 16)} for j in range(8)]
        ahead = [wide(d[t + 1][:, s + 8 + j : s + 9 + j]) for j in range(8)] if t < 15 else None
        for j in range(8):
            r = lax.rsqrt(wide(head[j][j : j + 1, :]))
            top = head[j] * r
            pivots = {k: wide(top[k : k + 1, :]) for k in range(j + 1, 8)}
            for k in range(j + 1, 8):
                head[k] = head[k] - top * pivots[k]
            row_d = wide(d[t][j : j + 1, :]) * r
            row_e = wide(e[t][j : j + 1, :]) * r
            rows(s + j, row_d[0:1], row_e[0:1])
            if j < 7:
                d[t] = d[t] - top * row_d
                e[t] = e[t] - top * row_e
            for i in range(t + 1, 16):
                low = column[j][i] * r
                if i == t + 1:
                    for k in range(8):
                        ahead[k] = ahead[k] - low * wide(low[k : k + 1, :])
                for k in range(j + 1, 8):
                    column[k][i] = column[k][i] - low * pivots[k]
                d[i] = d[i] - low * row_d
                e[i] = e[i] - low * row_e
        head = ahead


def dot(a, b, dims=((1,), (0,))):
    return lax.dot_general(a, b, (dims, ((), ())), precision=HI, preferred_element_type=jnp.float32)


def factor(scale, g_ref, inv_ref, fac_ref, a_ref, e_ref, u_ref, w_ref):
    block = 0
    for i in range(4):
        for j in range(i, 4):
            for h in range(2):
                at, to = h * 640 + block * 64, i * 128 + h * 64
                a_ref[to : to + 64, j * 128 : j * 128 + 128] = g_ref[at : at + 64] * scale
            block += 1
    e_ref[...] = jnp.zeros_like(e_ref)
    u_ref[...] = jnp.zeros_like(u_ref)
    inv_ref[...] = jnp.zeros_like(inv_ref)

    def step(k, carry):
        at = pl.multiple_of(k * 128, 128)
        d = [a_ref[pl.ds(pl.multiple_of(at + 8 * i, 8), 8), pl.ds(at, 128)] for i in range(16)]

        def rows(j, row_d, row_e):
            w_ref[j : j + 1, 0:128] = row_d
            w_ref[j : j + 1, 128:256] = row_e

        factor_block(d, rows)
        for kk in range(4):
            @pl.when(k == kk)
            def _():
                lo, hi = kk * 128, kk * 128 + 128
                upper = lax.broadcasted_iota(jnp.int32, (128, 128), 1) >= lax.broadcasted_iota(jnp.int32, (128, 128), 0)
                u_ref[lo:hi, lo:hi] = jnp.where(upper, w_ref[:, 0:128], 0.0)
                w = w_ref[:, 128:256]
                inv_ref[lo:hi, lo:hi] = w
                if kk:
                    inv_ref[lo:hi, 0:lo] = dot(w, e_ref[lo:hi, 0:lo])
                if kk < 3:
                    right = dot(w, a_ref[lo:hi, hi:512])
                    u_ref[lo:hi, hi:512] = right
                    left = right.T
                    a_ref[hi:512, hi:512] = a_ref[hi:512, hi:512] - dot(left, right)
                    e_ref[hi:512, 0:hi] = e_ref[hi:512, 0:hi] - dot(left, inv_ref[lo:hi, 0:hi])
        return carry

    lax.fori_loop(0, 4, step, 0)
    t = pl.multiple_of(lax.axis_index("tan") * 128, 128)
    fac_ref[...] = u_ref[:, pl.ds(t, 128)].T


spread_u, spread_v, feed_rate, kill_rate, step_size = 1.0, 0.5, 0.04, 0.06, 0.33
STAGES = (0.5 * step_size, 0.5 * step_size, step_size, step_size / 6.0) * 2

def base_coefficients(u, v, coef_ref):
    def lap(x):
        return (pltpu.roll(x, 1, 0) + pltpu.roll(x, 23, 0) + pltpu.roll(x, 1, 1) + pltpu.roll(x, NY - 1, 1) - 4.0 * x)

    def slopes(u, v):
        growth = u * v * v
        return (
            spread_u * lap(u) - growth + feed_rate * (1.0 - u),
            spread_v * lap(v) + growth - (feed_rate + kill_rate) * v,
        )

    for step in range(2):
        su, sv = u, v
        tu = tv = 0.0
        for stage in range(4):
            scale = STAGES[stage]
            square, cross = v2uv(su, sv)
            own = {0: 1.0, 1: 0.0, 2: 0.0, 3: 1.0 / 3.0}[stage]
            coef_ref[step * 4 + stage, 0] = own - scale * (4.0 * spread_u + feed_rate + square)
            coef_ref[step * 4 + stage, 1] = scale * cross
            coef_ref[step * 4 + stage, 2] = scale * square
            coef_ref[step * 4 + stage, 3] = own + scale * (cross - 4.0 * spread_v - feed_rate - kill_rate)
            if step == 1 and stage == 3:
                break
            ku, kv = slopes(su, sv)
            weight = (1.0, 2.0, 2.0, 1.0)[stage]
            tu, tv = tu + weight * ku, tv + weight * kv
            if stage < 3:
                ahead = (0.5, 0.5, 1.0)[stage] * step_size
                su, sv = u + ahead * ku, v + ahead * kv
        u, v = u + step_size / 6.0 * tu, v + step_size / 6.0 * tv


def v2uv(u, v):
    return v * v, 2.0 * u * v


def advance_group(get, put, coef_ref, z_refs, y_ref):
    first = get
    for stage in range(8):
        phase = stage % 4
        scale = STAGES[stage]
        out_lo, out_hi = stage + 1, 23 - stage
        src = {0: first, 1: reader(z_refs[0]), 2: reader(z_refs[1]), 3: reader(z_refs[2])}[phase]
        window = {}

        def at(row):
            if row not in window:
                window[row] = (src(0, row), src(1, row))
            return window[row]

        for row in range(out_lo, out_hi):
            up, mid, down = at(row - 1), at(row), at(row + 1)
            sums = [
                (up[f] + down[f]) + (pltpu.roll(mid[f], 1, 1) + pltpu.roll(mid[f], NY - 1, 1))
                for f in range(2)
            ]
            cp, bp, cq, aq = (coef_ref[stage, n, row : row + 1, :] for n in range(4))
            p = scale * spread_u * sums[0] + (cp * mid[0] - bp * mid[1])
            q = scale * spread_v * sums[1] + (cq * mid[0] + aq * mid[1])
            for f, new in ((0, p), (1, q)):
                if phase in (1, 2):
                    new = new + first(f, row)
                if phase == 3:
                    two = z_refs[1][f, row]
                    new = new + (1.0 / 3.0) * ((z_refs[0][f, row] - first(f, row)) + (two + two))
                if stage == 7:
                    put(f, row - 8, new)
                elif phase == 3:
                    y_ref[f, row] = new
                else:
                    z_refs[phase][f, row] = new
            del window[row - 1]
        if stage == 3:
            first = reader(y_ref)


def reader(ref):
    return lambda f, row: ref[f, row]


CHUNK = 8
CHUNKS = 128 // CHUNK
PACKED = [(i, j) for i in range(4) for j in range(i, 4)]
MESH_ID = pl.DeviceIdType.MESH


def place():
    return tuple(lax.axis_index(a) for a in ("tan",) + GRID)


def band_at(index):
    return {"grid_0": index // 8, "grid_1": index // 2 % 4, "grid_2": index % 2}


def along(core, turn, shift):
    x, z, y, _ = place()
    if turn == 2:
        return {"tan": (x + shift) % 4}, x
    on_y = 1 - core if turn == 0 else core
    spot = y * on_y + z * (1 - on_y)
    return {"grid_0": (z + shift * (1 - on_y)) % 4, "grid_1": (y + shift * on_y) % 4}, spot


def remote(source, target, send, receive, device):
    return pltpu.make_async_remote_copy(
        src_ref=source, dst_ref=target, send_sem=send, recv_sem=receive, device_id=device, device_id_type=MESH_ID
    )


def greet(devices):
    barrier = pltpu.get_barrier_semaphore()
    for device in devices:
        pl.semaphore_signal(barrier, inc=1, device_id=device, device_id_type=MESH_ID)
    pl.semaphore_wait(barrier, len(devices))


def packed_gram(i, v, part):
    lo = i * 256
    total = None
    for f in range(2):
        for row in range(2):
            term = dot(v[f, row, lo : lo + 256, :], v[f, row, lo:K, :], ((1,), (1,)))
            total = term if total is None else total + term
    for a in range(2):
        for b in range(a, 4 - 2 * i):
            block = PACKED.index((2 * i + a, 2 * i + b))
            for h in range(2):
                to, at = h * 640 + block * 64, a * 128 + h * 64
                part[to : to + 64] = total[at : at + 64, b * 128 : b * 128 + 128]


def sum_over_devices(v, part, acc, from_core, got_a, got_b, got_c, mid, low, total, sends, receives, then):
    core = place()[3]
    other = {"grid_2": 1 - core}

    def swap(n):
        lo, count = ((0, 224), (224, 224), (448, 192))[n]
        away = pl.ds(pl.multiple_of((1 - core) * 640 + lo, 32), count)
        return remote(part.at[away], from_core.at[lo : lo + count], sends.at[n], receives.at[n], other)

    packed_gram(0, v, part)
    swap(0).start()
    swap(1).start()
    packed_gram(1, v, part)
    swap(2).start()
    for n in range(3):
        swap(n).wait()
    acc[...] = part[pl.ds(pl.multiple_of(core * 640, 128), 640)] + from_core[...]
    copies = []
    for k in (2, 1, 3):
        there, spot = along(core, 0, k)
        rows = pl.ds(pl.multiple_of((spot + k) % 4 * 160, 8), 160)
        copies.append(remote(acc.at[rows], got_a.at[k - 1], sends.at[2 + k], receives.at[2 + k], there))
        copies[-1].start()
    for copy in copies:
        copy.wait()
    spot_a = along(core, 0, 0)[1]
    mid[...] = (acc[pl.ds(pl.multiple_of(spot_a * 160, 8), 160)] + got_a[0]) + (got_a[1] + got_a[2])
    copies = []
    for k in (2, 1, 3):
        there, spot = along(core, 1, k)
        rows = pl.ds(pl.multiple_of((spot + k) % 4 * 40, 8), 40)
        copies.append(remote(mid.at[rows], got_b.at[k - 1], sends.at[5 + k], receives.at[5 + k], there))
        copies[-1].start()
    for copy in copies:
        copy.wait()
    spot_b = along(core, 1, 0)[1]
    low[...] = (mid[pl.ds(pl.multiple_of(spot_b * 40, 8), 40)] + got_b[0]) + (got_b[1] + got_b[2])
    copies = []
    for k in (2, 1, 3):
        there, spot_c = along(core, 2, k)
        copies.append(remote(low, got_c.at[spot_c], sends.at[8 + k], receives.at[8 + k], there))
        copies[-1].start()
    got_c[along(core, 2, 0)[1]] = low[...]
    for copy in copies:
        copy.wait()

    def piece(of_core, a, b):
        return total.at[pl.ds(pl.multiple_of(of_core * 640 + a % 4 * 160 + b % 4 * 40, 8), 40)]

    def to_b(k):
        mine = piece(core, spot_a, spot_b)
        return remote(mine, mine, sends.at[11 + k], receives.at[11 + k], along(core, 1, k)[0])

    def to_a(k, kb):
        held = piece(core, spot_a, spot_b + 4 - kb)
        return remote(held, held, sends.at[15 + (k - 1) * 4 + kb], receives.at[15 + (k - 1) * 4 + kb], along(core, 0, k)[0])

    def to_core(ka, kb):
        held = piece(core, spot_a + 4 - ka, spot_b + 4 - kb)
        return remote(held, held, sends.at[27 + ka * 4 + kb], receives.at[27 + ka * 4 + kb], other)

    total[pl.ds(pl.multiple_of(spot_a * 160 + spot_b * 40 + core * 640, 8), 40)] = (got_c[0] + got_c[1]) + (got_c[2] + got_c[3])
    for k in (2, 1, 3):
        to_b(k).start()
    for k in (2, 1, 3):
        to_a(k, 0).start()
    to_core(0, 0).start()
    then()
    for kb in (1, 3, 2):
        to_b(kb).wait_recv()
        for k in (2, 1, 3):
            to_a(k, kb).start()
        to_core(0, kb).start()
    for kb in (0, 1, 3, 2):
        for ka in (1, 3, 2):
            to_a(ka, kb).wait_recv()
            to_core(ka, kb).start()
    for kb in range(4):
        for ka in range(4):
            to_core(ka, kb).wait_recv()
    for k in (1, 2, 3):
        to_b(k).wait_send()
        for kb in range(4):
            to_a(k, kb).wait_send()
    for kb in range(4):
        for ka in range(4):
            to_core(ka, kb).wait_send()


def whole_kernel(
    base_hbm, x_hbm, o_ref, fac_ref, base_ref, x_ref,
    base_above, base_below, top, bottom, out, v, part, acc, from_core, got_a, got_b, got_c, mid, low, total,
    coef_ref, z0, z1, z2, y_ref, first, a_ref, e_ref, u_ref, w_ref, inv, turned, opposite, made, own,
    base_send, base_recv, halo_send, halo_recv, give_send, give_recv, sum_send, sum_recv,
    ahead_send, ahead_recv, back_send, back_recv, own_sem, load_sem,
):
    x, z, y, core = place()
    band = (z * 4 + y) * 2 + core
    after, before = band_at((band + 1) % 32), band_at((band + 31) % 32)
    peers = [{"tan": (x + k) % 4} for k in (1, 2, 3)]
    load = pltpu.make_async_copy(x_hbm, x_ref, load_sem.at[0])
    load_base = pltpu.make_async_copy(base_hbm, base_ref, load_sem.at[1])
    load_base.start()
    load.start()
    greet(
        [after, before, {"grid_2": 1 - core}] + peers
        + [{"grid_1": (y + k) % 4} for k in (1, 2, 3)] + [{"grid_0": (z + k) % 4} for k in (1, 2, 3)]
    )
    bases = (
        remote(base_ref, base_above, base_send.at[0], base_recv.at[0], after),
        remote(base_ref, base_below, base_send.at[1], base_recv.at[1], before),
    )
    load_base.wait()
    for copy in bases:
        copy.start()

    def halos(c):
        some = pl.ds(pl.multiple_of(c * CHUNK, CHUNK), CHUNK)
        return (
            remote(x_ref.at[some], top.at[some], halo_send.at[c, 0], halo_recv.at[c, 0], after),
            remote(x_ref.at[some], bottom.at[some], halo_send.at[c, 1], halo_recv.at[c, 1], before),
        )

    def gifts(c):
        some = pl.ds(pl.multiple_of(c * CHUNK, CHUNK), CHUNK)
        mine = pl.ds(pl.multiple_of(x * 128 + c * CHUNK, CHUNK), CHUNK)
        return [
            remote(
                out.at[:, pl.ds((x + k) % 4 * 2, 2), some], v.at[:, :, mine],
                give_send.at[c, k - 1], give_recv.at[c, k - 1], {"tan": (x + k) % 4},
            )
            for k in (2, 1, 3)
        ]

    def give(c):
        some = pl.ds(pl.multiple_of(c * CHUNK, CHUNK), CHUNK)
        mine = pl.ds(pl.multiple_of(x * 128 + c * CHUNK, CHUNK), CHUNK)
        v[:, :, mine] = out[:, pl.ds(x * 2, 2), some]
        for copy in gifts(c):
            copy.start()

    def start_halo(c, carry):
        for copy in halos(c):
            copy.start()
        return carry

    load.wait()
    lax.fori_loop(0, CHUNKS, start_halo, 0)
    for copy in bases:
        copy.wait_recv()
    u, w = (jnp.concatenate([base_above[f], base_ref[f], base_below[f]], 0) for f in range(2))
    base_coefficients(u, w, coef_ref)

    def advance_chunk(c, carry):
        for copy in halos(c):
            copy.wait_recv()

        @pl.when(c > 0)
        def _():
            give(c - 1)

        def group(g, carry):
            eight = pl.ds(pl.multiple_of(c * CHUNK + g * 8, 8), 8)

            for n, ref in enumerate((top, x_ref, bottom)):
                for f in range(2):
                    first[f, n * 8 : n * 8 + 8] = jnp.swapaxes(ref[eight, f], 0, 1)

            def put(f, row, value):
                out[f, row, eight, :] = value

            advance_group(reader(first), put, coef_ref, (z0, z1, z2), y_ref)
            return carry

        return lax.fori_loop(0, CHUNK // 8, group, carry)

    lax.fori_loop(0, CHUNKS, advance_chunk, 0)
    give(CHUNKS - 1)

    def receive(c, carry):
        for copy in gifts(c):
            copy.wait_recv()
        return carry

    lax.fori_loop(0, CHUNKS, receive, 0)
    def ahead(k, chip):
        rows = pl.ds((chip + k + 2) % 4 * 2, 2)
        block = pl.ds(pl.multiple_of(chip * 128, 128), 128)
        return remote(
            out.at[:, rows], opposite.at[:, :, block], ahead_send.at[k - 1], ahead_recv.at[k - 1], {"tan": (chip + k) % 4}
        )

    def send_ahead(shifts):
        for k in shifts:
            @pl.when(x + k < 4)
            def _():
                ahead(k, x).start()

    send_ahead((1, 3))
    sum_over_devices(v, part, acc, from_core, got_a, got_b, got_c, mid, low, total, sum_send, sum_recv, lambda: send_ahead((2,)))
    factor(1.0 / (2.0 * NX * NY), total, inv, fac_ref, a_ref, e_ref, u_ref, w_ref)

    pairs = [(f, row) for f in range(2) for row in range(2)]

    def back(n, k, f, row):
        return remote(
            made.at[n, f, row], o_ref.at[f, x * 2 + row],
            back_send.at[n, f * 2 + row], back_recv.at[n, f * 2 + row], {"tan": (x + k) % 4},
        )

    def rows_of(block):
        return inv[pl.ds(pl.multiple_of(block % 4 * 128, 128), 128), :]

    turned[...] = jnp.concatenate([rows_of(x + 1), rows_of(x + 3), rows_of(x)], 0)
    keeps = []

    def keep(n, chip, f, row, value):
        own[n, f, row] = value
        copy = pltpu.make_async_copy(own.at[n, f, row], o_ref.at[f, chip * 2 + row], own_sem.at[n, f * 2 + row])
        copy.start()
        return copy

    for f, row in pairs:
        frames = dot(turned[...], v[f, row])
        for n, k in ((0, 1), (1, 3)):
            made[n, f, row] = frames[n * 128 : n * 128 + 128]
            back(n, k, f, row).start()
        keeps.append(keep(0, x, f, row, frames[256:384]))
    opposite[:, :, pl.ds(pl.multiple_of(x * 128, 128), 128)] = out[:, pl.ds((x + 2) % 4 * 2, 2)]
    for k in (1, 2, 3):
        @pl.when(x + k < 4)
        def _():
            opposite[:, :, pl.ds(pl.multiple_of((x + k) % 4 * 128, 128), 128)] = jnp.zeros((2, 2, 128, NY), jnp.float32)

        @pl.when(x >= k)
        def _():
            ahead(k, x - k).wait_recv()
    for f, row in pairs:
        keeps.append(keep(1, (x + 2) % 4, f, row, dot(turned[256:384, :], opposite[f, row])))

    for f, row in pairs:
        for n, k in ((0, 1), (1, 3)):
            back(n, k, f, row).wait()
    for k in (1, 2, 3):
        @pl.when(x + k < 4)
        def _():
            ahead(k, x).wait_send()

    def finish(c, carry):
        for copy in halos(c):
            copy.wait_send()
        for copy in gifts(c):
            copy.wait_send()
        return carry

    lax.fori_loop(0, CHUNKS, finish, 0)
    for copy in bases:
        copy.wait_send()
    for copy in keeps:
        copy.wait()


def whole(base, x):
    f32 = lambda *shape: pltpu.VMEM(shape, jnp.float32)
    sem = pltpu.SemaphoreType.DMA
    return pl.pallas_call(
        whole_kernel,
        out_shape=(jax.ShapeDtypeStruct((2, 8, 128, NY), jnp.float32), jax.ShapeDtypeStruct((128, K), jnp.float32)),
        in_specs=[pl.BlockSpec(memory_space=pltpu.HBM)] * 2,
        out_specs=(pl.BlockSpec(memory_space=pl.ANY), pl.BlockSpec(memory_space=pltpu.VMEM)),
        scratch_shapes=[
            f32(2, 8, NY), f32(128, 2, 8, NY), f32(2, 8, NY), f32(2, 8, NY), f32(128, 2, 8, NY), f32(128, 2, 8, NY), f32(2, 8, 128, NY), f32(2, 2, K, NY),
            f32(1280, 128), f32(640, 128), f32(640, 128), f32(3, 160, 128), f32(3, 40, 128), f32(4, 40, 128),
            f32(160, 128), f32(40, 128), f32(1280, 128),
            f32(8, 4, 24, NY), f32(2, 24, 8, NY), f32(2, 24, 8, NY), f32(2, 24, 8, NY), f32(2, 24, 8, NY), f32(2, 24, 8, NY),
            f32(K, K), f32(K, K), f32(K, K), f32(128, 256), f32(K, K), f32(384, K), f32(2, 2, K, NY),
            f32(2, 2, 2, 128, NY), f32(2, 2, 2, 128, NY),
            sem((2,)), sem((2,)), sem((CHUNKS, 2)), sem((CHUNKS, 2)), sem((CHUNKS, 3)), sem((CHUNKS, 3)),
            sem((43,)), sem((43,)), sem((3,)), sem((3,)), sem((2, 4)), sem((2, 4)), sem((2, 4)), sem((2,)),
        ],
        compiler_params=pltpu.CompilerParams(collective_id=0, has_side_effects=True, vmem_limit_bytes=52000 * 1024),
        name="whole",
    )(base, x)


SETTLE = 32


def settle_kernel(frames_ref, rows_ref, o_ref, fac_ref, turned, sem, fac_sem):
    rows = pltpu.make_async_copy(rows_ref, fac_ref, fac_sem)
    rows.start()
    copies = []
    for n in range(128 // SETTLE):
        for g in range(n * SETTLE, n * SETTLE + SETTLE, 8):
            for f in range(2):
                turned[g : g + 8, f] = jnp.swapaxes(frames_ref[f, :, g : g + 8, :], 0, 1)
        some = pl.ds(n * SETTLE, SETTLE)
        copies.append(pltpu.make_async_copy(turned.at[some], o_ref.at[some], sem.at[n]))
        copies[-1].start()
    for copy in copies:
        copy.wait()
    rows.wait()


def settled(frames, rows):
    return pl.pallas_call(
        settle_kernel,
        out_shape=(jax.ShapeDtypeStruct((128, 2, 8, NY), jnp.float32), jax.ShapeDtypeStruct((128, K), jnp.float32)),
        in_specs=[pl.BlockSpec(memory_space=pltpu.VMEM)] * 2,
        out_specs=(pl.BlockSpec(memory_space=pl.ANY),) * 2,
        scratch_shapes=[
            pltpu.VMEM((128, 2, 8, NY), jnp.float32),
            pltpu.SemaphoreType.DMA((128 // SETTLE,)), pltpu.SemaphoreType.DMA(()),
        ],
        compiler_params=pltpu.CompilerParams(vmem_limit_bytes=16 * 1024 * 1024),
        name="settle",
    )(frames, rows)


def per_device(base, tangents):
    return settled(*whole(base, tangents))


def solution(mesh):
    split = Mesh(
        mesh.devices.reshape(mesh.shape["tan"], 4, 4, 2), ("tan", "grid_0", "grid_1", "grid_2")
    )
    placed = (P(None, GRID, None), P("tan", None, GRID, None))
    return jax.shard_map(
        per_device,
        mesh=split,
        in_specs=placed,
        out_specs=(P("tan", None, GRID, None), P("tan", None)),
        check_vma=False,
    )
```

```python
import functools
import jax
import jax.numpy as jnp
from jax import lax
from jax.experimental import pallas as pl
from jax.experimental.pallas import tpu as pltpu
from jax.sharding import Mesh
from jax.sharding import PartitionSpec as P

K = 512
NX = 256
NY = 256
GRID = ("grid_0", "grid_1", "grid_2")
HI = lax.Precision.HIGHEST

def factor_block(d, rows):
    lane = lax.broadcasted_iota(jnp.int32, (8, 128), 1)
    sub = lax.broadcasted_iota(jnp.int32, (8, 128), 0)
    wide = lambda x: jnp.broadcast_to(x, (8, 128))
    e = [jnp.where(lane == sub + 8 * i, 1.0, 0.0).astype(jnp.float32) for i in range(16)]
    head = [wide(d[0][:, j : j + 1]) for j in range(8)]
    for t in range(16):
        s = t * 8
        column = [{i: wide(d[i][:, s + j : s + j + 1]) for i in range(t + 1, 16)} for j in range(8)]
        ahead = [wide(d[t + 1][:, s + 8 + j : s + 9 + j]) for j in range(8)] if t < 15 else None
        for j in range(8):
            r = lax.rsqrt(wide(head[j][j : j + 1, :]))
            top = head[j] * r
            pivots = {k: wide(top[k : k + 1, :]) for k in range(j + 1, 8)}
            for k in range(j + 1, 8):
                head[k] = head[k] - top * pivots[k]
            row_d = wide(d[t][j : j + 1, :]) * r
            row_e = wide(e[t][j : j + 1, :]) * r
            rows(s + j, row_d[0:1], row_e[0:1])
            if j < 7:
                d[t] = d[t] - top * row_d
                e[t] = e[t] - top * row_e
            for i in range(t + 1, 16):
                low = column[j][i] * r
                if i == t + 1:
                    for k in range(8):
                        ahead[k] = ahead[k] - low * wide(low[k : k + 1, :])
                for k in range(j + 1, 8):
                    column[k][i] = column[k][i] - low * pivots[k]
                d[i] = d[i] - low * row_d
                e[i] = e[i] - low * row_e
        head = ahead


def dot(a, b, dims=((1,), (0,))):
    return lax.dot_general(a, b, (dims, ((), ())), precision=HI, preferred_element_type=jnp.float32)


def factor(scale, arrived, g_ref, inv_ref, fac_ref, a_ref, e_ref, u_ref, w_ref):
    def unpack(block):
        i, j = PACKED[block]
        for h in range(2):
            at, to = h * 640 + block * 64, i * 128 + h * 64
            a_ref[to : to + 64, j * 128 : j * 128 + 128] = g_ref[at : at + 64] * scale

    unpack(0)
    e_ref[...] = jnp.zeros_like(e_ref)
    u_ref[...] = jnp.zeros_like(u_ref)
    inv_ref[...] = jnp.zeros_like(inv_ref)

    def step(k, carry):
        at = pl.multiple_of(k * 128, 128)
        d = [a_ref[pl.ds(pl.multiple_of(at + 8 * i, 8), 8), pl.ds(at, 128)] for i in range(16)]

        def rows(j, row_d, row_e):
            w_ref[j : j + 1, 0:128] = row_d
            w_ref[j : j + 1, 128:256] = row_e

        factor_block(d, rows)

        @pl.when(k == 0)
        def _():
            arrived()
            for block in range(1, 10):
                unpack(block)

        for kk in range(4):
            @pl.when(k == kk)
            def _():
                lo, hi = kk * 128, kk * 128 + 128
                upper = lax.broadcasted_iota(jnp.int32, (128, 128), 1) >= lax.broadcasted_iota(jnp.int32, (128, 128), 0)
                u_ref[lo:hi, lo:hi] = jnp.where(upper, w_ref[:, 0:128], 0.0)
                w = w_ref[:, 128:256]
                inv_ref[lo:hi, lo:hi] = w
                if kk:
                    inv_ref[lo:hi, 0:lo] = dot(w, e_ref[lo:hi, 0:lo])
                if kk < 3:
                    right = dot(w, a_ref[lo:hi, hi:512])
                    u_ref[lo:hi, hi:512] = right
                    left = right.T
                    a_ref[hi:512, hi:512] = a_ref[hi:512, hi:512] - dot(left, right)
                    e_ref[hi:512, 0:hi] = e_ref[hi:512, 0:hi] - dot(left, inv_ref[lo:hi, 0:hi])
        return carry

    lax.fori_loop(0, 4, step, 0)
    t = pl.multiple_of(lax.axis_index("tan") * 128, 128)
    fac_ref[...] = u_ref[:, pl.ds(t, 128)].T


spread_u, spread_v, feed_rate, kill_rate, step_size = 1.0, 0.5, 0.04, 0.06, 0.33
STAGES = (0.5 * step_size, 0.5 * step_size, step_size, step_size / 6.0) * 2

def base_coefficients(u, v, coef_ref):
    def lap(x):
        return (pltpu.roll(x, 1, 0) + pltpu.roll(x, 23, 0) + pltpu.roll(x, 1, 1) + pltpu.roll(x, NY - 1, 1) - 4.0 * x)

    def slopes(u, v):
        growth = u * v * v
        return (
            spread_u * lap(u) - growth + feed_rate * (1.0 - u),
            spread_v * lap(v) + growth - (feed_rate + kill_rate) * v,
        )

    for step in range(2):
        su, sv = u, v
        tu = tv = 0.0
        for stage in range(4):
            scale = STAGES[stage]
            square, cross = v2uv(su, sv)
            own = {0: 1.0, 1: 0.0, 2: 0.0, 3: 1.0 / 3.0}[stage]
            coef_ref[step * 4 + stage, 0] = own - scale * (4.0 * spread_u + feed_rate + square)
            coef_ref[step * 4 + stage, 1] = scale * cross
            coef_ref[step * 4 + stage, 2] = scale * square
            coef_ref[step * 4 + stage, 3] = own + scale * (cross - 4.0 * spread_v - feed_rate - kill_rate)
            if step == 1 and stage == 3:
                break
            ku, kv = slopes(su, sv)
            weight = (1.0, 2.0, 2.0, 1.0)[stage]
            tu, tv = tu + weight * ku, tv + weight * kv
            if stage < 3:
                ahead = (0.5, 0.5, 1.0)[stage] * step_size
                su, sv = u + ahead * ku, v + ahead * kv
        u, v = u + step_size / 6.0 * tu, v + step_size / 6.0 * tv


def v2uv(u, v):
    return v * v, 2.0 * u * v


def advance_group(get, put, coef_ref, z_refs, y_ref):
    first = get
    for stage in range(8):
        phase = stage % 4
        scale = STAGES[stage]
        out_lo, out_hi = stage + 1, 23 - stage
        src = {0: first, 1: reader(z_refs[0]), 2: reader(z_refs[1]), 3: reader(z_refs[2])}[phase]
        window = {}

        def at(row):
            if row not in window:
                window[row] = (src(0, row), src(1, row))
            return window[row]

        for row in range(out_lo, out_hi):
            up, mid, down = at(row - 1), at(row), at(row + 1)
            sums = [
                (up[f] + down[f]) + (pltpu.roll(mid[f], 1, 1) + pltpu.roll(mid[f], NY - 1, 1))
                for f in range(2)
            ]
            cp, bp, cq, aq = (coef_ref[stage, n, row : row + 1, :] for n in range(4))
            p = scale * spread_u * sums[0] + (cp * mid[0] - bp * mid[1])
            q = scale * spread_v * sums[1] + (cq * mid[0] + aq * mid[1])
            for f, new in ((0, p), (1, q)):
                if phase in (1, 2):
                    new = new + first(f, row)
                if phase == 3:
                    two = z_refs[1][f, row]
                    new = new + (1.0 / 3.0) * ((z_refs[0][f, row] - first(f, row)) + (two + two))
                if stage == 7:
                    put(f, row - 8, new)
                elif phase == 3:
                    y_ref[f, row] = new
                else:
                    z_refs[phase][f, row] = new
            del window[row - 1]
        if stage == 3:
            first = reader(y_ref)


def reader(ref):
    return lambda f, row: ref[f, row]


CHUNK = 8
CHUNKS = 128 // CHUNK
PACKED = [(i, j) for i in range(4) for j in range(i, 4)]
MESH_ID = pl.DeviceIdType.MESH


def place():
    return tuple(lax.axis_index(a) for a in ("tan",) + GRID)


def band_at(index):
    return {"grid_0": index // 8, "grid_1": index // 2 % 4, "grid_2": index % 2}


def along(core, turn, shift):
    x, z, y, _ = place()
    if turn == 2:
        return {"tan": (x + shift) % 4}, x
    on_y = 1 - core if turn == 0 else core
    spot = y * on_y + z * (1 - on_y)
    return {"grid_0": (z + shift * (1 - on_y)) % 4, "grid_1": (y + shift * on_y) % 4}, spot


def remote(source, target, send, receive, device):
    return pltpu.make_async_remote_copy(
        src_ref=source, dst_ref=target, send_sem=send, recv_sem=receive, device_id=device, device_id_type=MESH_ID
    )


def greet(devices):
    barrier = pltpu.get_barrier_semaphore()
    for device in devices:
        pl.semaphore_signal(barrier, inc=1, device_id=device, device_id_type=MESH_ID)
    pl.semaphore_wait(barrier, len(devices))


def packed_gram(i, v, part):
    lo = i * 256
    total = None
    for f in range(2):
        for row in range(2):
            term = dot(v[f, row, lo : lo + 256, :], v[f, row, lo:K, :], ((1,), (1,)))
            total = term if total is None else total + term
    for a in range(2):
        for b in range(a, 4 - 2 * i):
            block = PACKED.index((2 * i + a, 2 * i + b))
            for h in range(2):
                to, at = h * 640 + block * 64, a * 128 + h * 64
                part[to : to + 64] = total[at : at + 64, b * 128 : b * 128 + 128]


def sum_over_devices(v, part, acc, from_core, got_a, got_b, got_c, mid, low, total, sends, receives, then):
    core = place()[3]
    other = {"grid_2": 1 - core}

    def swap(n):
        lo, count = ((0, 224), (224, 224), (448, 192))[n]
        away = pl.ds(pl.multiple_of((1 - core) * 640 + lo, 32), count)
        return remote(part.at[away], from_core.at[lo : lo + count], sends.at[n], receives.at[n], other)

    packed_gram(0, v, part)
    swap(0).start()
    swap(1).start()
    packed_gram(1, v, part)
    swap(2).start()
    for n in range(3):
        swap(n).wait()
    acc[...] = part[pl.ds(pl.multiple_of(core * 640, 128), 640)] + from_core[...]
    copies = []
    for k in (2, 1, 3):
        there, spot = along(core, 0, k)
        rows = pl.ds(pl.multiple_of((spot + k) % 4 * 160, 8), 160)
        copies.append(remote(acc.at[rows], got_a.at[k - 1], sends.at[2 + k], receives.at[2 + k], there))
        copies[-1].start()
    for copy in copies:
        copy.wait()
    spot_a = along(core, 0, 0)[1]
    mid[...] = (acc[pl.ds(pl.multiple_of(spot_a * 160, 8), 160)] + got_a[0]) + (got_a[1] + got_a[2])
    copies = []
    for k in (2, 1, 3):
        there, spot = along(core, 1, k)
        rows = pl.ds(pl.multiple_of((spot + k) % 4 * 40, 8), 40)
        copies.append(remote(mid.at[rows], got_b.at[k - 1], sends.at[5 + k], receives.at[5 + k], there))
        copies[-1].start()
    for copy in copies:
        copy.wait()
    spot_b = along(core, 1, 0)[1]
    low[...] = (mid[pl.ds(pl.multiple_of(spot_b * 40, 8), 40)] + got_b[0]) + (got_b[1] + got_b[2])
    copies = []
    for k in (2, 1, 3):
        there, spot_c = along(core, 2, k)
        copies.append(remote(low, got_c.at[spot_c], sends.at[8 + k], receives.at[8 + k], there))
        copies[-1].start()
    got_c[along(core, 2, 0)[1]] = low[...]
    for copy in copies:
        copy.wait()

    def piece(of_core, a, b):
        return total.at[pl.ds(pl.multiple_of(of_core * 640 + a % 4 * 160 + b % 4 * 40, 8), 40)]

    def to_b(k):
        mine = piece(core, spot_a, spot_b)
        return remote(mine, mine, sends.at[11 + k], receives.at[11 + k], along(core, 1, k)[0])

    def to_a(k, kb):
        held = piece(core, spot_a, spot_b + 4 - kb)
        return remote(held, held, sends.at[15 + (k - 1) * 4 + kb], receives.at[15 + (k - 1) * 4 + kb], along(core, 0, k)[0])

    def to_core(ka, kb):
        held = piece(core, spot_a + 4 - ka, spot_b + 4 - kb)
        return remote(held, held, sends.at[27 + ka * 4 + kb], receives.at[27 + ka * 4 + kb], other)

    total[pl.ds(pl.multiple_of(spot_a * 160 + spot_b * 40 + core * 640, 8), 40)] = (got_c[0] + got_c[1]) + (got_c[2] + got_c[3])
    for k in (2, 1, 3):
        to_b(k).start()
    for k in (2, 1, 3):
        to_a(k, 0).start()
    to_core(0, 0).start()
    then()
    for kb in (1, 3, 2):
        to_b(kb).wait_recv()
        for k in (2, 1, 3):
            to_a(k, kb).start()
        to_core(0, kb).start()
    for kb in (0, 1, 3, 2):
        for ka in (1, 3, 2):
            to_a(ka, kb).wait_recv()
            to_core(ka, kb).start()
    def from_partner(a, b):
        held = piece(1 - core, a, b)
        n = 27 + (spot_b + 4 - a) % 4 * 4 + (spot_a + 4 - b) % 4
        return remote(held, held, sends.at[n], receives.at[n], other)

    early = [(0, 0), (0, 1)]
    for a, b in early:
        from_partner(a, b).wait_recv()

    def arrived():
        for a in range(4):
            for b in range(4):
                if (a, b) not in early:
                    from_partner(a, b).wait_recv()

    def sent():
        for k in (1, 2, 3):
            to_b(k).wait_send()
            for kb in range(4):
                to_a(k, kb).wait_send()
        for kb in range(4):
            for ka in range(4):
                to_core(ka, kb).wait_send()

    return arrived, sent


def whole_kernel(
    base_hbm, x_hbm, o_ref, fac_ref, base_ref, x_ref,
    base_above, base_below, top, bottom, out, v, part, acc, from_core, got_a, got_b, got_c, mid, low, total,
    coef_ref, z0, z1, z2, y_ref, first, a_ref, e_ref, u_ref, w_ref, inv, turned, opposite, made, own,
    base_send, base_recv, halo_send, halo_recv, give_send, give_recv, sum_send, sum_recv,
    ahead_send, ahead_recv, back_send, back_recv, own_sem, load_sem,
):
    x, z, y, core = place()
    band = (z * 4 + y) * 2 + core
    after, before = band_at((band + 1) % 32), band_at((band + 31) % 32)
    peers = [{"tan": (x + k) % 4} for k in (1, 2, 3)]
    load = pltpu.make_async_copy(x_hbm, x_ref, load_sem.at[0])
    load_base = pltpu.make_async_copy(base_hbm, base_ref, load_sem.at[1])
    load_base.start()
    load.start()
    greet(
        [after, before, {"grid_2": 1 - core}] + peers
        + [{"grid_1": (y + k) % 4} for k in (1, 2, 3)] + [{"grid_0": (z + k) % 4} for k in (1, 2, 3)]
    )
    bases = (
        remote(base_ref, base_above, base_send.at[0], base_recv.at[0], after),
        remote(base_ref, base_below, base_send.at[1], base_recv.at[1], before),
    )
    load_base.wait()
    for copy in bases:
        copy.start()

    def halos(c):
        some = pl.ds(pl.multiple_of(c * CHUNK, CHUNK), CHUNK)
        return (
            remote(x_ref.at[some], top.at[some], halo_send.at[c, 0], halo_recv.at[c, 0], after),
            remote(x_ref.at[some], bottom.at[some], halo_send.at[c, 1], halo_recv.at[c, 1], before),
        )

    def gifts(c):
        some = pl.ds(pl.multiple_of(c * CHUNK, CHUNK), CHUNK)
        mine = pl.ds(pl.multiple_of(x * 128 + c * CHUNK, CHUNK), CHUNK)
        return [
            remote(
                out.at[:, pl.ds((x + k) % 4 * 2, 2), some], v.at[:, :, mine],
                give_send.at[c, k - 1], give_recv.at[c, k - 1], {"tan": (x + k) % 4},
            )
            for k in (2, 1, 3)
        ]

    def give(c):
        some = pl.ds(pl.multiple_of(c * CHUNK, CHUNK), CHUNK)
        mine = pl.ds(pl.multiple_of(x * 128 + c * CHUNK, CHUNK), CHUNK)
        v[:, :, mine] = out[:, pl.ds(x * 2, 2), some]
        for copy in gifts(c):
            copy.start()

    def start_halo(c, carry):
        for copy in halos(c):
            copy.start()
        return carry

    load.wait()
    lax.fori_loop(0, CHUNKS, start_halo, 0)
    for copy in bases:
        copy.wait_recv()
    u, w = (jnp.concatenate([base_above[f], base_ref[f], base_below[f]], 0) for f in range(2))
    base_coefficients(u, w, coef_ref)

    def advance_chunk(c, carry):
        for copy in halos(c):
            copy.wait_recv()

        @pl.when(c > 0)
        def _():
            give(c - 1)

        def group(g, carry):
            eight = pl.ds(pl.multiple_of(c * CHUNK + g * 8, 8), 8)

            for n, ref in enumerate((top, x_ref, bottom)):
                for f in range(2):
                    first[f, n * 8 : n * 8 + 8] = jnp.swapaxes(ref[eight, f], 0, 1)

            def put(f, row, value):
                out[f, row, eight, :] = value

            advance_group(reader(first), put, coef_ref, (z0, z1, z2), y_ref)
            return carry

        return lax.fori_loop(0, CHUNK // 8, group, carry)

    lax.fori_loop(0, CHUNKS, advance_chunk, 0)
    give(CHUNKS - 1)

    def receive(c, carry):
        for copy in gifts(c):
            copy.wait_recv()
        return carry

    lax.fori_loop(0, CHUNKS, receive, 0)
    def ahead(k, chip):
        rows = pl.ds((chip + k + 2) % 4 * 2, 2)
        block = pl.ds(pl.multiple_of(chip * 128, 128), 128)
        return remote(
            out.at[:, rows], opposite.at[:, :, block], ahead_send.at[k - 1], ahead_recv.at[k - 1], {"tan": (chip + k) % 4}
        )

    def send_ahead(shifts):
        for k in shifts:
            @pl.when(x + k < 4)
            def _():
                ahead(k, x).start()

    send_ahead((1, 3))
    arrived, sent = sum_over_devices(v, part, acc, from_core, got_a, got_b, got_c, mid, low, total, sum_send, sum_recv, lambda: send_ahead((2,)))
    factor(1.0 / (2.0 * NX * NY), arrived, total, inv, fac_ref, a_ref, e_ref, u_ref, w_ref)

    pairs = [(f, row) for f in range(2) for row in range(2)]

    def back(n, k, f, row):
        return remote(
            made.at[n, f, row], o_ref.at[f, x * 2 + row],
            back_send.at[n, f * 2 + row], back_recv.at[n, f * 2 + row], {"tan": (x + k) % 4},
        )

    def rows_of(block):
        return inv[pl.ds(pl.multiple_of(block % 4 * 128, 128), 128), :]

    turned[...] = jnp.concatenate([rows_of(x + 1), rows_of(x + 3), rows_of(x)], 0)
    keeps = []

    def keep(n, chip, f, row, value):
        own[n, f, row] = value
        copy = pltpu.make_async_copy(own.at[n, f, row], o_ref.at[f, chip * 2 + row], own_sem.at[n, f * 2 + row])
        copy.start()
        return copy

    for f, row in pairs:
        frames = dot(turned[...], v[f, row])
        for n, k in ((0, 1), (1, 3)):
            made[n, f, row] = frames[n * 128 : n * 128 + 128]
            back(n, k, f, row).start()
        keeps.append(keep(0, x, f, row, frames[256:384]))
    opposite[:, :, pl.ds(pl.multiple_of(x * 128, 128), 128)] = out[:, pl.ds((x + 2) % 4 * 2, 2)]
    for k in (1, 2, 3):
        @pl.when(x + k < 4)
        def _():
            opposite[:, :, pl.ds(pl.multiple_of((x + k) % 4 * 128, 128), 128)] = jnp.zeros((2, 2, 128, NY), jnp.float32)

        @pl.when(x >= k)
        def _():
            ahead(k, x - k).wait_recv()
    for f, row in pairs:
        keeps.append(keep(1, (x + 2) % 4, f, row, dot(turned[256:384, :], opposite[f, row])))

    for f, row in pairs:
        for n, k in ((0, 1), (1, 3)):
            back(n, k, f, row).wait()
    for k in (1, 2, 3):
        @pl.when(x + k < 4)
        def _():
            ahead(k, x).wait_send()

    def finish(c, carry):
        for copy in halos(c):
            copy.wait_send()
        for copy in gifts(c):
            copy.wait_send()
        return carry

    sent()
    lax.fori_loop(0, CHUNKS, finish, 0)
    for copy in bases:
        copy.wait_send()
    for copy in keeps:
        copy.wait()


def whole(base, x):
    f32 = lambda *shape: pltpu.VMEM(shape, jnp.float32)
    sem = pltpu.SemaphoreType.DMA
    return pl.pallas_call(
        whole_kernel,
        out_shape=(jax.ShapeDtypeStruct((2, 8, 128, NY), jnp.float32), jax.ShapeDtypeStruct((128, K), jnp.float32)),
        in_specs=[pl.BlockSpec(memory_space=pltpu.HBM)] * 2,
        out_specs=(pl.BlockSpec(memory_space=pl.ANY), pl.BlockSpec(memory_space=pltpu.VMEM)),
        scratch_shapes=[
            f32(2, 8, NY), f32(128, 2, 8, NY), f32(2, 8, NY), f32(2, 8, NY), f32(128, 2, 8, NY), f32(128, 2, 8, NY), f32(2, 8, 128, NY), f32(2, 2, K, NY),
            f32(1280, 128), f32(640, 128), f32(640, 128), f32(3, 160, 128), f32(3, 40, 128), f32(4, 40, 128),
            f32(160, 128), f32(40, 128), f32(1280, 128),
            f32(8, 4, 24, NY), f32(2, 24, 8, NY), f32(2, 24, 8, NY), f32(2, 24, 8, NY), f32(2, 24, 8, NY), f32(2, 24, 8, NY),
            f32(K, K), f32(K, K), f32(K, K), f32(128, 256), f32(K, K), f32(384, K), f32(2, 2, K, NY),
            f32(2, 2, 2, 128, NY), f32(2, 2, 2, 128, NY),
            sem((2,)), sem((2,)), sem((CHUNKS, 2)), sem((CHUNKS, 2)), sem((CHUNKS, 3)), sem((CHUNKS, 3)),
            sem((43,)), sem((43,)), sem((3,)), sem((3,)), sem((2, 4)), sem((2, 4)), sem((2, 4)), sem((2,)),
        ],
        compiler_params=pltpu.CompilerParams(collective_id=0, has_side_effects=True, vmem_limit_bytes=52000 * 1024),
        name="whole",
    )(base, x)


SETTLE = 32


def settle_kernel(frames_ref, rows_ref, o_ref, fac_ref, turned, sem, fac_sem):
    rows = pltpu.make_async_copy(rows_ref, fac_ref, fac_sem)
    rows.start()
    copies = []
    for n in range(128 // SETTLE):
        for g in range(n * SETTLE, n * SETTLE + SETTLE, 8):
            for f in range(2):
                turned[g : g + 8, f] = jnp.swapaxes(frames_ref[f, :, g : g + 8, :], 0, 1)
        some = pl.ds(n * SETTLE, SETTLE)
        copies.append(pltpu.make_async_copy(turned.at[some], o_ref.at[some], sem.at[n]))
        copies[-1].start()
    for copy in copies:
        copy.wait()
    rows.wait()


def settled(frames, rows):
    return pl.pallas_call(
        settle_kernel,
        out_shape=(jax.ShapeDtypeStruct((128, 2, 8, NY), jnp.float32), jax.ShapeDtypeStruct((128, K), jnp.float32)),
        in_specs=[pl.BlockSpec(memory_space=pltpu.VMEM)] * 2,
        out_specs=(pl.BlockSpec(memory_space=pl.ANY),) * 2,
        scratch_shapes=[
            pltpu.VMEM((128, 2, 8, NY), jnp.float32),
            pltpu.SemaphoreType.DMA((128 // SETTLE,)), pltpu.SemaphoreType.DMA(()),
        ],
        compiler_params=pltpu.CompilerParams(vmem_limit_bytes=16 * 1024 * 1024),
        name="settle",
    )(frames, rows)


def per_device(base, tangents):
    return settled(*whole(base, tangents))


def solution(mesh):
    split = Mesh(
        mesh.devices.reshape(mesh.shape["tan"], 4, 4, 2), ("tan", "grid_0", "grid_1", "grid_2")
    )
    placed = (P(None, GRID, None), P("tan", None, GRID, None))
    return jax.shard_map(
        per_device,
        mesh=split,
        in_specs=placed,
        out_specs=(P("tan", None, GRID, None), P("tan", None)),
        check_vma=False,
    )
```

```python
import functools
import jax
import jax.numpy as jnp
from jax import lax
from jax.experimental import pallas as pl
from jax.experimental.pallas import tpu as pltpu
from jax.sharding import Mesh
from jax.sharding import PartitionSpec as P

K = 512
NX = 256
NY = 256
GRID = ("grid_0", "grid_1", "grid_2")
HI = lax.Precision.HIGHEST

def factor_block(d, rows):
    lane = lax.broadcasted_iota(jnp.int32, (8, 128), 1)
    sub = lax.broadcasted_iota(jnp.int32, (8, 128), 0)
    wide = lambda x: jnp.broadcast_to(x, (8, 128))
    e = [jnp.where(lane == sub + 8 * i, 1.0, 0.0).astype(jnp.float32) for i in range(16)]
    head = [wide(d[0][:, j : j + 1]) for j in range(8)]
    for t in range(16):
        s = t * 8
        column = [{i: wide(d[i][:, s + j : s + j + 1]) for i in range(t + 1, 16)} for j in range(8)]
        ahead = [wide(d[t + 1][:, s + 8 + j : s + 9 + j]) for j in range(8)] if t < 15 else None
        for j in range(8):
            r = lax.rsqrt(wide(head[j][j : j + 1, :]))
            top = head[j] * r
            pivots = {k: wide(top[k : k + 1, :]) for k in range(j + 1, 8)}
            for k in range(j + 1, 8):
                head[k] = head[k] - top * pivots[k]
            row_d = wide(d[t][j : j + 1, :]) * r
            row_e = wide(e[t][j : j + 1, :]) * r
            rows(s + j, row_d[0:1], row_e[0:1])
            if j < 7:
                d[t] = d[t] - top * row_d
                e[t] = e[t] - top * row_e
            for i in range(t + 1, 16):
                low = column[j][i] * r
                if i == t + 1:
                    for k in range(8):
                        ahead[k] = ahead[k] - low * wide(low[k : k + 1, :])
                for k in range(j + 1, 8):
                    column[k][i] = column[k][i] - low * pivots[k]
                d[i] = d[i] - low * row_d
                e[i] = e[i] - low * row_e
        head = ahead


def dot(a, b, dims=((1,), (0,))):
    return lax.dot_general(a, b, (dims, ((), ())), precision=HI, preferred_element_type=jnp.float32)


def factor(scale, arrived, g_ref, inv_ref, fac_ref, a_ref, e_ref, u_ref, w_ref):
    def unpack(block):
        i, j = PACKED[block]
        for h in range(2):
            at, to = h * 640 + block * 64, i * 128 + h * 64
            a_ref[to : to + 64, j * 128 : j * 128 + 128] = g_ref[at : at + 64] * scale

    unpack(0)

    def step(k, carry):
        at = pl.multiple_of(k * 128, 128)
        d = [a_ref[pl.ds(pl.multiple_of(at + 8 * i, 8), 8), pl.ds(at, 128)] for i in range(16)]

        def rows(j, row_d, row_e):
            w_ref[j : j + 1, 0:128] = row_d
            w_ref[j : j + 1, 128:256] = row_e

        factor_block(d, rows)

        @pl.when(k == 0)
        def _():
            arrived()
            for block in range(1, 10):
                unpack(block)

        for kk in range(4):
            @pl.when(k == kk)
            def _():
                lo, hi = kk * 128, kk * 128 + 128
                upper = lax.broadcasted_iota(jnp.int32, (128, 128), 1) >= lax.broadcasted_iota(jnp.int32, (128, 128), 0)
                u_ref[lo:hi, lo:hi] = jnp.where(upper, w_ref[:, 0:128], 0.0)
                w = w_ref[:, 128:256]
                inv_ref[lo:hi, lo:hi] = w
                if kk:
                    inv_ref[lo:hi, 0:lo] = dot(w, e_ref[lo:hi, 0:lo])
                if kk < 3:
                    right = dot(w, a_ref[lo:hi, hi:512])
                    u_ref[lo:hi, hi:512] = right
                    left = right.T
                    a_ref[hi:512, hi:512] = a_ref[hi:512, hi:512] - dot(left, right)
                    e_ref[hi:512, 0:hi] = e_ref[hi:512, 0:hi] - dot(left, inv_ref[lo:hi, 0:hi])
        return carry

    lax.fori_loop(0, 4, step, 0)
    t = pl.multiple_of(lax.axis_index("tan") * 128, 128)
    fac_ref[...] = u_ref[:, pl.ds(t, 128)].T


spread_u, spread_v, feed_rate, kill_rate, step_size = 1.0, 0.5, 0.04, 0.06, 0.33
STAGES = (0.5 * step_size, 0.5 * step_size, step_size, step_size / 6.0) * 2

def base_coefficients(u, v, coef_ref):
    def lap(x):
        return (pltpu.roll(x, 1, 0) + pltpu.roll(x, 23, 0) + pltpu.roll(x, 1, 1) + pltpu.roll(x, NY - 1, 1) - 4.0 * x)

    def slopes(u, v):
        growth = u * v * v
        return (
            spread_u * lap(u) - growth + feed_rate * (1.0 - u),
            spread_v * lap(v) + growth - (feed_rate + kill_rate) * v,
        )

    for step in range(2):
        su, sv = u, v
        tu = tv = 0.0
        for stage in range(4):
            scale = STAGES[stage]
            square, cross = v2uv(su, sv)
            own = {0: 1.0, 1: 0.0, 2: 0.0, 3: 1.0 / 3.0}[stage]
            coef_ref[step * 4 + stage, 0] = own - scale * (4.0 * spread_u + feed_rate + square)
            coef_ref[step * 4 + stage, 1] = scale * cross
            coef_ref[step * 4 + stage, 2] = scale * square
            coef_ref[step * 4 + stage, 3] = own + scale * (cross - 4.0 * spread_v - feed_rate - kill_rate)
            if step == 1 and stage == 3:
                break
            ku, kv = slopes(su, sv)
            weight = (1.0, 2.0, 2.0, 1.0)[stage]
            tu, tv = tu + weight * ku, tv + weight * kv
            if stage < 3:
                ahead = (0.5, 0.5, 1.0)[stage] * step_size
                su, sv = u + ahead * ku, v + ahead * kv
        u, v = u + step_size / 6.0 * tu, v + step_size / 6.0 * tv


def v2uv(u, v):
    return v * v, 2.0 * u * v


def advance_group(get, put, coef_ref, z_refs, y_ref):
    first = get
    for stage in range(8):
        phase = stage % 4
        scale = STAGES[stage]
        out_lo, out_hi = stage + 1, 23 - stage
        src = {0: first, 1: reader(z_refs[0]), 2: reader(z_refs[1]), 3: reader(z_refs[2])}[phase]
        window = {}

        def at(row):
            if row not in window:
                window[row] = (src(0, row), src(1, row))
            return window[row]

        for row in range(out_lo, out_hi):
            up, mid, down = at(row - 1), at(row), at(row + 1)
            sums = [
                (up[f] + down[f]) + (pltpu.roll(mid[f], 1, 1) + pltpu.roll(mid[f], NY - 1, 1))
                for f in range(2)
            ]
            cp, bp, cq, aq = (coef_ref[stage, n, row : row + 1, :] for n in range(4))
            p = scale * spread_u * sums[0] + (cp * mid[0] - bp * mid[1])
            q = scale * spread_v * sums[1] + (cq * mid[0] + aq * mid[1])
            for f, new in ((0, p), (1, q)):
                if phase in (1, 2):
                    new = new + first(f, row)
                if phase == 3:
                    two = z_refs[1][f, row]
                    new = new + (1.0 / 3.0) * ((z_refs[0][f, row] - first(f, row)) + (two + two))
                if stage == 7:
                    put(f, row - 8, new)
                elif phase == 3:
                    y_ref[f, row] = new
                else:
                    z_refs[phase][f, row] = new
            del window[row - 1]
        if stage == 3:
            first = reader(y_ref)


def reader(ref):
    return lambda f, row: ref[f, row]


CHUNK = 8
CHUNKS = 128 // CHUNK
PACKED = [(i, j) for i in range(4) for j in range(i, 4)]
MESH_ID = pl.DeviceIdType.MESH


def place():
    return tuple(lax.axis_index(a) for a in ("tan",) + GRID)


def band_at(index):
    return {"grid_0": index // 8, "grid_1": index // 2 % 4, "grid_2": index % 2}


def along(core, turn, shift):
    x, z, y, _ = place()
    if turn == 2:
        return {"tan": (x + shift) % 4}, x
    on_y = 1 - core if turn == 0 else core
    spot = y * on_y + z * (1 - on_y)
    return {"grid_0": (z + shift * (1 - on_y)) % 4, "grid_1": (y + shift * on_y) % 4}, spot


def remote(source, target, send, receive, device):
    return pltpu.make_async_remote_copy(
        src_ref=source, dst_ref=target, send_sem=send, recv_sem=receive, device_id=device, device_id_type=MESH_ID
    )


def greet(devices):
    barrier = pltpu.get_barrier_semaphore()
    for device in devices:
        pl.semaphore_signal(barrier, inc=1, device_id=device, device_id_type=MESH_ID)
    pl.semaphore_wait(barrier, len(devices))


def packed_gram(i, v, part):
    lo = i * 256
    total = None
    for f in range(2):
        for row in range(2):
            term = dot(v[f, row, lo : lo + 256, :], v[f, row, lo:K, :], ((1,), (1,)))
            total = term if total is None else total + term
    for a in range(2):
        for b in range(a, 4 - 2 * i):
            block = PACKED.index((2 * i + a, 2 * i + b))
            for h in range(2):
                to, at = h * 640 + block * 64, a * 128 + h * 64
                part[to : to + 64] = total[at : at + 64, b * 128 : b * 128 + 128]


def sum_over_devices(v, part, acc, from_core, got_a, got_b, got_c, mid, low, total, sends, receives, then):
    core = place()[3]
    other = {"grid_2": 1 - core}

    def swap(n):
        lo, count = ((0, 224), (224, 224), (448, 192))[n]
        away = pl.ds(pl.multiple_of((1 - core) * 640 + lo, 32), count)
        return remote(part.at[away], from_core.at[lo : lo + count], sends.at[n], receives.at[n], other)

    packed_gram(0, v, part)
    swap(0).start()
    swap(1).start()
    packed_gram(1, v, part)
    swap(2).start()
    for n in range(3):
        swap(n).wait()
    acc[...] = part[pl.ds(pl.multiple_of(core * 640, 128), 640)] + from_core[...]
    copies = []
    for k in (2, 1, 3):
        there, spot = along(core, 0, k)
        rows = pl.ds(pl.multiple_of((spot + k) % 4 * 160, 8), 160)
        copies.append(remote(acc.at[rows], got_a.at[k - 1], sends.at[2 + k], receives.at[2 + k], there))
        copies[-1].start()
    for copy in copies:
        copy.wait()
    spot_a = along(core, 0, 0)[1]
    mid[...] = (acc[pl.ds(pl.multiple_of(spot_a * 160, 8), 160)] + got_a[0]) + (got_a[1] + got_a[2])
    copies = []
    for k in (2, 1, 3):
        there, spot = along(core, 1, k)
        rows = pl.ds(pl.multiple_of((spot + k) % 4 * 40, 8), 40)
        copies.append(remote(mid.at[rows], got_b.at[k - 1], sends.at[5 + k], receives.at[5 + k], there))
        copies[-1].start()
    for copy in copies:
        copy.wait()
    spot_b = along(core, 1, 0)[1]
    low[...] = (mid[pl.ds(pl.multiple_of(spot_b * 40, 8), 40)] + got_b[0]) + (got_b[1] + got_b[2])
    copies = []
    for k in (2, 1, 3):
        there, spot_c = along(core, 2, k)
        copies.append(remote(low, got_c.at[spot_c], sends.at[8 + k], receives.at[8 + k], there))
        copies[-1].start()
    got_c[along(core, 2, 0)[1]] = low[...]
    for copy in copies:
        copy.wait()

    def piece(of_core, a, b):
        return total.at[pl.ds(pl.multiple_of(of_core * 640 + a % 4 * 160 + b % 4 * 40, 8), 40)]

    def to_b(k):
        mine = piece(core, spot_a, spot_b)
        return remote(mine, mine, sends.at[11 + k], receives.at[11 + k], along(core, 1, k)[0])

    def to_a(k, kb):
        held = piece(core, spot_a, spot_b + 4 - kb)
        return remote(held, held, sends.at[15 + (k - 1) * 4 + kb], receives.at[15 + (k - 1) * 4 + kb], along(core, 0, k)[0])

    def to_core(ka, kb):
        held = piece(core, spot_a + 4 - ka, spot_b + 4 - kb)
        return remote(held, held, sends.at[27 + ka * 4 + kb], receives.at[27 + ka * 4 + kb], other)

    total[pl.ds(pl.multiple_of(spot_a * 160 + spot_b * 40 + core * 640, 8), 40)] = (got_c[0] + got_c[1]) + (got_c[2] + got_c[3])
    for k in (2, 1, 3):
        to_b(k).start()
    for k in (2, 1, 3):
        to_a(k, 0).start()
    to_core(0, 0).start()
    then()
    for kb in (1, 3, 2):
        to_b(kb).wait_recv()
        for k in (2, 1, 3):
            to_a(k, kb).start()
        to_core(0, kb).start()
    for kb in (0, 1, 3, 2):
        for ka in (1, 3, 2):
            to_a(ka, kb).wait_recv()
            to_core(ka, kb).start()
    def from_partner(a, b):
        held = piece(1 - core, a, b)
        n = 27 + (spot_b + 4 - a) % 4 * 4 + (spot_a + 4 - b) % 4
        return remote(held, held, sends.at[n], receives.at[n], other)

    early = [(0, 0), (0, 1)]
    for a, b in early:
        from_partner(a, b).wait_recv()

    def arrived():
        for a in range(4):
            for b in range(4):
                if (a, b) not in early:
                    from_partner(a, b).wait_recv()

    def sent():
        for k in (1, 2, 3):
            to_b(k).wait_send()
            for kb in range(4):
                to_a(k, kb).wait_send()
        for kb in range(4):
            for ka in range(4):
                to_core(ka, kb).wait_send()

    return arrived, sent


def whole_kernel(
    base_hbm, x_hbm, o_ref, fac_ref, base_ref, x_ref,
    base_above, base_below, top, bottom, out, v, part, acc, from_core, got_a, got_b, got_c, mid, low, total,
    coef_ref, z0, z1, z2, y_ref, first, a_ref, e_ref, u_ref, w_ref, inv, turned, opposite, made, own,
    base_send, base_recv, halo_send, halo_recv, give_send, give_recv, sum_send, sum_recv,
    ahead_send, ahead_recv, back_send, back_recv, own_sem, load_sem,
):
    x, z, y, core = place()
    band = (z * 4 + y) * 2 + core
    after, before = band_at((band + 1) % 32), band_at((band + 31) % 32)
    peers = [{"tan": (x + k) % 4} for k in (1, 2, 3)]
    load = pltpu.make_async_copy(x_hbm, x_ref, load_sem.at[0])
    load_base = pltpu.make_async_copy(base_hbm, base_ref, load_sem.at[1])
    load_base.start()
    load.start()
    greet(
        [after, before, {"grid_2": 1 - core}] + peers
        + [{"grid_1": (y + k) % 4} for k in (1, 2, 3)] + [{"grid_0": (z + k) % 4} for k in (1, 2, 3)]
    )
    bases = (
        remote(base_ref, base_above, base_send.at[0], base_recv.at[0], after),
        remote(base_ref, base_below, base_send.at[1], base_recv.at[1], before),
    )
    load_base.wait()
    for copy in bases:
        copy.start()

    def halos(c):
        some = pl.ds(pl.multiple_of(c * CHUNK, CHUNK), CHUNK)
        return (
            remote(x_ref.at[some], top.at[some], halo_send.at[c, 0], halo_recv.at[c, 0], after),
            remote(x_ref.at[some], bottom.at[some], halo_send.at[c, 1], halo_recv.at[c, 1], before),
        )

    def gifts(c):
        some = pl.ds(pl.multiple_of(c * CHUNK, CHUNK), CHUNK)
        mine = pl.ds(pl.multiple_of(x * 128 + c * CHUNK, CHUNK), CHUNK)
        return [
            remote(
                out.at[:, pl.ds((x + k) % 4 * 2, 2), some], v.at[:, :, mine],
                give_send.at[c, k - 1], give_recv.at[c, k - 1], {"tan": (x + k) % 4},
            )
            for k in (2, 1, 3)
        ]

    def give(c):
        some = pl.ds(pl.multiple_of(c * CHUNK, CHUNK), CHUNK)
        mine = pl.ds(pl.multiple_of(x * 128 + c * CHUNK, CHUNK), CHUNK)
        v[:, :, mine] = out[:, pl.ds(x * 2, 2), some]
        for copy in gifts(c):
            copy.start()

    def start_halo(c, carry):
        for copy in halos(c):
            copy.start()
        return carry

    load.wait()
    lax.fori_loop(0, CHUNKS, start_halo, 0)
    e_ref[...] = jnp.zeros_like(e_ref)
    u_ref[...] = jnp.zeros_like(u_ref)
    inv[...] = jnp.zeros_like(inv)
    for copy in bases:
        copy.wait_recv()
    u, w = (jnp.concatenate([base_above[f], base_ref[f], base_below[f]], 0) for f in range(2))
    base_coefficients(u, w, coef_ref)

    def advance_chunk(c, carry):
        for copy in halos(c):
            copy.wait_recv()

        @pl.when(c > 0)
        def _():
            give(c - 1)

        def group(g, carry):
            eight = pl.ds(pl.multiple_of(c * CHUNK + g * 8, 8), 8)

            for n, ref in enumerate((top, x_ref, bottom)):
                for f in range(2):
                    first[f, n * 8 : n * 8 + 8] = jnp.swapaxes(ref[eight, f], 0, 1)

            def put(f, row, value):
                out[f, row, eight, :] = value

            advance_group(reader(first), put, coef_ref, (z0, z1, z2), y_ref)
            return carry

        return lax.fori_loop(0, CHUNK // 8, group, carry)

    lax.fori_loop(0, CHUNKS, advance_chunk, 0)
    give(CHUNKS - 1)

    def receive(c, carry):
        for copy in gifts(c):
            copy.wait_recv()
        return carry

    lax.fori_loop(0, CHUNKS, receive, 0)
    def ahead(k, chip):
        rows = pl.ds((chip + k + 2) % 4 * 2, 2)
        block = pl.ds(pl.multiple_of(chip * 128, 128), 128)
        return remote(
            out.at[:, rows], opposite.at[:, :, block], ahead_send.at[k - 1], ahead_recv.at[k - 1], {"tan": (chip + k) % 4}
        )

    def send_ahead(shifts):
        for k in shifts:
            @pl.when(x + k < 4)
            def _():
                ahead(k, x).start()

    send_ahead((1, 3))
    arrived, sent = sum_over_devices(v, part, acc, from_core, got_a, got_b, got_c, mid, low, total, sum_send, sum_recv, lambda: send_ahead((2,)))
    factor(1.0 / (2.0 * NX * NY), arrived, total, inv, fac_ref, a_ref, e_ref, u_ref, w_ref)

    pairs = [(f, row) for f in range(2) for row in range(2)]

    def back(n, k, f, row):
        return remote(
            made.at[n, f, row], o_ref.at[f, x * 2 + row],
            back_send.at[n, f * 2 + row], back_recv.at[n, f * 2 + row], {"tan": (x + k) % 4},
        )

    def rows_of(block):
        return inv[pl.ds(pl.multiple_of(block % 4 * 128, 128), 128), :]

    turned[...] = jnp.concatenate([rows_of(x + 1), rows_of(x + 3), rows_of(x)], 0)
    keeps = []

    def keep(n, chip, f, row, value):
        own[n, f, row] = value
        copy = pltpu.make_async_copy(own.at[n, f, row], o_ref.at[f, chip * 2 + row], own_sem.at[n, f * 2 + row])
        copy.start()
        return copy

    for f, row in pairs:
        frames = dot(turned[0:256, :], v[f, row])
        for n, k in ((0, 1), (1, 3)):
            made[n, f, row] = frames[n * 128 : n * 128 + 128]
            back(n, k, f, row).start()
    for f, row in pairs:
        keeps.append(keep(0, x, f, row, dot(turned[256:384, :], v[f, row])))
    opposite[:, :, pl.ds(pl.multiple_of(x * 128, 128), 128)] = out[:, pl.ds((x + 2) % 4 * 2, 2)]
    for k in (1, 2, 3):
        @pl.when(x + k < 4)
        def _():
            opposite[:, :, pl.ds(pl.multiple_of((x + k) % 4 * 128, 128), 128)] = jnp.zeros((2, 2, 128, NY), jnp.float32)

        @pl.when(x >= k)
        def _():
            ahead(k, x - k).wait_recv()
    for f, row in pairs:
        keeps.append(keep(1, (x + 2) % 4, f, row, dot(turned[256:384, :], opposite[f, row])))

    for f, row in pairs:
        for n, k in ((0, 1), (1, 3)):
            back(n, k, f, row).wait()
    for k in (1, 2, 3):
        @pl.when(x + k < 4)
        def _():
            ahead(k, x).wait_send()

    def finish(c, carry):
        for copy in halos(c):
            copy.wait_send()
        for copy in gifts(c):
            copy.wait_send()
        return carry

    sent()
    lax.fori_loop(0, CHUNKS, finish, 0)
    for copy in bases:
        copy.wait_send()
    for copy in keeps:
        copy.wait()


def whole(base, x):
    f32 = lambda *shape: pltpu.VMEM(shape, jnp.float32)
    sem = pltpu.SemaphoreType.DMA
    return pl.pallas_call(
        whole_kernel,
        out_shape=(jax.ShapeDtypeStruct((2, 8, 128, NY), jnp.float32), jax.ShapeDtypeStruct((128, K), jnp.float32)),
        in_specs=[pl.BlockSpec(memory_space=pltpu.HBM)] * 2,
        out_specs=(pl.BlockSpec(memory_space=pl.ANY), pl.BlockSpec(memory_space=pltpu.VMEM)),
        scratch_shapes=[
            f32(2, 8, NY), f32(128, 2, 8, NY), f32(2, 8, NY), f32(2, 8, NY), f32(128, 2, 8, NY), f32(128, 2, 8, NY), f32(2, 8, 128, NY), f32(2, 2, K, NY),
            f32(1280, 128), f32(640, 128), f32(640, 128), f32(3, 160, 128), f32(3, 40, 128), f32(4, 40, 128),
            f32(160, 128), f32(40, 128), f32(1280, 128),
            f32(8, 4, 24, NY), f32(2, 24, 8, NY), f32(2, 24, 8, NY), f32(2, 24, 8, NY), f32(2, 24, 8, NY), f32(2, 24, 8, NY),
            f32(K, K), f32(K, K), f32(K, K), f32(128, 256), f32(K, K), f32(384, K), f32(2, 2, K, NY),
            f32(2, 2, 2, 128, NY), f32(2, 2, 2, 128, NY),
            sem((2,)), sem((2,)), sem((CHUNKS, 2)), sem((CHUNKS, 2)), sem((CHUNKS, 3)), sem((CHUNKS, 3)),
            sem((43,)), sem((43,)), sem((3,)), sem((3,)), sem((2, 4)), sem((2, 4)), sem((2, 4)), sem((2,)),
        ],
        compiler_params=pltpu.CompilerParams(collective_id=0, has_side_effects=True, vmem_limit_bytes=52000 * 1024),
        name="whole",
    )(base, x)


SETTLE = 32


def settle_kernel(frames_ref, rows_ref, o_ref, fac_ref, turned, sem, fac_sem):
    rows = pltpu.make_async_copy(rows_ref, fac_ref, fac_sem)
    rows.start()
    copies = []
    for n in range(128 // SETTLE):
        for g in range(n * SETTLE, n * SETTLE + SETTLE, 8):
            for f in range(2):
                turned[g : g + 8, f] = jnp.swapaxes(frames_ref[f, :, g : g + 8, :], 0, 1)
        some = pl.ds(n * SETTLE, SETTLE)
        copies.append(pltpu.make_async_copy(turned.at[some], o_ref.at[some], sem.at[n]))
        copies[-1].start()
    for copy in copies:
        copy.wait()
    rows.wait()


def settled(frames, rows):
    return pl.pallas_call(
        settle_kernel,
        out_shape=(jax.ShapeDtypeStruct((128, 2, 8, NY), jnp.float32), jax.ShapeDtypeStruct((128, K), jnp.float32)),
        in_specs=[pl.BlockSpec(memory_space=pltpu.VMEM)] * 2,
        out_specs=(pl.BlockSpec(memory_space=pl.ANY),) * 2,
        scratch_shapes=[
            pltpu.VMEM((128, 2, 8, NY), jnp.float32),
            pltpu.SemaphoreType.DMA((128 // SETTLE,)), pltpu.SemaphoreType.DMA(()),
        ],
        compiler_params=pltpu.CompilerParams(vmem_limit_bytes=16 * 1024 * 1024),
        name="settle",
    )(frames, rows)


def per_device(base, tangents):
    return settled(*whole(base, tangents))


def solution(mesh):
    split = Mesh(
        mesh.devices.reshape(mesh.shape["tan"], 4, 4, 2), ("tan", "grid_0", "grid_1", "grid_2")
    )
    placed = (P(None, GRID, None), P("tan", None, GRID, None))
    return jax.shard_map(
        per_device,
        mesh=split,
        in_specs=placed,
        out_specs=(P("tan", None, GRID, None), P("tan", None)),
        check_vma=False,
    )
```
